32 devices in a mesh: gx: 2 (over x), gy: 4 (over z), gz: 4 (over y, core).
Axes of the slice: x: 2, y: 2, z: 4, core: 2. Of those that a mesh axis runs over, the one named last changes fastest.
Arguments:
- fields: float32 [1, 64, 128, 512], P(None, 'gx', 'gy', 'gz'), may hold values from -13 to 13
- exponents: int32 [5], replicated, may hold values from -5 to -1
Outputs:
- coefficients: float32 [1, 64, 128, 512], P(None, 'gx', 'gy', 'gz')
- statistics: float32 [2, 1, 5], replicated
The draws below stay inside these ranges and needn't reach their ends.
All inputs are finite; a program needn't handle non-finite values.
Results may differ from the reference program's by a relative error of at most 0.0003.
Values sent between devices are 32-bit elements; how exact they have to be, the bound alone decides.
A program may use at most 64 MiB of HBM per device.

```python
import jax
import jax.numpy as jnp
from jax import lax

FIELDS = 1
FINE = 3
COARSE = 2
LEVELS = 5
NX = 64
NY = 128
NZ = 512


def coarse_rough(key):
    block = 2 ** FINE
    values = jax.random.uniform(jax.random.fold_in(key, 23), (FIELDS, NX // block, NY // block, NZ // block), jnp.float32, -3.0, 3.0)
    values = jnp.repeat(values, block, axis=1)
    values = jnp.repeat(values, block, axis=2)
    return jnp.repeat(values, block, axis=3)


def draw_fields(key, part):
    shape = (FIELDS, NX, NY, NZ)
    coord_x = jnp.arange(NX, dtype=jnp.float32)[None, :, None, None] / NX
    coord_y = jnp.arange(NY, dtype=jnp.float32)[None, None, :, None] / NY
    coord_z = jnp.arange(NZ, dtype=jnp.float32)[None, None, None, :] / NZ
    rising = 0.5 + 1.5 * (coord_x + coord_y + coord_z) / 3.0
    rough = coarse_rough(key)
    noise = jax.random.truncated_normal(jax.random.fold_in(key, 7), -5.0, 5.0, shape, jnp.float32)
    return (rising * noise + rough).astype(jnp.float32)


def touch_ends(array, key, smallest, largest):
    spot = [jax.random.randint(jax.random.fold_in(key, axis), (), 0, length) for axis, length in enumerate(array.shape)]
    widest = array.shape.index(max(array.shape))
    next_to = spot[:widest] + [(spot[widest] + 1) % array.shape[widest]] + spot[widest + 1:]
    return array.at[tuple(spot)].set(smallest).at[tuple(next_to)].set(largest)


def setup_inputs(seed: int = 0) -> dict:
    seeds = jax.random.split(jax.random.key(seed), 3)
    return {
        "fields": draw_fields(jax.random.fold_in(seeds[2], 71), 0),
        "exponents": touch_ends(jax.random.randint(seeds[1], (LEVELS,), -5, 0), jax.random.fold_in(seeds[1], 1), -5, -1).astype(jnp.int32),
    }


def split_pair(values, axis_dim):
    length = values.shape[axis_dim]
    even_part = lax.slice_in_dim(values, 0, length, 2, axis_dim)
    odd_part = lax.slice_in_dim(values, 1, length, 2, axis_dim)
    return even_part, odd_part


def lift_whole(values, axis_dim):
    even_part, odd_part = split_pair(values, axis_dim)
    detail = odd_part - 0.5 * (even_part + jnp.roll(even_part, -1, axis_dim))
    smooth = even_part + 0.25 * (jnp.roll(detail, 1, axis_dim) + detail)
    return jnp.stack((smooth, detail), axis_dim + 1).reshape(values.shape)


def detail_mask(shape):
    parity_flags = [(jnp.arange(shape[index_dim]) % 2) == 0 for index_dim in (1, 2, 3)]
    smooth_cells = parity_flags[0][:, None, None] & parity_flags[1][None, :, None] & parity_flags[2][None, None, :]
    return jnp.where(smooth_cells, 0.0, 1.0).astype(jnp.float32)[None]


def shrink(values, exponent):
    thresh = jnp.exp2(exponent.astype(jnp.float32))
    return jnp.sign(values) * jnp.maximum(jnp.abs(values) - thresh, 0.0)


def reference(fields, exponents):
    current = fields
    layers = []
    energies = []
    retained = []
    cell_total = NX * NY * NZ
    for layer_index in range(FINE + COARSE):
        for axis_dim in (1, 2, 3):
            current = lift_whole(current, axis_dim)
        masking = detail_mask(current.shape)
        shrunk = shrink(current, exponents[layer_index])
        level_count = 7.0 * cell_total / 8 ** (layer_index + 1)
        energies.append(jnp.sum(current * current * masking, axis=(1, 2, 3)) / level_count)
        retained.append(jnp.sum(jnp.abs(shrunk) * masking, axis=(1, 2, 3)) / level_count)
        layers.append(shrunk)
        current = current[:, ::2, ::2, ::2]
    result = current
    for shrunk in reversed(layers):
        result = shrunk.at[:, ::2, ::2, ::2].set(result)
    statistics = jnp.stack((jnp.stack(energies, 1), jnp.stack(retained, 1)))
    return result, statistics
```

```python
import functools

import numpy as np

import jax
import jax.numpy as jnp
from jax import lax
from jax.experimental import pallas as pl
from jax.experimental.pallas import tpu as pltpu
from jax.sharding import PartitionSpec as P

FINE = 3
LEVELS = 5
LANES = 128
CHUNKS = 4
BUFFERS = 19
VMEM_LIMIT = 33_554_432
MESH = pl.DeviceIdType.MESH


def periodic_lift(length):
    eye = np.eye(length)
    even, odd = eye[0::2], eye[1::2]
    detail = odd - 0.5 * (even + np.roll(even, -1, 0))
    smooth = even + 0.25 * (np.roll(detail, 1, 0) + detail)
    whole = np.zeros((length, length))
    whole[0::2] = smooth
    whole[1::2] = detail
    return whole


def second_lift(length):
    whole = np.zeros((length, length))
    whole[0::2, 0::2] = periodic_lift(length // 2)
    return whole


def coarse_matrices(sizes, coarse):
    nx, ny, nz = sizes
    cx, cy, cz = coarse
    rows = np.arange(nx * ny * cx * cy)
    dev, inner = rows // (cx * cy), rows % (cx * cy)
    gx = (dev // ny) * cx + inner // cy
    gy = (dev % ny) * cy + inner % cy
    step = LANES // cz
    lanes = np.array([z * step + d for d in range(nz) for z in range(cz)])
    result = []
    for both_levels in (False, True):
        mx, my, mz = periodic_lift(nx * cx), periodic_lift(ny * cy), periodic_lift(nz * cz)
        if both_levels:
            mx, my, mz = second_lift(nx * cx) @ mx, second_lift(ny * cy) @ my, second_lift(nz * cz) @ mz
        both = mx[gx[:, None], gx[None]] * my[gy[:, None], gy[None]]
        along = np.zeros((LANES, LANES))
        along[np.ix_(lanes, lanes)] = mz.T
        result.append((both.astype(np.float32), along.astype(np.float32)))
    return [np.stack(pair) for pair in zip(*result)]


def iota(shape, axis):
    return lax.broadcasted_iota(jnp.int32, shape, axis)


def roll(values, shift, axis):
    return pltpu.roll(values, shift % values.shape[axis], axis)


def lift_rows(v, low, high):
    n = v.shape[0]
    row = iota(v.shape, 0)
    odd = row % 2 == 1
    up = jnp.where(row == n - 1, high, roll(v, -1, 0))
    w = jnp.where(odd, v - 0.5 * (roll(v, 1, 0) + up), v)
    down = jnp.where(row == 0, low - 0.5 * v, roll(w, 1, 0))
    return jnp.where(odd, w, w + 0.25 * (down + roll(w, -1, 0)))


def lift_lanes(v, rim, s):
    lane = iota(v.shape, 1)
    up = jnp.where(lane == LANES - s, rim, roll(v, -s, 1))
    w = jnp.where(lane % (2 * s) == s, v - 0.5 * (roll(v, s, 1) + up), v)
    down = jnp.where(lane == 0, rim - 0.5 * v, roll(w, s, 1))
    return jnp.where(lane % (2 * s) == 0, w + 0.25 * (down + roll(w, -s, 1)), w)


def shrink(v, thresh):
    return v - jnp.clip(v, -thresh, thresh)


def kernel(sizes, cells, exps_in, field_in, rows_in, lanes_in, out, stats, *scratch):
    nx, ny, nz = sizes
    ndev = nx * ny * nz
    scratch = list(scratch)
    field, exps, k_s, l_s, in_sem = scratch[-5:]
    scratch = scratch[:-5]
    loads = [
        pltpu.make_async_copy(a, b, in_sem.at[i])
        for i, (a, b) in enumerate(((field_in, field), (exps_in, exps), (rows_in, k_s), (lanes_in, l_s)))
    ]
    for load in loads:
        load.start()
    me = (lax.axis_index("gx"), lax.axis_index("gy"), lax.axis_index("gz"))

    def device(dx, dy, dz):
        return (
            lax.rem(me[0] + (dx + nx), nx),
            lax.rem(me[1] + (dy + ny), ny),
            lax.rem(me[2] + (dz + nz), nz),
        )

    def thresh(level):
        return jnp.exp2(jnp.full((1, LANES), exps[level].astype(jnp.float32)))

    def split(j):
        return j // (ny * nz), (j // nz) % ny, j % nz

    barrier = pltpu.get_barrier_semaphore()

    near = max(sizes) // 2 <= FINE
    greeted = {
        tuple((d + size - 1) % size if near else d for d, size in zip(spot, sizes))
        for spot in np.ndindex(*(3, 3, 3) if near else sizes)
    } - {(0, 0, 0)}
    for spot in sorted(greeted):
        pl.semaphore_signal(barrier, inc=1, device_id=device(*spot), device_id_type=MESH)
    gath, msg, rows_s, final_s, g_send, g_recv = scratch[-6:]
    sums = []
    loads[0].wait()
    loads[1].wait()
    away = (-1, 1)
    alone = nx == 2

    for level in range(FINE):
        (xs, xr, ys, yr, es, er, yl, zs, zr, hs, hr, ds, dr, cs, cr, work, nxt, send_sem, recv_sem) = scratch[
            level * BUFFERS : level * BUFFERS + BUFFERS
        ]
        s = 2**level
        n = field.shape[2] // s
        px = field.shape[1] // s
        src = field.at[0] if level == 0 else scratch[(level - 1) * BUFFERS + 16]
        lane = iota((n, LANES), 1)

        def edge(v):
            return v[0:1], v[n - 1 : n] - 0.5 * v[n - 2 : n - 1]

        e_plane = src[0]
        p_plane = src[px - 1] - 0.5 * src[px - 2]
        xs[0] = e_plane
        xs[1] = p_plane
        ys[0] = src[:, 0, :]
        ys[1] = src[:, n - 1, :] - 0.5 * src[:, n - 2, :]
        for a, plane in ((0, e_plane), (1, p_plane)):
            es[2 * a], es[2 * a + 1] = edge(plane)

        packed = jnp.zeros((n, LANES), jnp.float32)
        for x in range(px):
            v = src[x]
            u = jnp.where(lane == LANES - s, v - 0.5 * roll(v, s, 1), v)
            at = 2 * s * x
            packed = jnp.where((lane == at) | (lane == at + s), roll(u, at + s, 1), packed)
        half = 2 * s * px
        combined = packed - 0.5 * roll(packed, 2 * s, 1)
        sides = roll(jnp.where(lane < half // 2, packed, combined), half, 1)
        zs[...] = packed
        hs[...] = sides
        ds[0], ds[1] = edge(packed)
        cs[0], cs[1] = edge(sides)

        if level == 0:
            pl.semaphore_wait(barrier, len(greeted))
        copies = []
        ways = (0,) if alone else (0, 1)
        for i in (0, 1):
            for b in (0, 1):
                for a in ways:
                    copies.append((cs.at[b], cr.at[4 * a + 2 * b + i], (away[a], away[b], away[i])))
                copies.append((ds.at[b], dr.at[2 * b + i], (0, away[b], away[i])))
        for a in (0, 1):
            for b in (0, 1):
                copies.append((es.at[2 * a + b], er.at[2 * a + b], (away[a], away[b], 0)))
        for b in (0, 1):
            copies.append((ys.at[b], yr.at[b], (0, away[b], 0)))
        for i in (0, 1):
            for a in ways:
                copies.append((hs, hr.at[2 * a + i], (away[a], 0, away[i])))
        for a in (0, 1):
            copies.append((xs.at[a], xr.at[a], (away[a], 0, 0)))
        for i in (0, 1):
            copies.append((zs, zr.at[i], (0, 0, away[i])))
        flights = [
            pltpu.make_async_remote_copy(
                src_ref=f, dst_ref=t, send_sem=send_sem.at[i], recv_sem=recv_sem.at[i],
                device_id=device(*d), device_id_type=MESH,
            )
            for i, (f, t, d) in enumerate(copies)
        ]
        for flight in flights:
            flight.start()
        if level > 0:
            sums += finish()
        for flight in flights:
            flight.wait()

        for b in (0, 1):
            yl[b] = lift_rows(yr[b], er[2 + b], er[b])

        def rim_of(main, side):
            spot = iota(main(0).shape, 1)
            parts = []
            for i in (0, 1):
                after = side(0, i)
                before = after if alone else side(1, i)
                v = jnp.where(spot < half, main(i), 0.0)
                v = jnp.where((spot >= half) & (spot < half + 2 * s), after, v)
                parts.append(jnp.where(spot >= LANES - 2 * s, before, v))
            v = jnp.where(spot % (2 * s) < s, roll(parts[0], -s, 1), roll(parts[1], s, 1))
            odd = (spot // (2 * s)) % 2 == 1
            w = jnp.where(odd, v - 0.5 * (roll(v, 2 * s, 1) + roll(v, -2 * s, 1)), v)
            return jnp.where(odd, w, w + 0.25 * (roll(w, 2 * s, 1) + roll(w, -2 * s, 1)))

        rim_rows = [
            rim_of(lambda i: dr[2 * b + i], lambda a, i: cr[4 * a + 2 * b + i]) for b in (0, 1)
        ]
        rim = rim_of(lambda i: zr[i], lambda a, i: hr[2 * a + i])
        rim = lift_rows(rim, rim_rows[1], rim_rows[0])
        level_thresh = thresh(level)
        inner = (lane % (2 * s) == 0) & (iota((n, LANES), 0) % 2 == 0)
        active = lane % s == 0

        def plane_step(x, v):
            v = lift_rows(v, yl[1, x : x + 1, :], yl[0, x : x + 1, :])
            v = lift_lanes(v, roll(rim, LANES - s - 2 * s * x, 1), s)
            work[x] = v
            if x % 2 == 0:
                nxt[x // 2] = work[x, pl.ds(0, n // 2, stride=2), :]

        def finish(level=level, work=work, px=px, n=n, s=s, inner=inner, active=active, t=level_thresh):
            energy = kept = jnp.zeros((n, LANES), jnp.float32)
            for x in range(px):
                v = work[x]
                small = shrink(v, t)
                use = active & ~inner if x % 2 == 0 else active
                energy += jnp.where(use, v * v, 0.0)
                kept += jnp.where(use, jnp.abs(small), 0.0)
                if level == 0:
                    out[0, x] = small
                else:
                    spot = (0, s * x, pl.ds(0, n, stride=s), slice(None))
                    out[spot] = jnp.where(active, small, out[spot])
            return [
                jnp.sum(jnp.sum(v, axis=0, keepdims=True), axis=1, keepdims=True) for v in (energy, kept)
            ]

        even = src[0]
        before = xr[1] - 0.5 * even
        for k in range(px // 2):
            after = src[2 * k + 2] if 2 * k + 2 < px else xr[0]
            detail = src[2 * k + 1] - 0.5 * (even + after)
            smooth = even + 0.25 * (before + detail)
            plane_step(2 * k, smooth)
            plane_step(2 * k + 1, detail)
            even, before = after, detail

    last = scratch[(FINE - 1) * BUFFERS + 16]
    cx, cy = last.shape[0], last.shape[1]
    step = 2**FINE
    count = cx * cy
    for x in range(cx):
        rows_s[pl.ds(x * cy, cy), :] = last[x]
    here = rows_s[...]
    lane = iota((count, LANES), 1)
    row = iota((count, LANES), 0)
    here = jnp.where(lane % step == 0, here, 0.0)
    for bit in (1, 2, 4):
        here = jnp.where((row & bit) != 0, roll(here, bit, 1), here)
    groups = count // 8
    one = iota((1, LANES), 1)
    for g in range(groups):
        msg[g : g + 1] = jnp.sum(here[8 * g : 8 * g + 8], axis=0, keepdims=True)
    tail = jnp.zeros((1, LANES), jnp.float32)
    for i, whole in enumerate(sums + finish()):
        tail = jnp.where(one == i, whole, tail)
    msg[groups:] = jnp.broadcast_to(tail, (msg.shape[0] - groups, LANES))
    flat = (me[0] * ny + me[1]) * nz + me[2]

    def post(j):
        return pltpu.make_async_remote_copy(
            src_ref=msg, dst_ref=gath.at[flat], send_sem=g_send.at[j], recv_sem=g_recv.at[j],
            device_id=device(*split(j)), device_id_type=MESH,
        )

    def send(j, carry):
        post(ndev - j).start()
        return carry

    def settle(j, carry):
        post(j).wait()
        return carry

    if ndev <= 32:
        posts = [post(ndev - j) for j in range(1, ndev)]
        for flight in posts:
            flight.start()
        gath[flat] = msg[...]
        for flight in posts:
            flight.wait()
    else:
        lax.fori_loop(1, ndev, send, 0)
        gath[flat] = msg[...]
        lax.fori_loop(1, ndev, settle, 0)

    sub = iota((8, LANES), 0)
    lane8 = iota((8, LANES), 1)

    def unpack(d, tail):
        for g in range(groups):
            acc = jnp.zeros((8, LANES), jnp.float32)
            for z in range(nz):
                v = jnp.broadcast_to(gath[d * nz + z, g : g + 1, :], (8, LANES))
                for bit in (1, 2, 4):
                    v = jnp.where((sub & bit) != 0, roll(v, -bit, 1), v)
                acc += roll(jnp.where(lane8 % step == 0, v, 0.0), z, 1)
            final_s[pl.ds(pl.multiple_of(d * count + 8 * g, 8), 8), :] = acc
        for z in range(nz):
            tail += gath[d * nz + z, groups : groups + 1, :]
        return tail

    tail = lax.fori_loop(0, nx * ny, unpack, jnp.zeros((1, LANES), jnp.float32), unroll=nx * ny <= 8)

    def dot(a, b):
        return jnp.dot(a, b, precision=lax.Precision.HIGHEST, preferred_element_type=jnp.float32)

    grid = final_s[...]
    loads[2].wait()
    loads[3].wait()
    half3, half4 = dot(k_s[0], grid), dot(k_s[1], grid)
    grid, grid4 = dot(half3, l_s[0]), dot(half4, l_s[1])
    row = iota(grid.shape, 0)
    lane = iota(grid.shape, 1)
    inner_row = row % count
    gx, gy, gz = inner_row // cy, inner_row % cy, lane // step
    valid = lane % step < nz
    even3 = (gx % 2 == 0) & (gy % 2 == 0) & (gz % 2 == 0)
    even4 = (gx % 4 == 0) & (gy % 4 == 0) & (gz % 4 == 0)
    det3 = valid & ~even3
    det4 = valid & even3 & ~even4
    small3 = shrink(grid, thresh(FINE))
    small4 = shrink(grid4, thresh(FINE + 1))
    final_s[...] = jnp.where(even3, jnp.where(even4, grid4, small4), small3)

    def total(mask, v):
        return jnp.sum(jnp.sum(jnp.where(mask, v, 0.0), axis=0, keepdims=True), axis=1, keepdims=True)

    coarse = ((total(det3, grid * grid), total(det3, jnp.abs(small3))),
              (total(det4, grid4 * grid4), total(det4, jnp.abs(small4))))
    for q in (0, 1):
        line = jnp.zeros((1, LANES), jnp.float32)
        for level in range(LEVELS):
            weight = 8.0 ** (level + 1) / (7.0 * cells)
            if level < FINE:
                value = jnp.sum(jnp.where(one == 2 * level + q, tail, 0.0), axis=1, keepdims=True)
            else:
                value = coarse[level - FINE][q]
            line = jnp.where(one == level, value * weight, line)
        stats[q] = line[:, 0:LEVELS]

    first = pl.multiple_of((me[0] * ny + me[1]) * count, count)
    mine = pltpu.roll(final_s[pl.ds(first, count), :], lax.rem(LANES - me[2], LANES), 1)
    rows_s[...] = mine
    keep = iota((cy, LANES), 1) % step == 0
    for x in range(cx):
        spot = (0, step * x, pl.ds(0, cy, stride=step), slice(None))
        out[spot] = jnp.where(keep, rows_s[pl.ds(x * cy, cy), :], out[spot])


def deliver(held, held_stats, out, stats, sem):
    rows = held.shape[1] // CHUNKS
    copies = [pltpu.make_async_copy(held_stats, stats, sem.at[CHUNKS])]
    for i in range(CHUNKS):
        part = pl.ds(i * rows, rows)
        copies.append(pltpu.make_async_copy(held.at[:, part], out.at[:, part], sem.at[i]))
    for copy in copies:
        copy.start()
    for copy in copies:
        copy.wait()


def shards(sizes, fields, exponents):
    nx, ny, nz = sizes
    ndev = nx * ny * nz
    _, lx, ly, lz = fields.shape
    cells = fields.size * ndev
    step = 2**FINE
    coarse = (lx // step, ly // step, lz // step)
    count = coarse[0] * coarse[1]
    tables = coarse_matrices(sizes, coarse)
    scratch = []
    for level in range(FINE):
        x, y = lx >> level, ly >> level
        scratch += [
            *(pltpu.VMEM(shape, jnp.float32) for shape in (
                (2, y, LANES), (2, y, LANES), (2, x, LANES), (2, x, LANES), (4, 1, LANES), (4, 1, LANES),
                (2, x, LANES), (y, LANES), (2, y, LANES), (y, LANES), (4, y, LANES), (2, 1, LANES),
                (4, 1, LANES), (2, 1, LANES), (8, 1, LANES), (x, y, LANES), (x // 2, y // 2, LANES),
            )),
            pltpu.SemaphoreType.DMA((26,)),
            pltpu.SemaphoreType.DMA((26,)),
        ]
    height = -(-(count // 8 + 1) // 4) * 4
    scratch += [
        pltpu.VMEM((ndev, height, LANES), jnp.float32),
        pltpu.VMEM((height, LANES), jnp.float32),
        pltpu.VMEM((count, LANES), jnp.float32),
        pltpu.VMEM((nx * ny * count, LANES), jnp.float32),
        pltpu.SemaphoreType.DMA((ndev,)),
        pltpu.SemaphoreType.DMA((ndev,)),
        pltpu.VMEM(fields.shape, jnp.float32),
        pltpu.SMEM(exponents.shape, jnp.int32),
        pltpu.VMEM(tables[0].shape, jnp.float32),
        pltpu.VMEM(tables[1].shape, jnp.float32),
        pltpu.SemaphoreType.DMA((4,)),
    ]
    vmem = pl.BlockSpec(memory_space=pltpu.VMEM)
    held = pl.pallas_call(
        functools.partial(kernel, sizes, cells),
        out_shape=(
            pltpu.VMEM(fields.shape, jnp.float32),
            pltpu.VMEM((2, 1, LEVELS), jnp.float32),
        ),
        in_specs=[pl.BlockSpec(memory_space=pltpu.HBM)] * 4,
        out_specs=(vmem, vmem),
        scratch_shapes=scratch,
        compiler_params=pltpu.CompilerParams(
            collective_id=0, has_side_effects=True, vmem_limit_bytes=VMEM_LIMIT
        ),
    )(*(pltpu.with_memory_space_constraint(x, pltpu.HBM) for x in (exponents, fields, *map(jnp.asarray, tables))))
    hbm = pl.BlockSpec(memory_space=pltpu.HBM)
    return pl.pallas_call(
        deliver,
        out_shape=(
            jax.ShapeDtypeStruct(fields.shape, jnp.float32),
            jax.ShapeDtypeStruct((2, 1, LEVELS), jnp.float32),
        ),
        in_specs=(vmem, vmem),
        out_specs=(hbm, hbm),
        scratch_shapes=[pltpu.SemaphoreType.DMA((CHUNKS + 1,))],
    )(*(pltpu.with_memory_space_constraint(x, pltpu.VMEM) for x in held))


def solution(mesh):
    sizes = tuple(mesh.shape[name] for name in ("gx", "gy", "gz"))
    placed = (P(None, "gx", "gy", "gz"), P())
    return jax.shard_map(
        functools.partial(shards, sizes),
        mesh=mesh,
        in_specs=placed,
        out_specs=placed,
        check_vma=False,
    )
```

```python
import functools

import numpy as np

import jax
import jax.numpy as jnp
from jax import lax
from jax.experimental import pallas as pl
from jax.experimental.pallas import tpu as pltpu
from jax.sharding import PartitionSpec as P

FINE = 3
LEVELS = 5
LANES = 128
CHUNKS = 4
BUFFERS = 18
TABLES = 7
ROUNDS = 2
VMEM_LIMIT = 33_554_432
MESH = pl.DeviceIdType.MESH


def periodic_lift(length):
    eye = np.eye(length)
    even, odd = eye[0::2], eye[1::2]
    detail = odd - 0.5 * (even + np.roll(even, -1, 0))
    smooth = even + 0.25 * (np.roll(detail, 1, 0) + detail)
    whole = np.zeros((length, length))
    whole[0::2] = smooth
    whole[1::2] = detail
    return whole


def second_lift(length):
    whole = np.zeros((length, length))
    whole[0::2, 0::2] = periodic_lift(length // 2)
    return whole


def coarse_matrices(sizes, coarse):
    nx, ny, nz = sizes
    cx, cy, cz = coarse
    rows = np.arange(nx * ny * cx * cy)
    dev, inner = rows // (cx * cy), rows % (cx * cy)
    gx = (dev // ny) * cx + inner // cy
    gy = (dev % ny) * cy + inner % cy
    step = LANES // cz
    lanes = np.array([z * step + d for d in range(nz) for z in range(cz)])
    result = []
    for both_levels in (False, True):
        mx, my, mz = periodic_lift(nx * cx), periodic_lift(ny * cy), periodic_lift(nz * cz)
        if both_levels:
            mx, my, mz = second_lift(nx * cx) @ mx, second_lift(ny * cy) @ my, second_lift(nz * cz) @ mz
        both = mx[gx[:, None], gx[None]] * my[gy[:, None], gy[None]]
        along = np.zeros((LANES, LANES))
        along[np.ix_(lanes, lanes)] = mz.T
        result.append((both.astype(np.float32), along.astype(np.float32)))
    return [np.stack(pair) for pair in zip(*result)]


def lift_line(n):
    whole = np.zeros((n, n + 2))
    cells = np.eye(n + 2)
    even, odd = cells[0:n:2], cells[1:n:2]
    after = np.concatenate((even[1:], cells[n + 1 :]))
    detail = odd - 0.5 * (even + after)
    before = np.concatenate((cells[n : n + 1] - 0.5 * even[:1], detail[:-1]))
    whole[0::2] = even + 0.25 * (before + detail)
    whole[1::2] = detail
    return whole

def line_tables(n):
    lift = lift_line(n)
    own = lift[:, :n]
    sent = np.zeros((4, n))
    sent[0, n - 1], sent[0, n - 2] = 1.0, -0.5
    sent[1] = own[n - 2] - 0.5 * own[n - 4]
    sent[2, 0] = 1.0
    sent[3] = own[0]
    first = np.zeros((n + 2, n + 4))
    first[:n, :n] = own
    first[:n, n], first[:n, n + 2] = lift[:, n], lift[:, n + 1]
    first[n, n + 1], first[n, 0] = 1.0, lift[n - 2, n + 1]
    first[n + 1, n + 3] = 1.0
    first[n + 1, :n] = lift[0, n] * sent[0]
    return sent, first, lift_line(n // 2)


def middle_tables(ax, ay, az):
    step = LANES // az
    sent_x, first_x, second_x = line_tables(ax)
    sent_y, first_y, second_y = line_tables(ay)
    sent_z, first_z, second_z = line_tables(az)
    own = [(x, y) for x in range(ax) for y in range(ay)]
    corners = [(x, 2 * g + y) for g in range(2) for x in range(4) for y in range(2)]
    extra = [(ax + k, y) for k in range(4) for y in range(ay)]
    extra += [(x, ay + k) for k in range(4) for x in range(ax)]
    extra += [(ax + x, ay + y) for x, y in corners]
    taken = np.array(own + extra)
    given = own + [(ax + k, y) for k in range(2) for y in range(0, ay, 2)]
    given += [(x, ay + k) for k in range(2) for x in range(0, ax, 2)]
    given += [(ax + x, ay + y) for x in range(2) for y in range(2)]
    height = -(-len(given) // 16) * 16

    whole_x, whole_y = np.concatenate((np.eye(ax), sent_x)), np.concatenate((np.eye(ay), sent_y))
    ex, ey = np.array(extra).T
    ox, oy = np.array(own).T
    send_rows = whole_x[np.ix_(ex, ox)] * whole_y[np.ix_(ey, oy)]
    gx, gy = np.array(given).T
    tx, ty = taken.T
    rows = np.zeros((height, len(taken)))
    rows[: len(given)] = first_x[np.ix_(gx, tx)] * first_y[np.ix_(gy, ty)]

    def spot(at, n):
        return np.where(at >= n, n // 2 + at - n, at // 2)

    half = np.array([(x, y) for x in range(ax // 2) for y in range(ay // 2)])
    use = ((gx % 2 == 0) | (gx >= ax)) & ((gy % 2 == 0) | (gy >= ay))
    last = np.zeros((len(half), height))
    pick_x = second_x[np.ix_(half[:, 0], spot(gx, ax))]
    pick_y = second_y[np.ix_(half[:, 1], spot(gy, ay))]
    last[:, : len(given)] = pick_x * pick_y * use

    lanes = np.arange(az) * step
    out = np.concatenate((lanes, [1, step + 1]))
    send_lanes = np.zeros((8, LANES))
    send_lanes[np.ix_(np.arange(4), lanes)] = sent_z
    along = np.zeros((LANES, LANES))
    along[np.ix_(lanes, out)] = first_z[:, :az].T
    rim = np.zeros((16, LANES))
    for part in range(3):
        rim[np.ix_(4 * part + np.arange(4), out)] = first_z[:, az:].T
    along_last = np.zeros((LANES, LANES))
    source = np.concatenate((lanes[0::2], [1, step + 1]))
    along_last[np.ix_(source, lanes[0::2])] = second_z.T
    result = (send_rows, rows, last, send_lanes, along, rim, along_last)
    return tuple(table.astype(jnp.bfloat16) for table in result)


def iota(shape, axis):
    return lax.broadcasted_iota(jnp.int32, shape, axis)


def roll(values, shift, axis):
    return pltpu.roll(values, shift % values.shape[axis], axis)


def lift_rows(v, low, high):
    n = v.shape[0]
    row = iota(v.shape, 0)
    odd = row % 2 == 1
    up = jnp.where(row == n - 1, high, roll(v, -1, 0))
    w = jnp.where(odd, v - 0.5 * (roll(v, 1, 0) + up), v)
    down = jnp.where(row == 0, low - 0.5 * v, roll(w, 1, 0))
    return jnp.where(odd, w, w + 0.25 * (down + roll(w, -1, 0)))


def lift_lanes(v, rim, s):
    lane = iota(v.shape, 1)
    up = jnp.where(lane == LANES - s, rim, roll(v, -s, 1))
    w = jnp.where(lane % (2 * s) == s, v - 0.5 * (roll(v, s, 1) + up), v)
    down = jnp.where(lane == 0, rim - 0.5 * v, roll(w, s, 1))
    return jnp.where(lane % (2 * s) == 0, w + 0.25 * (down + roll(w, -s, 1)), w)


def shrink(v, thresh):
    return v - jnp.clip(v, -thresh, thresh)


def three(v):
    parts = []
    for _ in range(3):
        parts.append(v.astype(jnp.bfloat16))
        v = v - parts[-1].astype(jnp.float32)
    return parts


def mix(a, b, dims):
    return lax.dot_general(a, b, (dims, ((), ())), preferred_element_type=jnp.float32)


def mix_rows(table, v):
    return sum(mix(table, part, ((1,), (0,))) for part in three(v))


def mix_lanes(v, table):
    return sum(mix(part, table, ((1,), (0,))) for part in three(v))


def total(v):
    return jnp.sum(jnp.sum(v, axis=0, keepdims=True), axis=1, keepdims=True)


def kernel(sizes, cells, exps_in, field_in, rows_in, lanes_in, *rest):
    tables_in, (out, stats), scratch = rest[:TABLES], rest[TABLES : TABLES + 2], rest[TABLES + 2 :]
    nx, ny, nz = sizes
    ndev = nx * ny * nz
    scratch = list(scratch)
    tables = scratch[-TABLES:]
    scratch = scratch[:-TABLES]
    field, exps, k_s, l_s, in_sem = scratch[-5:]
    scratch = scratch[:-5]
    pairs = [(field_in, field), (exps_in, exps), *zip(tables_in, tables), (rows_in, k_s), (lanes_in, l_s)]
    loads = [pltpu.make_async_copy(a, b, in_sem.at[i]) for i, (a, b) in enumerate(pairs)]
    for load in loads:
        load.start()
    me = (lax.axis_index("gx"), lax.axis_index("gy"), lax.axis_index("gz"))

    def device(dx, dy, dz):
        return (
            lax.rem(me[0] + (dx + nx), nx),
            lax.rem(me[1] + (dy + ny), ny),
            lax.rem(me[2] + (dz + nz), nz),
        )

    def thresh(level):
        return jnp.exp2(jnp.full((1, LANES), exps[level].astype(jnp.float32)))

    def split(j):
        return j // (ny * nz), (j // nz) % ny, j % nz

    barrier = pltpu.get_barrier_semaphore()

    near = max(sizes) // 2 <= ROUNDS
    greeted = {
        tuple((d + size - 1) % size if near else d for d, size in zip(spot, sizes))
        for spot in np.ndindex(*(3, 3, 3) if near else sizes)
    } - {(0, 0, 0)}
    for spot in sorted(greeted):
        pl.semaphore_signal(barrier, inc=1, device_id=device(*spot), device_id_type=MESH)
    gath, msg, rows_s, final_s, g_send, g_recv = scratch[-6:]
    loads[0].wait()
    loads[1].wait()
    away = (-1, 1)
    alone = nx == 2

    (xs, xr, ys, yr, es, er, yl, zs, zr, hs, hr, ds, dr, cs, cr, work, send_sem, recv_sem) = scratch[:BUFFERS]
    grown, sent, rims, side, hz, t2r, t3r, o1s, o2s, m_send, m_recv = scratch[BUFFERS : BUFFERS + 11]
    s = 1
    n = field.shape[2] // s
    px = field.shape[1] // s
    src = field.at[0]
    lane = iota((n, LANES), 1)

    def edge(v):
        return v[0:1], v[n - 1 : n] - 0.5 * v[n - 2 : n - 1]

    e_plane = src[0]
    p_plane = src[px - 1] - 0.5 * src[px - 2]
    xs[0] = e_plane
    xs[1] = p_plane
    ys[0] = src[:, 0, :]
    ys[1] = src[:, n - 1, :] - 0.5 * src[:, n - 2, :]
    for a, plane in ((0, e_plane), (1, p_plane)):
        es[2 * a], es[2 * a + 1] = edge(plane)

    packed = jnp.zeros((n, LANES), jnp.float32)
    for x in range(px):
        v = src[x]
        u = jnp.where(lane == LANES - s, v - 0.5 * roll(v, s, 1), v)
        at = 2 * s * x
        packed = jnp.where((lane == at) | (lane == at + s), roll(u, at + s, 1), packed)
    half = 2 * s * px
    combined = packed - 0.5 * roll(packed, 2 * s, 1)
    sides = roll(jnp.where(lane < half // 2, packed, combined), half, 1)
    zs[...] = packed
    hs[...] = sides
    ds[0], ds[1] = edge(packed)
    cs[0], cs[1] = edge(sides)

    pl.semaphore_wait(barrier, len(greeted))
    copies = []
    ways = (0,) if alone else (0, 1)
    for i in (0, 1):
        for b in (0, 1):
            for a in ways:
                copies.append((cs.at[b], cr.at[4 * a + 2 * b + i], (away[a], away[b], away[i])))
            copies.append((ds.at[b], dr.at[2 * b + i], (0, away[b], away[i])))
    for a in (0, 1):
        for b in (0, 1):
            copies.append((es.at[2 * a + b], er.at[2 * a + b], (away[a], away[b], 0)))
    for b in (0, 1):
        copies.append((ys.at[b], yr.at[b], (0, away[b], 0)))
    for i in (0, 1):
        for a in ways:
            copies.append((hs, hr.at[2 * a + i], (away[a], 0, away[i])))
    for a in (0, 1):
        copies.append((xs.at[a], xr.at[a], (away[a], 0, 0)))
    for i in (0, 1):
        copies.append((zs, zr.at[i], (0, 0, away[i])))
    flights = [
        pltpu.make_async_remote_copy(
            src_ref=f, dst_ref=t, send_sem=send_sem.at[i], recv_sem=recv_sem.at[i],
            device_id=device(*d), device_id_type=MESH,
        )
        for i, (f, t, d) in enumerate(copies)
    ]
    for flight in flights:
        flight.start()
    for flight in flights:
        flight.wait()

    for b in (0, 1):
        yl[b] = lift_rows(yr[b], er[2 + b], er[b])

    def rim_of(main, side):
        spot = iota(main(0).shape, 1)
        parts = []
        for i in (0, 1):
            after = side(0, i)
            before = after if alone else side(1, i)
            v = jnp.where(spot < half, main(i), 0.0)
            v = jnp.where((spot >= half) & (spot < half + 2 * s), after, v)
            parts.append(jnp.where(spot >= LANES - 2 * s, before, v))
        v = jnp.where(spot % (2 * s) < s, roll(parts[0], -s, 1), roll(parts[1], s, 1))
        odd = (spot // (2 * s)) % 2 == 1
        w = jnp.where(odd, v - 0.5 * (roll(v, 2 * s, 1) + roll(v, -2 * s, 1)), v)
        return jnp.where(odd, w, w + 0.25 * (roll(w, 2 * s, 1) + roll(w, -2 * s, 1)))

    rim_rows = [
        rim_of(lambda i: dr[2 * b + i], lambda a, i: cr[4 * a + 2 * b + i]) for b in (0, 1)
    ]
    rim = rim_of(lambda i: zr[i], lambda a, i: hr[2 * a + i])
    rim = lift_rows(rim, rim_rows[1], rim_rows[0])
    level_thresh = thresh(0)
    inner = (lane % (2 * s) == 0) & (iota((n, LANES), 0) % 2 == 0)

    def plane_step(x, v):
        v = lift_rows(v, yl[1, x : x + 1, :], yl[0, x : x + 1, :])
        v = lift_lanes(v, roll(rim, LANES - s - 2 * s * x, 1), s)
        work[x] = v
        if x % 2 == 0:
            grown[pl.ds(x // 2 * (n // 2), n // 2), :] = work[x, pl.ds(0, n // 2, stride=2), :]

    def finish():
        energy = kept = jnp.zeros((n, LANES), jnp.float32)
        for x in range(px):
            v = work[x]
            small = shrink(v, level_thresh)
            if x % 2 == 0:
                energy += jnp.where(inner, 0.0, v * v)
                kept += jnp.where(inner, 0.0, jnp.abs(small))
            else:
                energy += v * v
                kept += jnp.abs(small)
            out[0, x] = small
        return [total(energy), total(kept)]

    even = src[0]
    before = xr[1] - 0.5 * even
    for k in range(px // 2):
        after = src[2 * k + 2] if 2 * k + 2 < px else xr[0]
        detail = src[2 * k + 1] - 0.5 * (even + after)
        smooth = even + 0.25 * (before + detail)
        plane_step(2 * k, smooth)
        plane_step(2 * k + 1, detail)
        even, before = after, detail

    ax, ay = px // 2, n // 2
    own = ax * ay
    send_rows, rows1, rows2, send_lanes, lanes1, rim1, lanes2 = tables
    for load in loads[2 : 2 + TABLES]:
        load.wait()
    here = grown[0:own]
    halo = mix_rows(send_rows[...], here)
    sent[...] = halo
    edges = sum(
        mix(send_lanes[...], part, ((1,), (1,)))
        for part in three(jnp.concatenate((here, halo), axis=0))
    )
    extra = halo.shape[0]
    for g in (0, 1):
        side[g, :, pl.ds(own, 2 * LANES)] = jnp.zeros((2, 2 * LANES), jnp.float32)
        side[g, :, pl.ds(0, own + extra)] = edges[2 * g : 2 * g + 2]

    step_to = (1, -1)
    px_rows, py_rows = 4 * ay, 4 * ax
    copies = []
    for g in (0, 1):
        dz = step_to[g]
        tail = pl.ds(own + LANES, LANES)
        for gy in (0, 1):
            for gx in ways:
                copies.append((side.at[g, :, tail], t3r.at[g, gy, gx], (step_to[gx], step_to[gy], dz)))
        middle = pl.ds(own, LANES)
        for gx in ways:
            copies.append((side.at[g, :, middle], t2r.at[g, gx], (step_to[gx], 0, dz)))
        for gy in (0, 1):
            copies.append((side.at[g, :, middle], t2r.at[g, 2 + gy], (0, step_to[gy], dz)))
        copies.append((side.at[g, :, pl.ds(0, own)], hz.at[g, :, pl.ds(0, own)], (0, 0, dz)))

    def rows_copy(start, size, to):
        copies.append((sent.at[pl.ds(start, size)], grown.at[pl.ds(own + start, size)], to))

    parts = len(ways)
    for gy in (0, 1):
        for gx in ways:
            rows_copy(px_rows + py_rows + 8 * gy + 4 * gx, 8 // parts, (step_to[gx], step_to[gy], 0))
    for gx in ways:
        rows_copy(px_rows // 2 * gx, px_rows // parts, (step_to[gx], 0, 0))
    for gy in (0, 1):
        rows_copy(px_rows + py_rows // 2 * gy, py_rows // 2, (0, step_to[gy], 0))
    flights = [
        pltpu.make_async_remote_copy(
            src_ref=f, dst_ref=t, send_sem=m_send.at[i], recv_sem=m_recv.at[i],
            device_id=device(*d), device_id_type=MESH,
        )
        for i, (f, t, d) in enumerate(copies)
    ]
    for flight in flights:
        flight.start()
    sums = finish()
    for flight in flights:
        flight.wait()

    lane2 = iota((2, LANES), 1)
    for g in (0, 1):
        v = jnp.where(lane2 < px_rows // 2, t2r[g, 0], t2r[g, 0 if alone else 1])
        v = jnp.where(lane2 < px_rows, v, jnp.where(lane2 < px_rows + py_rows // 2, t2r[g, 2], t2r[g, 3]))
        hz[g, :, pl.ds(own, LANES)] = v
        u = []
        for gy in (0, 1):
            u.append(jnp.where(lane2 % 8 < 4, t3r[g, gy, 0], t3r[g, gy, 0 if alone else 1]))
        v = jnp.where(lane2 < 8, u[0], u[1])
        hz[g, :, pl.ds(own + LANES, LANES)] = jnp.where(lane2 < 16, v, 0.0)
    pieces = []
    for part in three(jnp.concatenate((hz[0], hz[1]), axis=0)):
        pieces.append(part.astype(jnp.float32))
    pieces.append(jnp.zeros_like(pieces[0]))
    rim_rows = mix(jnp.concatenate(pieces, axis=0).astype(jnp.bfloat16), rim1[...], ((0,), (0,)))
    wide = mix_lanes(grown[...], lanes1[...]) + rim_rows[0 : own + extra]
    first = mix_rows(rows1[...], wide)
    second = mix_lanes(mix_rows(rows2[...], first), lanes2[...])
    o1s[...] = first[0:own]
    o2s[...] = second.reshape(o2s.shape)

    def tally(v, level, ny):
        s = 2**level
        row, at = iota(v.shape, 0), iota(v.shape, 1)
        smooth = ((row // ny) % 2 == 0) & (row % 2 == 0) & (at % (2 * s) == 0)
        use = (at % s == 0) & ~smooth
        small = shrink(v, thresh(level))
        return [total(jnp.where(use, v * v, 0.0)), total(jnp.where(use, jnp.abs(small), 0.0))]

    sums += tally(first[0:own], 1, ay) + tally(second, 2, ay // 2)

    def place(source, level):
        s = 2**level
        small_y = ay >> (level - 1)
        keep = iota((small_y, LANES), 1) % s == 0
        for x in range(ax >> (level - 1)):
            spot = (0, s * x, pl.ds(0, small_y, stride=s), slice(None))
            out[spot] = jnp.where(keep, shrink(source(x), thresh(level)), out[spot])

    cx, cy = ax // 4, ay // 4
    step = 2**FINE
    count = cx * cy
    for x in range(cx):
        rows_s[pl.ds(x * cy, cy), :] = o2s[2 * x, pl.ds(0, cy, stride=2), :]
    here = rows_s[...]
    lane = iota((count, LANES), 1)
    row = iota((count, LANES), 0)
    here = jnp.where(lane % step == 0, here, 0.0)
    for bit in (1, 2, 4):
        here = jnp.where((row & bit) != 0, roll(here, bit, 1), here)
    groups = count // 8
    one = iota((1, LANES), 1)
    for g in range(groups):
        msg[g : g + 1] = jnp.sum(here[8 * g : 8 * g + 8], axis=0, keepdims=True)
    tail = jnp.zeros((1, LANES), jnp.float32)
    for i, whole in enumerate(sums):
        tail = jnp.where(one == i, whole, tail)
    msg[groups:] = jnp.broadcast_to(tail, (msg.shape[0] - groups, LANES))
    flat = (me[0] * ny + me[1]) * nz + me[2]

    def post(j):
        return pltpu.make_async_remote_copy(
            src_ref=msg, dst_ref=gath.at[flat], send_sem=g_send.at[j], recv_sem=g_recv.at[j],
            device_id=device(*split(j)), device_id_type=MESH,
        )

    def send(j, carry):
        post(ndev - j).start()
        return carry

    def settle(j, carry):
        post(j).wait()
        return carry

    def place_all():
        place(lambda x: o1s[pl.ds(x * ay, ay), :], 1)
        place(lambda x: o2s[x], 2)

    if ndev <= 32:
        posts = [post(ndev - j) for j in range(1, ndev)]
        for flight in posts:
            flight.start()
        gath[flat] = msg[...]
        place_all()
        for flight in posts:
            flight.wait()
    else:
        lax.fori_loop(1, ndev, send, 0)
        gath[flat] = msg[...]
        place_all()
        lax.fori_loop(1, ndev, settle, 0)

    sub = iota((8, LANES), 0)
    lane8 = iota((8, LANES), 1)

    def unpack(d, tail):
        for g in range(groups):
            acc = jnp.zeros((8, LANES), jnp.float32)
            for z in range(nz):
                v = jnp.broadcast_to(gath[d * nz + z, g : g + 1, :], (8, LANES))
                for bit in (1, 2, 4):
                    v = jnp.where((sub & bit) != 0, roll(v, -bit, 1), v)
                acc += roll(jnp.where(lane8 % step == 0, v, 0.0), z, 1)
            final_s[pl.ds(pl.multiple_of(d * count + 8 * g, 8), 8), :] = acc
        for z in range(nz):
            tail += gath[d * nz + z, groups : groups + 1, :]
        return tail

    tail = lax.fori_loop(0, nx * ny, unpack, jnp.zeros((1, LANES), jnp.float32), unroll=nx * ny <= 8)

    def dot(a, b):
        return jnp.dot(a, b, precision=lax.Precision.HIGHEST, preferred_element_type=jnp.float32)

    grid = final_s[...]
    loads[2 + TABLES].wait()
    loads[3 + TABLES].wait()
    half3, half4 = dot(k_s[0], grid), dot(k_s[1], grid)
    grid, grid4 = dot(half3, l_s[0]), dot(half4, l_s[1])
    row = iota(grid.shape, 0)
    lane = iota(grid.shape, 1)
    inner_row = row % count
    gx, gy, gz = inner_row // cy, inner_row % cy, lane // step
    valid = lane % step < nz
    even3 = (gx % 2 == 0) & (gy % 2 == 0) & (gz % 2 == 0)
    even4 = (gx % 4 == 0) & (gy % 4 == 0) & (gz % 4 == 0)
    det3 = valid & ~even3
    det4 = valid & even3 & ~even4
    small3 = shrink(grid, thresh(FINE))
    small4 = shrink(grid4, thresh(FINE + 1))
    final_s[...] = jnp.where(even3, jnp.where(even4, grid4, small4), small3)

    def masked(mask, v):
        return total(jnp.where(mask, v, 0.0))

    coarse = ((masked(det3, grid * grid), masked(det3, jnp.abs(small3))),
              (masked(det4, grid4 * grid4), masked(det4, jnp.abs(small4))))
    for q in (0, 1):
        line = jnp.zeros((1, LANES), jnp.float32)
        for level in range(LEVELS):
            weight = 8.0 ** (level + 1) / (7.0 * cells)
            if level < FINE:
                value = jnp.sum(jnp.where(one == 2 * level + q, tail, 0.0), axis=1, keepdims=True)
            else:
                value = coarse[level - FINE][q]
            line = jnp.where(one == level, value * weight, line)
        stats[q] = line[:, 0:LEVELS]

    first = pl.multiple_of((me[0] * ny + me[1]) * count, count)
    mine = pltpu.roll(final_s[pl.ds(first, count), :], lax.rem(LANES - me[2], LANES), 1)
    rows_s[...] = mine
    keep = iota((cy, LANES), 1) % step == 0
    for x in range(cx):
        spot = (0, step * x, pl.ds(0, cy, stride=step), slice(None))
        out[spot] = jnp.where(keep, rows_s[pl.ds(x * cy, cy), :], out[spot])


def deliver(held, held_stats, out, stats, sem):
    rows = held.shape[1] // CHUNKS
    copies = [pltpu.make_async_copy(held_stats, stats, sem.at[CHUNKS])]
    for i in range(CHUNKS):
        part = pl.ds(i * rows, rows)
        copies.append(pltpu.make_async_copy(held.at[:, part], out.at[:, part], sem.at[i]))
    for copy in copies:
        copy.start()
    for copy in copies:
        copy.wait()


def shards(sizes, fields, exponents):
    nx, ny, nz = sizes
    ndev = nx * ny * nz
    _, lx, ly, lz = fields.shape
    cells = fields.size * ndev
    step = 2**FINE
    coarse = (lx // step, ly // step, lz // step)
    count = coarse[0] * coarse[1]
    tables = coarse_matrices(sizes, coarse)
    middle = middle_tables(lx // 2, ly // 2, lz // 2)
    own, extra = lx // 2 * (ly // 2), middle[0].shape[0]
    scratch = [
        *(pltpu.VMEM(shape, jnp.float32) for shape in (
            (2, ly, LANES), (2, ly, LANES), (2, lx, LANES), (2, lx, LANES), (4, 1, LANES), (4, 1, LANES),
            (2, lx, LANES), (ly, LANES), (2, ly, LANES), (ly, LANES), (4, ly, LANES), (2, 1, LANES),
            (4, 1, LANES), (2, 1, LANES), (8, 1, LANES), (lx, ly, LANES),
        )),
        pltpu.SemaphoreType.DMA((26,)),
        pltpu.SemaphoreType.DMA((26,)),
        *(pltpu.VMEM(shape, jnp.float32) for shape in (
            (own + extra, LANES), (extra, LANES), (1, LANES), (2, 2, own + 2 * LANES), (2, 2, own + 2 * LANES),
            (2, 4, 2, LANES), (2, 2, 2, 2, LANES), (own, LANES), (lx // 4, ly // 4, LANES),
        )),
        pltpu.SemaphoreType.DMA((26,)),
        pltpu.SemaphoreType.DMA((26,)),
    ]
    height = -(-(count // 8 + 1) // 4) * 4
    scratch += [
        pltpu.VMEM((ndev, height, LANES), jnp.float32),
        pltpu.VMEM((height, LANES), jnp.float32),
        pltpu.VMEM((count, LANES), jnp.float32),
        pltpu.VMEM((nx * ny * count, LANES), jnp.float32),
        pltpu.SemaphoreType.DMA((ndev,)),
        pltpu.SemaphoreType.DMA((ndev,)),
        pltpu.VMEM(fields.shape, jnp.float32),
        pltpu.SMEM(exponents.shape, jnp.int32),
        pltpu.VMEM(tables[0].shape, jnp.float32),
        pltpu.VMEM(tables[1].shape, jnp.float32),
        pltpu.SemaphoreType.DMA((4 + TABLES,)),
        *(pltpu.VMEM(table.shape, table.dtype) for table in middle),
    ]
    vmem = pl.BlockSpec(memory_space=pltpu.VMEM)
    held = pl.pallas_call(
        functools.partial(kernel, sizes, cells),
        out_shape=(
            pltpu.VMEM(fields.shape, jnp.float32),
            pltpu.VMEM((2, 1, LEVELS), jnp.float32),
        ),
        in_specs=[pl.BlockSpec(memory_space=pltpu.HBM)] * (4 + TABLES),
        out_specs=(vmem, vmem),
        scratch_shapes=scratch,
        compiler_params=pltpu.CompilerParams(
            collective_id=0, has_side_effects=True, vmem_limit_bytes=VMEM_LIMIT
        ),
    )(*(pltpu.with_memory_space_constraint(x, pltpu.HBM) for x in (exponents, fields, *map(jnp.asarray, (*tables, *middle)))))
    hbm = pl.BlockSpec(memory_space=pltpu.HBM)
    return pl.pallas_call(
        deliver,
        out_shape=(
            jax.ShapeDtypeStruct(fields.shape, jnp.float32),
            jax.ShapeDtypeStruct((2, 1, LEVELS), jnp.float32),
        ),
        in_specs=(vmem, vmem),
        out_specs=(hbm, hbm),
        scratch_shapes=[pltpu.SemaphoreType.DMA((CHUNKS + 1,))],
    )(*(pltpu.with_memory_space_constraint(x, pltpu.VMEM) for x in held))


def solution(mesh):
    sizes = tuple(mesh.shape[name] for name in ("gx", "gy", "gz"))
    placed = (P(None, "gx", "gy", "gz"), P())
    return jax.shard_map(
        functools.partial(shards, sizes),
        mesh=mesh,
        in_specs=placed,
        out_specs=placed,
        check_vma=False,
    )
```

```python
import functools

import numpy as np

import jax
import jax.numpy as jnp
from jax import lax
from jax.experimental import pallas as pl
from jax.experimental.pallas import tpu as pltpu
from jax.sharding import PartitionSpec as P

FINE = 3
LEVELS = 5
LANES = 128
CHUNKS = 4
BUFFERS = 18
TABLES = 7
ROUNDS = 2
VMEM_LIMIT = 33_554_432
MESH = pl.DeviceIdType.MESH


def periodic_lift(length):
    eye = np.eye(length)
    even, odd = eye[0::2], eye[1::2]
    detail = odd - 0.5 * (even + np.roll(even, -1, 0))
    smooth = even + 0.25 * (np.roll(detail, 1, 0) + detail)
    whole = np.zeros((length, length))
    whole[0::2] = smooth
    whole[1::2] = detail
    return whole


def second_lift(length):
    whole = np.zeros((length, length))
    whole[0::2, 0::2] = periodic_lift(length // 2)
    return whole


def coarse_matrices(sizes, coarse):
    nx, ny, nz = sizes
    cx, cy, cz = coarse
    rows = np.arange(nx * ny * cx * cy)
    dev, inner = rows // (cx * cy), rows % (cx * cy)
    gx = (dev // ny) * cx + inner // cy
    gy = (dev % ny) * cy + inner % cy
    step = LANES // cz
    lanes = np.array([z * step + d for d in range(nz) for z in range(cz)])
    order = np.arange(nx * ny * cx * cy).reshape(nx * ny, -1, 8).transpose(2, 1, 0).reshape(-1)
    result = []
    for both_levels in (False, True):
        mx, my, mz = periodic_lift(nx * cx), periodic_lift(ny * cy), periodic_lift(nz * cz)
        if both_levels:
            mx, my, mz = second_lift(nx * cx) @ mx, second_lift(ny * cy) @ my, second_lift(nz * cz) @ mz
        both = mx[gx[:, None], gx[None]] * my[gy[:, None], gy[None]]
        along = np.zeros((LANES, LANES))
        along[np.ix_(lanes, lanes)] = mz.T
        result.append((both[:, order].astype(np.float32), along.astype(np.float32)))
    return [np.stack(pair) for pair in zip(*result)]


def lift_line(n):
    whole = np.zeros((n, n + 2))
    cells = np.eye(n + 2)
    even, odd = cells[0:n:2], cells[1:n:2]
    after = np.concatenate((even[1:], cells[n + 1 :]))
    detail = odd - 0.5 * (even + after)
    before = np.concatenate((cells[n : n + 1] - 0.5 * even[:1], detail[:-1]))
    whole[0::2] = even + 0.25 * (before + detail)
    whole[1::2] = detail
    return whole

def line_tables(n):
    lift = lift_line(n)
    own = lift[:, :n]
    sent = np.zeros((4, n))
    sent[0, n - 1], sent[0, n - 2] = 1.0, -0.5
    sent[1] = own[n - 2] - 0.5 * own[n - 4]
    sent[2, 0] = 1.0
    sent[3] = own[0]
    first = np.zeros((n + 2, n + 4))
    first[:n, :n] = own
    first[:n, n], first[:n, n + 2] = lift[:, n], lift[:, n + 1]
    first[n, n + 1], first[n, 0] = 1.0, lift[n - 2, n + 1]
    first[n + 1, n + 3] = 1.0
    first[n + 1, :n] = lift[0, n] * sent[0]
    return sent, first, lift_line(n // 2)


def middle_tables(ax, ay, az):
    step = LANES // az
    sent_x, first_x, second_x = line_tables(ax)
    sent_y, first_y, second_y = line_tables(ay)
    sent_z, first_z, second_z = line_tables(az)
    own = [(x, y) for x in range(ax) for y in range(ay)]
    corners = [(x, 2 * g + y) for g in range(2) for x in range(4) for y in range(2)]
    extra = [(ax + k, y) for k in range(4) for y in range(ay)]
    extra += [(x, ay + k) for k in range(4) for x in range(ax)]
    extra += [(ax + x, ay + y) for x, y in corners]
    taken = np.array(own + extra)
    given = own + [(ax + k, y) for k in range(2) for y in range(0, ay, 2)]
    given += [(x, ay + k) for k in range(2) for x in range(0, ax, 2)]
    given += [(ax + x, ay + y) for x in range(2) for y in range(2)]
    height = -(-len(given) // 16) * 16

    whole_x, whole_y = np.concatenate((np.eye(ax), sent_x)), np.concatenate((np.eye(ay), sent_y))
    ex, ey = np.array(extra).T
    ox, oy = np.array(own).T
    send_rows = whole_x[np.ix_(ex, ox)] * whole_y[np.ix_(ey, oy)]
    gx, gy = np.array(given).T
    tx, ty = taken.T
    rows = np.zeros((height, len(taken)))
    rows[: len(given)] = first_x[np.ix_(gx, tx)] * first_y[np.ix_(gy, ty)]

    def spot(at, n):
        return np.where(at >= n, n // 2 + at - n, at // 2)

    half = np.array([(x, y) for x in range(ax // 2) for y in range(ay // 2)])
    use = ((gx % 2 == 0) | (gx >= ax)) & ((gy % 2 == 0) | (gy >= ay))
    last = np.zeros((len(half), height))
    pick_x = second_x[np.ix_(half[:, 0], spot(gx, ax))]
    pick_y = second_y[np.ix_(half[:, 1], spot(gy, ay))]
    last[:, : len(given)] = pick_x * pick_y * use

    lanes = np.arange(az) * step
    out = np.concatenate((lanes, [1, step + 1]))
    send_lanes = np.zeros((8, LANES))
    send_lanes[np.ix_(np.arange(4), lanes)] = sent_z
    along = np.zeros((LANES, LANES))
    along[np.ix_(lanes, out)] = first_z[:, :az].T
    rim = np.zeros((16, LANES))
    for part in range(3):
        rim[np.ix_(4 * part + np.arange(4), out)] = first_z[:, az:].T
    along_last = np.zeros((LANES, LANES))
    source = np.concatenate((lanes[0::2], [1, step + 1]))
    along_last[np.ix_(source, lanes[0::2])] = second_z.T
    result = (send_rows, rows, last, send_lanes, along, rim, along_last)
    return tuple(table.astype(jnp.bfloat16) for table in result)


def iota(shape, axis):
    return lax.broadcasted_iota(jnp.int32, shape, axis)


def roll(values, shift, axis):
    return pltpu.roll(values, shift % values.shape[axis], axis)


def lift_rows(v, low, high):
    n = v.shape[0]
    row = iota(v.shape, 0)
    odd = row % 2 == 1
    up = jnp.where(row == n - 1, high, roll(v, -1, 0))
    w = jnp.where(odd, v - 0.5 * (roll(v, 1, 0) + up), v)
    down = jnp.where(row == 0, low - 0.5 * v, roll(w, 1, 0))
    return jnp.where(odd, w, w + 0.25 * (down + roll(w, -1, 0)))


def lift_lanes(v, rim, s):
    lane = iota(v.shape, 1)
    up = jnp.where(lane == LANES - s, rim, roll(v, -s, 1))
    w = jnp.where(lane % (2 * s) == s, v - 0.5 * (roll(v, s, 1) + up), v)
    down = jnp.where(lane == 0, rim - 0.5 * v, roll(w, s, 1))
    return jnp.where(lane % (2 * s) == 0, w + 0.25 * (down + roll(w, -s, 1)), w)


def shrink(v, thresh):
    return v - jnp.clip(v, -thresh, thresh)


def three(v):
    parts = []
    for _ in range(3):
        parts.append(v.astype(jnp.bfloat16))
        v = v - parts[-1].astype(jnp.float32)
    return parts


def mix(a, b, dims):
    return lax.dot_general(a, b, (dims, ((), ())), preferred_element_type=jnp.float32)


def mix_rows(table, v):
    wide = mix(table, jnp.concatenate(three(v), axis=1), ((1,), (0,)))
    return wide[:, :LANES] + wide[:, LANES : 2 * LANES] + wide[:, 2 * LANES :]


def mix_lanes(v, table):
    return mix(jnp.concatenate(three(v), axis=1), jnp.concatenate([table] * 3, axis=0), ((1,), (0,)))


def total(v):
    return jnp.sum(jnp.sum(v, axis=0, keepdims=True), axis=1, keepdims=True)


def kernel(sizes, cells, exps_in, field_in, rows_in, lanes_in, *rest):
    tables_in, (out, stats), scratch = rest[:TABLES], rest[TABLES : TABLES + 2], rest[TABLES + 2 :]
    nx, ny, nz = sizes
    ndev = nx * ny * nz
    scratch = list(scratch)
    tables = scratch[-TABLES:]
    scratch = scratch[:-TABLES]
    field, exps, k_s, l_s, in_sem = scratch[-5:]
    scratch = scratch[:-5]
    pairs = [(field_in, field), (exps_in, exps), *zip(tables_in, tables), (rows_in, k_s), (lanes_in, l_s)]
    loads = [pltpu.make_async_copy(a, b, in_sem.at[i]) for i, (a, b) in enumerate(pairs)]
    for load in loads:
        load.start()
    me = (lax.axis_index("gx"), lax.axis_index("gy"), lax.axis_index("gz"))

    def device(dx, dy, dz):
        return (
            lax.rem(me[0] + (dx + nx), nx),
            lax.rem(me[1] + (dy + ny), ny),
            lax.rem(me[2] + (dz + nz), nz),
        )

    def thresh(level):
        return jnp.exp2(jnp.full((1, LANES), exps[level].astype(jnp.float32)))

    def split(j):
        return j // (ny * nz), (j // nz) % ny, j % nz

    def launch(copies, send_sem, recv_sem):
        flights = [
            pltpu.make_async_remote_copy(
                src_ref=f, dst_ref=t, send_sem=send_sem, recv_sem=recv_sem,
                device_id=device(*d), device_id_type=MESH,
            )
            for f, t, d in copies
        ]
        for flight in flights:
            flight.start()
        return sum(t.size for _, t, _ in copies) // LANES

    def settle(span, send_sem, recv_sem):
        for sem in (recv_sem, send_sem):
            pltpu.make_async_copy(span, span, sem).wait()

    barrier = pltpu.get_barrier_semaphore()

    near = max(sizes) // 2 <= ROUNDS
    greeted = {
        tuple((d + size - 1) % size if near else d for d, size in zip(spot, sizes))
        for spot in np.ndindex(*(3, 3, 3) if near else sizes)
    } - {(0, 0, 0)}
    for spot in sorted(greeted):
        pl.semaphore_signal(barrier, inc=1, device_id=device(*spot), device_id_type=MESH)
    gath, msg, rows_s, final_s, g_send, g_recv = scratch[-6:]
    loads[0].wait()
    loads[1].wait()
    away = (-1, 1)
    alone = nx == 2

    (xs, xr, ys, yr, es, er, yl, zs, zr, hs, hr, ds, dr, cs, cr, work, send_sem, recv_sem) = scratch[:BUFFERS]
    grown, sent, side, hz, t2r, t3r, o1s, o2s, m_send, m_recv = scratch[BUFFERS : BUFFERS + 10]
    s = 1
    n = field.shape[2] // s
    px = field.shape[1] // s
    src = field.at[0]
    lane = iota((n, LANES), 1)

    def edge(v):
        return v[0:1], v[n - 1 : n] - 0.5 * v[n - 2 : n - 1]

    e_plane = src[0]
    p_plane = src[px - 1] - 0.5 * src[px - 2]
    xs[0] = e_plane
    xs[1] = p_plane
    ys[0] = src[:, 0, :]
    ys[1] = src[:, n - 1, :] - 0.5 * src[:, n - 2, :]
    for a, plane in ((0, e_plane), (1, p_plane)):
        es[2 * a], es[2 * a + 1] = edge(plane)

    packed = jnp.zeros((n, LANES), jnp.float32)
    for x in range(px):
        v = src[x]
        u = jnp.where(lane == LANES - s, v - 0.5 * roll(v, s, 1), v)
        at = 2 * s * x
        packed = jnp.where((lane == at) | (lane == at + s), roll(u, at + s, 1), packed)
    half = 2 * s * px
    combined = packed - 0.5 * roll(packed, 2 * s, 1)
    sides = roll(jnp.where(lane < half // 2, packed, combined), half, 1)
    zs[...] = packed
    hs[...] = sides
    ds[0], ds[1] = edge(packed)
    cs[0], cs[1] = edge(sides)

    pl.semaphore_wait(barrier, len(greeted))
    copies = []
    ways = (0,) if alone else (0, 1)
    for i in (0, 1):
        for b in (0, 1):
            for a in ways:
                copies.append((cs.at[b], cr.at[4 * a + 2 * b + i], (away[a], away[b], away[i])))
            copies.append((ds.at[b], dr.at[2 * b + i], (0, away[b], away[i])))
    for a in (0, 1):
        for b in (0, 1):
            copies.append((es.at[2 * a + b], er.at[2 * a + b], (away[a], away[b], 0)))
    for b in (0, 1):
        copies.append((ys.at[b], yr.at[b], (0, away[b], 0)))
    for i in (0, 1):
        for a in ways:
            copies.append((hs, hr.at[2 * a + i], (away[a], 0, away[i])))
    for a in (0, 1):
        copies.append((xs.at[a], xr.at[a], (away[a], 0, 0)))
    for i in (0, 1):
        copies.append((zs, zr.at[i], (0, 0, away[i])))
    sent_rows = launch(copies, send_sem, recv_sem)
    settle(grown.at[pl.ds(0, sent_rows)], send_sem, recv_sem)

    for b in (0, 1):
        yl[b] = lift_rows(yr[b], er[2 + b], er[b])

    def rim_of(main, side):
        spot = iota(main(0).shape, 1)
        parts = []
        for i in (0, 1):
            after = side(0, i)
            before = after if alone else side(1, i)
            v = jnp.where(spot < half, main(i), 0.0)
            v = jnp.where((spot >= half) & (spot < half + 2 * s), after, v)
            parts.append(jnp.where(spot >= LANES - 2 * s, before, v))
        v = jnp.where(spot % (2 * s) < s, roll(parts[0], -s, 1), roll(parts[1], s, 1))
        odd = (spot // (2 * s)) % 2 == 1
        w = jnp.where(odd, v - 0.5 * (roll(v, 2 * s, 1) + roll(v, -2 * s, 1)), v)
        return jnp.where(odd, w, w + 0.25 * (roll(w, 2 * s, 1) + roll(w, -2 * s, 1)))

    rim_rows = [
        rim_of(lambda i: dr[2 * b + i], lambda a, i: cr[4 * a + 2 * b + i]) for b in (0, 1)
    ]
    rim = rim_of(lambda i: zr[i], lambda a, i: hr[2 * a + i])
    rim = lift_rows(rim, rim_rows[1], rim_rows[0])
    level_thresh = thresh(0)
    inner = (lane % (2 * s) == 0) & (iota((n, LANES), 0) % 2 == 0)

    def plane_step(x, v):
        v = lift_rows(v, yl[1, x : x + 1, :], yl[0, x : x + 1, :])
        v = lift_lanes(v, roll(rim, LANES - s - 2 * s * x, 1), s)
        work[x] = v
        if x % 2 == 0:
            grown[pl.ds(x // 2 * (n // 2), n // 2), :] = work[x, pl.ds(0, n // 2, stride=2), :]

    def finish():
        energy = kept = jnp.zeros((n, LANES), jnp.float32)
        for x in range(px):
            v = work[x]
            small = shrink(v, level_thresh)
            if x % 2 == 0:
                energy += jnp.where(inner, 0.0, v * v)
                kept += jnp.where(inner, 0.0, jnp.abs(small))
            else:
                energy += v * v
                kept += jnp.abs(small)
            out[0, x] = small
        return [total(energy), total(kept)]

    even = src[0]
    before = xr[1] - 0.5 * even
    for k in range(px // 2):
        after = src[2 * k + 2] if 2 * k + 2 < px else xr[0]
        detail = src[2 * k + 1] - 0.5 * (even + after)
        smooth = even + 0.25 * (before + detail)
        plane_step(2 * k, smooth)
        plane_step(2 * k + 1, detail)
        even, before = after, detail

    ax, ay = px // 2, n // 2
    own = ax * ay
    send_rows, rows1, rows2, send_lanes, lanes1, rim1, lanes2 = tables
    for load in loads[2 : 2 + TABLES]:
        load.wait()
    here = grown[0:own]
    halo = mix_rows(send_rows[...], here)
    sent[...] = halo
    edges = sum(
        mix(send_lanes[...], part, ((1,), (1,)))
        for part in three(jnp.concatenate((here, halo), axis=0))
    )
    extra = halo.shape[0]
    for g in (0, 1):
        side[g, :, pl.ds(own, 2 * LANES)] = jnp.zeros((2, 2 * LANES), jnp.float32)
        side[g, :, pl.ds(0, own + extra)] = edges[2 * g : 2 * g + 2]

    step_to = (1, -1)
    px_rows, py_rows = 4 * ay, 4 * ax
    copies = []
    for g in (0, 1):
        dz = step_to[g]
        tail = pl.ds(own + LANES, LANES)
        for gy in (0, 1):
            for gx in ways:
                copies.append((side.at[g, :, tail], t3r.at[g, gy, gx], (step_to[gx], step_to[gy], dz)))
        middle = pl.ds(own, LANES)
        for gx in ways:
            copies.append((side.at[g, :, middle], t2r.at[g, gx], (step_to[gx], 0, dz)))
        for gy in (0, 1):
            copies.append((side.at[g, :, middle], t2r.at[g, 2 + gy], (0, step_to[gy], dz)))
        copies.append((side.at[g, :, pl.ds(0, own)], hz.at[g, :, pl.ds(0, own)], (0, 0, dz)))

    def rows_copy(start, size, to):
        copies.append((sent.at[pl.ds(start, size)], grown.at[pl.ds(own + start, size)], to))

    parts = len(ways)
    for gy in (0, 1):
        for gx in ways:
            rows_copy(px_rows + py_rows + 8 * gy + 4 * gx, 8 // parts, (step_to[gx], step_to[gy], 0))
    for gx in ways:
        rows_copy(px_rows // 2 * gx, px_rows // parts, (step_to[gx], 0, 0))
    for gy in (0, 1):
        rows_copy(px_rows + py_rows // 2 * gy, py_rows // 2, (0, step_to[gy], 0))
    sent_rows = launch(copies, m_send, m_recv)
    sums = finish()
    settle(grown.at[pl.ds(0, sent_rows)], m_send, m_recv)

    lane2 = iota((2, LANES), 1)
    for g in (0, 1):
        v = jnp.where(lane2 < px_rows // 2, t2r[g, 0], t2r[g, 0 if alone else 1])
        v = jnp.where(lane2 < px_rows, v, jnp.where(lane2 < px_rows + py_rows // 2, t2r[g, 2], t2r[g, 3]))
        hz[g, :, pl.ds(own, LANES)] = v
        u = []
        for gy in (0, 1):
            u.append(jnp.where(lane2 % 8 < 4, t3r[g, gy, 0], t3r[g, gy, 0 if alone else 1]))
        v = jnp.where(lane2 < 8, u[0], u[1])
        hz[g, :, pl.ds(own + LANES, LANES)] = jnp.where(lane2 < 16, v, 0.0)
    pieces = []
    for part in three(jnp.concatenate((hz[0], hz[1]), axis=0)):
        pieces.append(part.astype(jnp.float32))
    pieces.append(jnp.zeros_like(pieces[0]))
    rim_rows = mix(jnp.concatenate(pieces, axis=0).astype(jnp.bfloat16), rim1[...], ((0,), (0,)))
    wide = mix_lanes(grown[...], lanes1[...]) + rim_rows[0 : own + extra]
    first = mix_rows(rows1[...], wide)
    second = mix_lanes(mix_rows(rows2[...], first), lanes2[...])
    o1s[...] = first[0:own]
    o2s[...] = second.reshape(o2s.shape)

    def tally(v, level, ny):
        s = 2**level
        row, at = iota(v.shape, 0), iota(v.shape, 1)
        smooth = ((row // ny) % 2 == 0) & (row % 2 == 0) & (at % (2 * s) == 0)
        use = (at % s == 0) & ~smooth
        small = shrink(v, thresh(level))
        return [total(jnp.where(use, v * v, 0.0)), total(jnp.where(use, jnp.abs(small), 0.0))]

    sums += tally(first[0:own], 1, ay) + tally(second, 2, ay // 2)

    def place(source, level):
        s = 2**level
        small_y = ay >> (level - 1)
        keep = iota((small_y, LANES), 1) % s == 0
        for x in range(ax >> (level - 1)):
            spot = (0, s * x, pl.ds(0, small_y, stride=s), slice(None))
            out[spot] = jnp.where(keep, shrink(source(x), thresh(level)), out[spot])

    cx, cy = ax // 4, ay // 4
    step = 2**FINE
    count = cx * cy
    for x in range(cx):
        rows_s[pl.ds(x * cy, cy), :] = o2s[2 * x, pl.ds(0, cy, stride=2), :]
    here = rows_s[...]
    lane = iota((count, LANES), 1)
    row = iota((count, LANES), 0)
    here = jnp.where(lane % step == 0, here, 0.0)
    for bit in (1, 2, 4):
        here = jnp.where((row & bit) != 0, roll(here, bit, 1), here)
    groups = count // 8
    one = iota((1, LANES), 1)
    for g in range(groups):
        msg[g : g + 1] = jnp.sum(here[8 * g : 8 * g + 8], axis=0, keepdims=True)
    tail = jnp.zeros((1, LANES), jnp.float32)
    for i, whole in enumerate(sums):
        tail = jnp.where(one == i, whole, tail)
    msg[groups:] = jnp.broadcast_to(tail, (msg.shape[0] - groups, LANES))

    slot = (me[2] * nx + me[0]) * ny + me[1]

    def post(j):
        return pltpu.make_async_remote_copy(
            src_ref=msg, dst_ref=gath.at[slot], send_sem=g_send, recv_sem=g_recv,
            device_id=device(*split(j)), device_id_type=MESH,
        )

    def send(j, carry):
        post(ndev - j).start()
        return carry

    if ndev <= 32:
        for j in range(1, ndev):
            post(ndev - j).start()
    else:
        lax.fori_loop(1, ndev, send, 0)
    gath[slot] = msg[...]
    place(lambda x: o1s[pl.ds(x * ay, ay), :], 1)
    place(lambda x: o2s[x], 2)
    settle(gath.at[pl.ds(0, ndev - 1)], g_send, g_recv)

    spots = nx * ny
    at = iota((spots, LANES), 1) % step
    tail = jnp.zeros((1, LANES), jnp.float32)
    for g in range(groups):
        boxes = [gath[pl.ds(z * spots, spots), g, :] for z in range(nz)]
        for bit in range(8):
            v = jnp.zeros((spots, LANES), jnp.float32)
            for z in range(nz):
                v = jnp.where(at == z, roll(boxes[z], z - bit, 1), v)
            final_s[pl.ds((bit * groups + g) * spots, spots), :] = v
    tail = jnp.sum(gath[:, groups, :], axis=0, keepdims=True)

    def dot(a, b):
        return jnp.dot(a, b, precision=lax.Precision.HIGHEST, preferred_element_type=jnp.float32)

    grid = final_s[...]
    loads[2 + TABLES].wait()
    loads[3 + TABLES].wait()
    half3, half4 = dot(k_s[0], grid), dot(k_s[1], grid)
    grid, grid4 = dot(half3, l_s[0]), dot(half4, l_s[1])
    row = iota(grid.shape, 0)
    lane = iota(grid.shape, 1)
    inner_row = row % count
    gx, gy, gz = inner_row // cy, inner_row % cy, lane // step
    valid = lane % step < nz
    even3 = (gx % 2 == 0) & (gy % 2 == 0) & (gz % 2 == 0)
    even4 = (gx % 4 == 0) & (gy % 4 == 0) & (gz % 4 == 0)
    det3 = valid & ~even3
    det4 = valid & even3 & ~even4
    small3 = shrink(grid, thresh(FINE))
    small4 = shrink(grid4, thresh(FINE + 1))
    final_s[...] = jnp.where(even3, jnp.where(even4, grid4, small4), small3)

    def masked(mask, v):
        return total(jnp.where(mask, v, 0.0))

    coarse = ((masked(det3, grid * grid), masked(det3, jnp.abs(small3))),
              (masked(det4, grid4 * grid4), masked(det4, jnp.abs(small4))))
    for q in (0, 1):
        line = jnp.zeros((1, LANES), jnp.float32)
        for level in range(LEVELS):
            weight = 8.0 ** (level + 1) / (7.0 * cells)
            if level < FINE:
                value = jnp.sum(jnp.where(one == 2 * level + q, tail, 0.0), axis=1, keepdims=True)
            else:
                value = coarse[level - FINE][q]
            line = jnp.where(one == level, value * weight, line)
        stats[q] = line[:, 0:LEVELS]

    first = pl.multiple_of((me[0] * ny + me[1]) * count, count)
    mine = pltpu.roll(final_s[pl.ds(first, count), :], lax.rem(LANES - me[2], LANES), 1)
    rows_s[...] = mine
    keep = iota((cy, LANES), 1) % step == 0
    for x in range(cx):
        spot = (0, step * x, pl.ds(0, cy, stride=step), slice(None))
        out[spot] = jnp.where(keep, rows_s[pl.ds(x * cy, cy), :], out[spot])


def deliver(held, held_stats, out, stats, sem):
    rows = held.shape[1] // CHUNKS
    copies = [pltpu.make_async_copy(held_stats, stats, sem.at[CHUNKS])]
    for i in range(CHUNKS):
        part = pl.ds(i * rows, rows)
        copies.append(pltpu.make_async_copy(held.at[:, part], out.at[:, part], sem.at[i]))
    for copy in copies:
        copy.start()
    for copy in copies:
        copy.wait()


def shards(sizes, fields, exponents):
    nx, ny, nz = sizes
    ndev = nx * ny * nz
    _, lx, ly, lz = fields.shape
    cells = fields.size * ndev
    step = 2**FINE
    coarse = (lx // step, ly // step, lz // step)
    count = coarse[0] * coarse[1]
    tables = coarse_matrices(sizes, coarse)
    middle = middle_tables(lx // 2, ly // 2, lz // 2)
    own, extra = lx // 2 * (ly // 2), middle[0].shape[0]
    scratch = [
        *(pltpu.VMEM(shape, jnp.float32) for shape in (
            (2, ly, LANES), (2, ly, LANES), (2, lx, LANES), (2, lx, LANES), (4, 1, LANES), (4, 1, LANES),
            (2, lx, LANES), (ly, LANES), (2, ly, LANES), (ly, LANES), (4, ly, LANES), (2, 1, LANES),
            (4, 1, LANES), (2, 1, LANES), (8, 1, LANES), (lx, ly, LANES),
        )),
        pltpu.SemaphoreType.DMA,
        pltpu.SemaphoreType.DMA,
        *(pltpu.VMEM(shape, jnp.float32) for shape in (
            (own + extra, LANES), (extra, LANES), (2, 2, own + 2 * LANES), (2, 2, own + 2 * LANES),
            (2, 4, 2, LANES), (2, 2, 2, 2, LANES), (own, LANES), (lx // 4, ly // 4, LANES),
        )),
        pltpu.SemaphoreType.DMA,
        pltpu.SemaphoreType.DMA,
    ]
    height = -(-(count // 8 + 1) // 4) * 4
    scratch += [
        pltpu.VMEM((ndev, height, LANES), jnp.float32),
        pltpu.VMEM((height, LANES), jnp.float32),
        pltpu.VMEM((count, LANES), jnp.float32),
        pltpu.VMEM((nx * ny * count, LANES), jnp.float32),
        pltpu.SemaphoreType.DMA,
        pltpu.SemaphoreType.DMA,
        pltpu.VMEM(fields.shape, jnp.float32),
        pltpu.SMEM(exponents.shape, jnp.int32),
        pltpu.VMEM(tables[0].shape, jnp.float32),
        pltpu.VMEM(tables[1].shape, jnp.float32),
        pltpu.SemaphoreType.DMA((4 + TABLES,)),
        *(pltpu.VMEM(table.shape, table.dtype) for table in middle),
    ]
    vmem = pl.BlockSpec(memory_space=pltpu.VMEM)
    held = pl.pallas_call(
        functools.partial(kernel, sizes, cells),
        out_shape=(
            pltpu.VMEM(fields.shape, jnp.float32),
            pltpu.VMEM((2, 1, LEVELS), jnp.float32),
        ),
        in_specs=[pl.BlockSpec(memory_space=pltpu.HBM)] * (4 + TABLES),
        out_specs=(vmem, vmem),
        scratch_shapes=scratch,
        compiler_params=pltpu.CompilerParams(
            collective_id=0, has_side_effects=True, vmem_limit_bytes=VMEM_LIMIT
        ),
    )(*(pltpu.with_memory_space_constraint(x, pltpu.HBM) for x in (exponents, fields, *map(jnp.asarray, (*tables, *middle)))))
    hbm = pl.BlockSpec(memory_space=pltpu.HBM)
    return pl.pallas_call(
        deliver,
        out_shape=(
            jax.ShapeDtypeStruct(fields.shape, jnp.float32),
            jax.ShapeDtypeStruct((2, 1, LEVELS), jnp.float32),
        ),
        in_specs=(vmem, vmem),
        out_specs=(hbm, hbm),
        scratch_shapes=[pltpu.SemaphoreType.DMA((CHUNKS + 1,))],
    )(*(pltpu.with_memory_space_constraint(x, pltpu.VMEM) for x in held))


def solution(mesh):
    sizes = tuple(mesh.shape[name] for name in ("gx", "gy", "gz"))
    placed = (P(None, "gx", "gy", "gz"), P())
    return jax.shard_map(
        functools.partial(shards, sizes),
        mesh=mesh,
        in_specs=placed,
        out_specs=placed,
        check_vma=False,
    )
```

```python
import functools

import numpy as np

import jax
import jax.numpy as jnp
from jax import lax
from jax.experimental import pallas as pl
from jax.experimental.pallas import tpu as pltpu
from jax.sharding import PartitionSpec as P

FINE = 3
LEVELS = 5
LANES = 128
CHUNKS = 4
BUFFERS = 18
TABLES = 10
BATCH = 8
ROUNDS = 2
VMEM_LIMIT = 33_554_432
MESH = pl.DeviceIdType.MESH


def periodic_lift(length):
    eye = np.eye(length)
    even, odd = eye[0::2], eye[1::2]
    detail = odd - 0.5 * (even + np.roll(even, -1, 0))
    smooth = even + 0.25 * (np.roll(detail, 1, 0) + detail)
    whole = np.zeros((length, length))
    whole[0::2] = smooth
    whole[1::2] = detail
    return whole


def second_lift(length):
    whole = np.zeros((length, length))
    whole[0::2, 0::2] = periodic_lift(length // 2)
    return whole


def coarse_matrices(sizes, coarse):
    nx, ny, nz = sizes
    cx, cy, cz = coarse
    rows = np.arange(nx * ny * cx * cy)
    dev, inner = rows // (cx * cy), rows % (cx * cy)
    gx = (dev // ny) * cx + inner // cy
    gy = (dev % ny) * cy + inner % cy
    step = LANES // cz
    lanes = np.array([z * step + d for d in range(nz) for z in range(cz)])
    order = np.arange(nx * ny * cx * cy).reshape(nx * ny, -1, 8).transpose(2, 1, 0).reshape(-1)
    result = []
    for both_levels in (False, True):
        mx, my, mz = periodic_lift(nx * cx), periodic_lift(ny * cy), periodic_lift(nz * cz)
        if both_levels:
            mx, my, mz = second_lift(nx * cx) @ mx, second_lift(ny * cy) @ my, second_lift(nz * cz) @ mz
        both = mx[gx[:, None], gx[None]] * my[gy[:, None], gy[None]]
        along = np.zeros((LANES, LANES))
        along[np.ix_(lanes, lanes)] = mz.T
        result.append((both[:, order].astype(np.float32), along.astype(np.float32)))
    return [np.stack(pair) for pair in zip(*result)]


def lift_line(n):
    whole = np.zeros((n, n + 2))
    cells = np.eye(n + 2)
    even, odd = cells[0:n:2], cells[1:n:2]
    after = np.concatenate((even[1:], cells[n + 1 :]))
    detail = odd - 0.5 * (even + after)
    before = np.concatenate((cells[n : n + 1] - 0.5 * even[:1], detail[:-1]))
    whole[0::2] = even + 0.25 * (before + detail)
    whole[1::2] = detail
    return whole

def line_tables(n):
    lift = lift_line(n)
    own = lift[:, :n]
    sent = np.zeros((4, n))
    sent[0, n - 1], sent[0, n - 2] = 1.0, -0.5
    sent[1] = own[n - 2] - 0.5 * own[n - 4]
    sent[2, 0] = 1.0
    sent[3] = own[0]
    first = np.zeros((n + 2, n + 4))
    first[:n, :n] = own
    first[:n, n], first[:n, n + 2] = lift[:, n], lift[:, n + 1]
    first[n, n + 1], first[n, 0] = 1.0, lift[n - 2, n + 1]
    first[n + 1, n + 3] = 1.0
    first[n + 1, :n] = lift[0, n] * sent[0]
    return sent, first, lift_line(n // 2)


def fine_tables(px):
    q = LANES // px
    ends = np.zeros((2, px))
    ends[0, px - 1], ends[0, px - 2], ends[1, 0] = 1.0, -0.5, 1.0
    edges = np.zeros((8, LANES))
    place = np.zeros((16, LANES))
    for z in range(2):
        for x in range(2):
            edges[2 * z + x, 1 + z :: q] = ends[x]
            for part in range(3):
                place[4 * part + 2 * z + x, (LANES - q) * x + 1 + z] = 1.0
    result = (lift_line(LANES)[:, :LANES].T, edges, place)
    return tuple(table.astype(jnp.bfloat16) for table in result)


def middle_tables(ax, ay, az):
    step = LANES // az
    sent_x, first_x, second_x = line_tables(ax)
    sent_y, first_y, second_y = line_tables(ay)
    sent_z, first_z, second_z = line_tables(az)
    own = [(x, y) for x in range(ax) for y in range(ay)]
    corners = [(x, 2 * g + y) for g in range(2) for x in range(4) for y in range(2)]
    extra = [(ax + k, y) for k in range(4) for y in range(ay)]
    extra += [(x, ay + k) for k in range(4) for x in range(ax)]
    extra += [(ax + x, ay + y) for x, y in corners]
    taken = np.array(own + extra)
    given = own + [(ax + k, y) for k in range(2) for y in range(0, ay, 2)]
    given += [(x, ay + k) for k in range(2) for x in range(0, ax, 2)]
    given += [(ax + x, ay + y) for x in range(2) for y in range(2)]
    height = -(-len(given) // 16) * 16

    whole_x, whole_y = np.concatenate((np.eye(ax), sent_x)), np.concatenate((np.eye(ay), sent_y))
    ex, ey = np.array(extra).T
    ox, oy = np.array(own).T
    send_rows = whole_x[np.ix_(ex, ox)] * whole_y[np.ix_(ey, oy)]
    gx, gy = np.array(given).T
    tx, ty = taken.T
    rows = np.zeros((height, len(taken)))
    rows[: len(given)] = first_x[np.ix_(gx, tx)] * first_y[np.ix_(gy, ty)]

    def spot(at, n):
        return np.where(at >= n, n // 2 + at - n, at // 2)

    half = np.array([(x, y) for x in range(ax // 2) for y in range(ay // 2)])
    use = ((gx % 2 == 0) | (gx >= ax)) & ((gy % 2 == 0) | (gy >= ay))
    last = np.zeros((len(half), height))
    pick_x = second_x[np.ix_(half[:, 0], spot(gx, ax))]
    pick_y = second_y[np.ix_(half[:, 1], spot(gy, ay))]
    last[:, : len(given)] = pick_x * pick_y * use

    lanes = np.arange(az) * step
    out = np.concatenate((lanes, [1, step + 1]))
    send_lanes = np.zeros((8, LANES))
    send_lanes[np.ix_(np.arange(4), lanes)] = sent_z
    along = np.zeros((LANES, LANES))
    along[np.ix_(lanes, out)] = first_z[:, :az].T
    rim = np.zeros((16, LANES))
    for part in range(3):
        rim[np.ix_(4 * part + np.arange(4), out)] = first_z[:, az:].T
    along_last = np.zeros((LANES, LANES))
    source = np.concatenate((lanes[0::2], [1, step + 1]))
    along_last[np.ix_(source, lanes[0::2])] = second_z.T
    result = (send_rows, rows, last, send_lanes, along, rim, along_last)
    return tuple(table.astype(jnp.bfloat16) for table in result)


def iota(shape, axis):
    return lax.broadcasted_iota(jnp.int32, shape, axis)


def roll(values, shift, axis):
    return pltpu.roll(values, shift % values.shape[axis], axis)


def lift_rows(v, low, high):
    n = v.shape[0]
    row = iota(v.shape, 0)
    odd = row % 2 == 1
    up = jnp.where(row == n - 1, high, roll(v, -1, 0))
    w = jnp.where(odd, v - 0.5 * (roll(v, 1, 0) + up), v)
    down = jnp.where(row == 0, low - 0.5 * v, roll(w, 1, 0))
    return jnp.where(odd, w, w + 0.25 * (down + roll(w, -1, 0)))


def lift_groups(v, rim, s):
    lane = iota(v.shape, 1)
    odd = (lane // s) % 2 == 1
    up = jnp.where(lane >= LANES - s, rim, roll(v, -s, 1))
    w = jnp.where(odd, v - 0.5 * (roll(v, s, 1) + up), v)
    down = jnp.where(lane < s, rim - 0.5 * v, roll(w, s, 1))
    return jnp.where(odd, w, w + 0.25 * (down + roll(w, -s, 1)))


def shrink(v, thresh):
    return v - jnp.clip(v, -thresh, thresh)


def three(v):
    parts = []
    for _ in range(3):
        parts.append(v.astype(jnp.bfloat16))
        v = v - parts[-1].astype(jnp.float32)
    return parts


def mix(a, b, dims):
    return lax.dot_general(a, b, (dims, ((), ())), preferred_element_type=jnp.float32)


def mix_rows(table, v):
    wide = mix(table, jnp.concatenate(three(v), axis=1), ((1,), (0,)))
    return wide[:, :LANES] + wide[:, LANES : 2 * LANES] + wide[:, 2 * LANES :]


def mix_lanes(v, table):
    return mix(jnp.concatenate(three(v), axis=1), jnp.concatenate([table] * 3, axis=0), ((1,), (0,)))


def total(v):
    return jnp.sum(jnp.sum(v, axis=0, keepdims=True), axis=1, keepdims=True)


def kernel(sizes, cells, exps_in, field_in, rows_in, lanes_in, *rest):
    tables_in, (out, stats), scratch = rest[:TABLES], rest[TABLES : TABLES + 2], rest[TABLES + 2 :]
    nx, ny, nz = sizes
    ndev = nx * ny * nz
    scratch = list(scratch)
    tables = scratch[-TABLES:]
    scratch = scratch[:-TABLES]
    field, exps, k_s, l_s, in_sem = scratch[-5:]
    scratch = scratch[:-5]
    pairs = [(field_in, field), (exps_in, exps), *zip(tables_in, tables), (rows_in, k_s), (lanes_in, l_s)]
    loads = [pltpu.make_async_copy(a, b, in_sem.at[i]) for i, (a, b) in enumerate(pairs)]
    for load in loads:
        load.start()
    me = (lax.axis_index("gx"), lax.axis_index("gy"), lax.axis_index("gz"))

    def device(dx, dy, dz):
        return (
            lax.rem(me[0] + (dx + nx), nx),
            lax.rem(me[1] + (dy + ny), ny),
            lax.rem(me[2] + (dz + nz), nz),
        )

    def thresh(level):
        return jnp.exp2(jnp.full((1, LANES), exps[level].astype(jnp.float32)))

    def split(j):
        return j // (ny * nz), (j // nz) % ny, j % nz

    def launch(copies, send_sem, recv_sem):
        flights = [
            pltpu.make_async_remote_copy(
                src_ref=f, dst_ref=t, send_sem=send_sem, recv_sem=recv_sem,
                device_id=device(*d), device_id_type=MESH,
            )
            for f, t, d in copies
        ]
        for flight in flights:
            flight.start()
        return sum(t.size for _, t, _ in copies) // LANES

    def settle(span, send_sem, recv_sem):
        for sem in (recv_sem, send_sem):
            pltpu.make_async_copy(span, span, sem).wait()

    barrier = pltpu.get_barrier_semaphore()

    near = max(sizes) // 2 <= ROUNDS
    greeted = {
        tuple((d + size - 1) % size if near else d for d, size in zip(spot, sizes))
        for spot in np.ndindex(*(3, 3, 3) if near else sizes)
    } - {(0, 0, 0)}
    for spot in sorted(greeted):
        pl.semaphore_signal(barrier, inc=1, device_id=device(*spot), device_id_type=MESH)
    gath, msg, rows_s, final_s, g_send, g_recv = scratch[-6:]
    loads[0].wait()
    loads[1].wait()
    step_to = (1, -1)
    alone = nx == 2
    ways = (0,) if alone else (0, 1)
    (xs, xr, ys, yr, es, er, yl, zs, zr, ds, dr, ts, txr, tcr, rim, work, send_sem, recv_sem) = scratch[:BUFFERS]
    grown, sent, side, hz, t2r, t3r, o1s, o2s, m_send, m_recv = scratch[BUFFERS : BUFFERS + 10]
    fine_lanes, fine_edges, fine_place, *tables = tables
    src = field.at[0]
    px, n = src.shape[0], src.shape[1]
    half, q = n // 2, LANES // px
    lane = iota((n, LANES), 1)
    row8 = iota((8, LANES), 0)

    def ends(v):
        return v[n - 1 : n] - 0.5 * v[n - 2 : n - 1], v[0:1]

    def under(pair):
        return jnp.where(row8 == 0, pair[0], jnp.where(row8 == 1, pair[1], 0.0))

    planes = (src[px - 1] - 0.5 * src[px - 2], src[0])
    ys[0] = src[:, n - 1, :] - 0.5 * src[:, n - 2, :]
    ys[1] = src[:, 0, :]
    for gx in (0, 1):
        xs[gx] = planes[gx]
        es[2 * gx], es[2 * gx + 1] = ends(planes[gx])
    packed = jnp.zeros((n, LANES), jnp.float32)
    for x in range(px):
        packed = jnp.where(lane // q == x, roll(src[x], q * x + 2, 1), packed)
    packed = jnp.where(lane % q == 1, packed - 0.5 * roll(packed, 1, 1), packed)
    zs[...] = packed
    ds[0], ds[1] = ends(packed)
    for load in loads[2:5]:
        load.wait()
    edges = sum(
        mix(fine_edges[...], part, ((1,), (1,)))
        for part in three(jnp.concatenate((packed, under(ends(packed))), axis=0))
    )
    ts[...] = jnp.zeros(ts.shape, jnp.float32)
    for g in (0, 1):
        ts[g, :, pl.ds(0, n + 8)] = edges[2 * g : 2 * g + 2]

    pl.semaphore_wait(barrier, len(greeted))
    copies = []
    for g in (0, 1):
        dz = step_to[g]
        for gx in ways:
            for gy in (0, 1):
                copies.append((ts.at[g], tcr.at[g, gy, gx], (step_to[gx], step_to[gy], dz)))
            copies.append((ts.at[g], txr.at[g, gx], (step_to[gx], 0, dz)))
        for gy in (0, 1):
            copies.append((ds.at[gy], dr.at[2 * g + gy], (0, step_to[gy], dz)))
    for gx in (0, 1):
        for gy in (0, 1):
            copies.append((es.at[2 * gx + gy], er.at[2 * gx + gy], (step_to[gx], step_to[gy], 0)))
    for g in (0, 1):
        copies.append((xs.at[g], xr.at[g], (step_to[g], 0, 0)))
    for g in (0, 1):
        copies.append((ys.at[g], yr.at[g], (0, step_to[g], 0)))
    for g in (0, 1):
        copies.append((zs, zr.at[g], (0, 0, step_to[g])))
    sent_rows = launch(copies, send_sem, recv_sem)
    settle(grown.at[pl.ds(0, sent_rows)], send_sem, recv_sem)

    lane2, row2 = iota((2, LANES), 1), iota((2, LANES), 0)
    for g in (0, 1):
        yl[g] = lift_rows(yr[g], er[g], er[2 + g])

    def both(ref):
        return ref[0] if alone else jnp.where(row2 == 0, ref[0], ref[1])

    def columns(top, table):
        pieces = [part.astype(jnp.float32) for part in three(top)]
        pieces.append(jnp.zeros_like(top))
        return mix(jnp.concatenate(pieces, axis=0).astype(jnp.bfloat16), table, ((0,), (0,)))

    tops = []
    for g in (0, 1):
        v = jnp.where(lane2 == n, both(tcr.at[g, 0]), both(tcr.at[g, 1]))
        v = jnp.where(lane2 < n, both(txr.at[g]), v)
        tops.append(jnp.where(lane2 < n + 2, v, 0.0))
    beside = columns(jnp.concatenate(tops, axis=0), fine_place[...])[0 : n + 8]

    def kinds(a, b):
        return jnp.where(iota(a.shape, 1) % q == 1, a, b)

    lower = under((kinds(dr[0], dr[2]), kinds(dr[1], dr[3])))
    v = lift_groups(jnp.concatenate((kinds(zr[0], zr[1]), lower), axis=0), beside, q)
    v = lift_rows(v[0:n], v[n : n + 1], v[n + 1 : n + 2])
    v = jnp.where(lane % q == 2, roll(v, 1, 1), jnp.where(lane % q == 1, roll(v, -1, 1), roll(v, -2, 1)))
    rim[...] = v
    border = jnp.concatenate((rim[pl.ds(0, half, stride=2), :], rim[pl.ds(1, half, stride=2), :]), axis=0)
    share = jnp.where(lane == LANES - 1, -0.5, jnp.where(lane == LANES - 2, -0.125, jnp.where(lane == 0, 0.25, 0.0)))
    level_thresh = thresh(0)
    inner = (iota((n, LANES), 0) < half) & (lane % 2 == 0)
    row = iota((half, LANES), 0)

    def halves(ref, x):
        return [ref[x, pl.ds(start, half, stride=2), :] for start in (0, 1)]

    def lift_halves(v, x):
        even, odd = v
        after = jnp.where(row == half - 1, yl[1, x : x + 1, :], roll(even, -1, 0))
        detail = odd - 0.5 * (even + after)
        before = jnp.where(row == 0, yl[0, x : x + 1, :] - 0.5 * even, roll(detail, 1, 0))
        return [even + 0.25 * (before + detail), detail]

    even = halves(src, 0)
    before = [p - 0.5 * e for p, e in zip(halves(xr, 0), even)]
    stack = []
    for k in range(px // 2):
        after = halves(src, 2 * k + 2) if 2 * k + 2 < px else halves(xr, 1)
        detail = [o - 0.5 * (e + a) for o, e, a in zip(halves(src, 2 * k + 1), even, after)]
        smooth = [e + 0.25 * (b + d) for e, b, d in zip(even, before, detail)]
        stack += lift_halves(smooth, 2 * k) + lift_halves(detail, 2 * k + 1)
        even, before = after, detail
        if len(stack) == 2 * BATCH:
            wide = mix_lanes(jnp.concatenate(stack, axis=0), fine_lanes[...])
            for i in range(BATCH):
                x = 2 * k + 2 - BATCH + i
                v = wide[n * i : n * i + n] + roll(border, LANES - 2 - q * x, 1) * share
                work[x] = v
                if x % 2 == 0:
                    grown[pl.ds(x // 2 * half, half), :] = v[0:half]
            stack = []

    def finish():
        energy = kept = jnp.zeros((n, LANES), jnp.float32)
        for x in range(px):
            v = work[x]
            small = shrink(v, level_thresh)
            if x % 2 == 0:
                energy += jnp.where(inner, 0.0, v * v)
                kept += jnp.where(inner, 0.0, jnp.abs(small))
            else:
                energy += v * v
                kept += jnp.abs(small)
            for start in (0, 1):
                out[0, x, pl.ds(start, half, stride=2), :] = small[half * start : half * start + half]
        return [total(energy), total(kept)]

    ax, ay = px // 2, n // 2
    own = ax * ay
    send_rows, rows1, rows2, send_lanes, lanes1, rim1, lanes2 = tables
    for load in loads[5 : 2 + TABLES]:
        load.wait()
    here = grown[0:own]
    halo = mix_rows(send_rows[...], here)
    sent[...] = halo
    edges = sum(
        mix(send_lanes[...], part, ((1,), (1,)))
        for part in three(jnp.concatenate((here, halo), axis=0))
    )
    extra = halo.shape[0]
    for g in (0, 1):
        side[g, :, pl.ds(own, 2 * LANES)] = jnp.zeros((2, 2 * LANES), jnp.float32)
        side[g, :, pl.ds(0, own + extra)] = edges[2 * g : 2 * g + 2]

    px_rows, py_rows = 4 * ay, 4 * ax
    copies = []
    for g in (0, 1):
        dz = step_to[g]
        tail = pl.ds(own + LANES, LANES)
        for gy in (0, 1):
            for gx in ways:
                copies.append((side.at[g, :, tail], t3r.at[g, gy, gx], (step_to[gx], step_to[gy], dz)))
        middle = pl.ds(own, LANES)
        for gx in ways:
            copies.append((side.at[g, :, middle], t2r.at[g, gx], (step_to[gx], 0, dz)))
        for gy in (0, 1):
            copies.append((side.at[g, :, middle], t2r.at[g, 2 + gy], (0, step_to[gy], dz)))
        copies.append((side.at[g, :, pl.ds(0, own)], hz.at[g, :, pl.ds(0, own)], (0, 0, dz)))

    def rows_copy(start, size, to):
        copies.append((sent.at[pl.ds(start, size)], grown.at[pl.ds(own + start, size)], to))

    parts = len(ways)
    for gy in (0, 1):
        for gx in ways:
            rows_copy(px_rows + py_rows + 8 * gy + 4 * gx, 8 // parts, (step_to[gx], step_to[gy], 0))
    for gx in ways:
        rows_copy(px_rows // 2 * gx, px_rows // parts, (step_to[gx], 0, 0))
    for gy in (0, 1):
        rows_copy(px_rows + py_rows // 2 * gy, py_rows // 2, (0, step_to[gy], 0))
    sent_rows = launch(copies, m_send, m_recv)
    sums = finish()
    settle(grown.at[pl.ds(0, sent_rows)], m_send, m_recv)

    for g in (0, 1):
        v = jnp.where(lane2 < px_rows // 2, t2r[g, 0], t2r[g, 0 if alone else 1])
        v = jnp.where(lane2 < px_rows, v, jnp.where(lane2 < px_rows + py_rows // 2, t2r[g, 2], t2r[g, 3]))
        hz[g, :, pl.ds(own, LANES)] = v
        u = []
        for gy in (0, 1):
            u.append(jnp.where(lane2 % 8 < 4, t3r[g, gy, 0], t3r[g, gy, 0 if alone else 1]))
        v = jnp.where(lane2 < 8, u[0], u[1])
        hz[g, :, pl.ds(own + LANES, LANES)] = jnp.where(lane2 < 16, v, 0.0)
    rim_rows = columns(jnp.concatenate((hz[0], hz[1]), axis=0), rim1[...])
    wide = mix_lanes(grown[...], lanes1[...]) + rim_rows[0 : own + extra]
    first = mix_rows(rows1[...], wide)
    second = mix_lanes(mix_rows(rows2[...], first), lanes2[...])
    o1s[...] = first[0:own]
    o2s[...] = second.reshape(o2s.shape)

    def tally(v, level, ny):
        s = 2**level
        row, at = iota(v.shape, 0), iota(v.shape, 1)
        smooth = ((row // ny) % 2 == 0) & (row % 2 == 0) & (at % (2 * s) == 0)
        use = (at % s == 0) & ~smooth
        small = shrink(v, thresh(level))
        return [total(jnp.where(use, v * v, 0.0)), total(jnp.where(use, jnp.abs(small), 0.0))]

    sums += tally(first[0:own], 1, ay) + tally(second, 2, ay // 2)

    def place(source, level):
        s = 2**level
        small_y = ay >> (level - 1)
        keep = iota((small_y, LANES), 1) % s == 0
        for x in range(ax >> (level - 1)):
            spot = (0, s * x, pl.ds(0, small_y, stride=s), slice(None))
            out[spot] = jnp.where(keep, shrink(source(x), thresh(level)), out[spot])

    cx, cy = ax // 4, ay // 4
    step = 2**FINE
    count = cx * cy
    for x in range(cx):
        rows_s[pl.ds(x * cy, cy), :] = o2s[2 * x, pl.ds(0, cy, stride=2), :]
    here = rows_s[...]
    lane = iota((count, LANES), 1)
    row = iota((count, LANES), 0)
    here = jnp.where(lane % step == 0, here, 0.0)
    for bit in (1, 2, 4):
        here = jnp.where((row & bit) != 0, roll(here, bit, 1), here)
    groups = count // 8
    one = iota((1, LANES), 1)
    for g in range(groups):
        msg[g : g + 1] = jnp.sum(here[8 * g : 8 * g + 8], axis=0, keepdims=True)
    tail = jnp.zeros((1, LANES), jnp.float32)
    for i, whole in enumerate(sums):
        tail = jnp.where(one == i, whole, tail)
    msg[groups:] = jnp.broadcast_to(tail, (msg.shape[0] - groups, LANES))

    slot = (me[2] * nx + me[0]) * ny + me[1]

    def post(j):
        return pltpu.make_async_remote_copy(
            src_ref=msg, dst_ref=gath.at[slot], send_sem=g_send, recv_sem=g_recv,
            device_id=device(*split(j)), device_id_type=MESH,
        )

    def send(j, carry):
        post(ndev - j).start()
        return carry

    if ndev <= 32:
        for j in range(1, ndev):
            post(ndev - j).start()
    else:
        lax.fori_loop(1, ndev, send, 0)
    gath[slot] = msg[...]
    place(lambda x: o1s[pl.ds(x * ay, ay), :], 1)
    place(lambda x: o2s[x], 2)
    settle(gath.at[pl.ds(0, ndev - 1)], g_send, g_recv)

    spots = nx * ny
    at = iota((spots, LANES), 1) % step
    tail = jnp.zeros((1, LANES), jnp.float32)
    for g in range(groups):
        boxes = [gath[pl.ds(z * spots, spots), g, :] for z in range(nz)]
        for bit in range(8):
            v = jnp.zeros((spots, LANES), jnp.float32)
            for z in range(nz):
                v = jnp.where(at == z, roll(boxes[z], z - bit, 1), v)
            final_s[pl.ds((bit * groups + g) * spots, spots), :] = v
    tail = jnp.sum(gath[:, groups, :], axis=0, keepdims=True)

    def dot(a, b):
        return jnp.dot(a, b, precision=lax.Precision.HIGHEST, preferred_element_type=jnp.float32)

    grid = final_s[...]
    loads[2 + TABLES].wait()
    loads[3 + TABLES].wait()
    half3, half4 = dot(k_s[0], grid), dot(k_s[1], grid)
    grid, grid4 = dot(half3, l_s[0]), dot(half4, l_s[1])
    row = iota(grid.shape, 0)
    lane = iota(grid.shape, 1)
    inner_row = row % count
    gx, gy, gz = inner_row // cy, inner_row % cy, lane // step
    valid = lane % step < nz
    even3 = (gx % 2 == 0) & (gy % 2 == 0) & (gz % 2 == 0)
    even4 = (gx % 4 == 0) & (gy % 4 == 0) & (gz % 4 == 0)
    det3 = valid & ~even3
    det4 = valid & even3 & ~even4
    small3 = shrink(grid, thresh(FINE))
    small4 = shrink(grid4, thresh(FINE + 1))
    final_s[...] = jnp.where(even3, jnp.where(even4, grid4, small4), small3)

    def masked(mask, v):
        return total(jnp.where(mask, v, 0.0))

    coarse = ((masked(det3, grid * grid), masked(det3, jnp.abs(small3))),
              (masked(det4, grid4 * grid4), masked(det4, jnp.abs(small4))))
    for q in (0, 1):
        line = jnp.zeros((1, LANES), jnp.float32)
        for level in range(LEVELS):
            weight = 8.0 ** (level + 1) / (7.0 * cells)
            if level < FINE:
                value = jnp.sum(jnp.where(one == 2 * level + q, tail, 0.0), axis=1, keepdims=True)
            else:
                value = coarse[level - FINE][q]
            line = jnp.where(one == level, value * weight, line)
        stats[q] = line[:, 0:LEVELS]

    first = pl.multiple_of((me[0] * ny + me[1]) * count, count)
    mine = pltpu.roll(final_s[pl.ds(first, count), :], lax.rem(LANES - me[2], LANES), 1)
    rows_s[...] = mine
    keep = iota((cy, LANES), 1) % step == 0
    for x in range(cx):
        spot = (0, step * x, pl.ds(0, cy, stride=step), slice(None))
        out[spot] = jnp.where(keep, rows_s[pl.ds(x * cy, cy), :], out[spot])


def deliver(held, held_stats, out, stats, sem):
    rows = held.shape[1] // CHUNKS
    copies = [pltpu.make_async_copy(held_stats, stats, sem.at[CHUNKS])]
    for i in range(CHUNKS):
        part = pl.ds(i * rows, rows)
        copies.append(pltpu.make_async_copy(held.at[:, part], out.at[:, part], sem.at[i]))
    for copy in copies:
        copy.start()
    for copy in copies:
        copy.wait()


def shards(sizes, fields, exponents):
    nx, ny, nz = sizes
    ndev = nx * ny * nz
    _, lx, ly, lz = fields.shape
    cells = fields.size * ndev
    step = 2**FINE
    coarse = (lx // step, ly // step, lz // step)
    count = coarse[0] * coarse[1]
    tables = coarse_matrices(sizes, coarse)
    middle = middle_tables(lx // 2, ly // 2, lz // 2)
    own, extra = lx // 2 * (ly // 2), middle[0].shape[0]
    middle = fine_tables(lx) + middle
    scratch = [
        *(pltpu.VMEM(shape, jnp.float32) for shape in (
            (2, ly, LANES), (2, ly, LANES), (2, lx, LANES), (2, lx, LANES), (4, 1, LANES), (4, 1, LANES),
            (2, lx, LANES), (ly, LANES), (2, ly, LANES), (2, 1, LANES), (4, 1, LANES), (2, 2, LANES),
            (2, 2, 2, LANES), (2, 2, 2, 2, LANES), (ly, LANES), (lx, ly, LANES),
        )),
        pltpu.SemaphoreType.DMA,
        pltpu.SemaphoreType.DMA,
        *(pltpu.VMEM(shape, jnp.float32) for shape in (
            (own + extra, LANES), (extra, LANES), (2, 2, own + 2 * LANES), (2, 2, own + 2 * LANES),
            (2, 4, 2, LANES), (2, 2, 2, 2, LANES), (own, LANES), (lx // 4, ly // 4, LANES),
        )),
        pltpu.SemaphoreType.DMA,
        pltpu.SemaphoreType.DMA,
    ]
    height = -(-(count // 8 + 1) // 4) * 4
    scratch += [
        pltpu.VMEM((ndev, height, LANES), jnp.float32),
        pltpu.VMEM((height, LANES), jnp.float32),
        pltpu.VMEM((count, LANES), jnp.float32),
        pltpu.VMEM((nx * ny * count, LANES), jnp.float32),
        pltpu.SemaphoreType.DMA,
        pltpu.SemaphoreType.DMA,
        pltpu.VMEM(fields.shape, jnp.float32),
        pltpu.SMEM(exponents.shape, jnp.int32),
        pltpu.VMEM(tables[0].shape, jnp.float32),
        pltpu.VMEM(tables[1].shape, jnp.float32),
        pltpu.SemaphoreType.DMA((4 + TABLES,)),
        *(pltpu.VMEM(table.shape, table.dtype) for table in middle),
    ]
    vmem = pl.BlockSpec(memory_space=pltpu.VMEM)
    held = pl.pallas_call(
        functools.partial(kernel, sizes, cells),
        out_shape=(
            pltpu.VMEM(fields.shape, jnp.float32),
            pltpu.VMEM((2, 1, LEVELS), jnp.float32),
        ),
        in_specs=[pl.BlockSpec(memory_space=pltpu.HBM)] * (4 + TABLES),
        out_specs=(vmem, vmem),
        scratch_shapes=scratch,
        compiler_params=pltpu.CompilerParams(
            collective_id=0, has_side_effects=True, vmem_limit_bytes=VMEM_LIMIT
        ),
    )(*(pltpu.with_memory_space_constraint(x, pltpu.HBM) for x in (exponents, fields, *map(jnp.asarray, (*tables, *middle)))))
    hbm = pl.BlockSpec(memory_space=pltpu.HBM)
    return pl.pallas_call(
        deliver,
        out_shape=(
            jax.ShapeDtypeStruct(fields.shape, jnp.float32),
            jax.ShapeDtypeStruct((2, 1, LEVELS), jnp.float32),
        ),
        in_specs=(vmem, vmem),
        out_specs=(hbm, hbm),
        scratch_shapes=[pltpu.SemaphoreType.DMA((CHUNKS + 1,))],
    )(*(pltpu.with_memory_space_constraint(x, pltpu.VMEM) for x in held))


def solution(mesh):
    sizes = tuple(mesh.shape[name] for name in ("gx", "gy", "gz"))
    placed = (P(None, "gx", "gy", "gz"), P())
    return jax.shard_map(
        functools.partial(shards, sizes),
        mesh=mesh,
        in_specs=placed,
        out_specs=placed,
        check_vma=False,
    )
```

```python
import functools

import numpy as np

import jax
import jax.numpy as jnp
from jax import lax
from jax.experimental import pallas as pl
from jax.experimental.pallas import tpu as pltpu
from jax.sharding import PartitionSpec as P

FINE = 3
LEVELS = 5
LANES = 128
CHUNKS = 4
BUFFERS = 18
TABLES = 12
BATCH = 8
ROUNDS = 2
VMEM_LIMIT = 58_720_256
MESH = pl.DeviceIdType.MESH


def periodic_lift(length):
    eye = np.eye(length)
    even, odd = eye[0::2], eye[1::2]
    detail = odd - 0.5 * (even + np.roll(even, -1, 0))
    smooth = even + 0.25 * (np.roll(detail, 1, 0) + detail)
    whole = np.zeros((length, length))
    whole[0::2] = smooth
    whole[1::2] = detail
    return whole


def second_lift(length):
    whole = np.zeros((length, length))
    whole[0::2, 0::2] = periodic_lift(length // 2)
    return whole


def coarse_matrices(sizes, coarse):
    nx, ny, nz = sizes
    cx, cy, cz = coarse
    rows = np.arange(nx * ny * cx * cy)
    dev, inner = rows // (cx * cy), rows % (cx * cy)
    gx = (dev // ny) * cx + inner // cy
    gy = (dev % ny) * cy + inner % cy
    step = LANES // cz
    lanes = np.array([z * step + d for d in range(nz) for z in range(cz)])
    reach_y, reach_x, spot = np.indices((cy + 3, cx + 3, nx * ny)).reshape(3, -1)
    from_x = (spot // ny * cx + reach_x - 1) % (nx * cx)
    from_y = (spot % ny * cy + reach_y - 1) % (ny * cy)
    from_z = np.arange(-1, nz * cz + 2) % (nz * cz)
    result = []
    for both_levels in (False, True):
        mx, my, mz = periodic_lift(nx * cx), periodic_lift(ny * cy), periodic_lift(nz * cz)
        if both_levels:
            mx, my, mz = second_lift(nx * cx) @ mx, second_lift(ny * cy) @ my, second_lift(nz * cz) @ mz
        both = mx[gx[:, None], from_x[None]] * my[gy[:, None], from_y[None]]
        along = np.zeros((LANES, LANES))
        along[np.ix_(np.arange(len(from_z)), lanes)] = mz[:, from_z].T
        result.append((both.astype(np.float32), along.astype(np.float32)))
    return [np.stack(pair) for pair in zip(*result)]


def reach_line(n):
    twice = periodic_lift(3 * n // 2)[0::2] @ periodic_lift(3 * n)[0::2]
    return twice[n // 4 - 1 : n // 2 + 2, n : 2 * n]


def reach_tables(ax, ay, az):
    part_x, part_y, part_z = reach_line(ax), reach_line(ay), reach_line(az)
    wide, deep = len(part_z), len(part_y)
    rows = np.zeros((deep, 8, ax * ay))
    rows[:, : len(part_x)] = np.einsum("yb,xa->yxab", part_y, part_x).reshape(deep, -1, ax * ay)
    rows = rows.reshape(8 * deep, -1)
    high = rows.astype(jnp.bfloat16)
    low = (rows - high.astype(np.float64)).astype(jnp.bfloat16)
    along = np.zeros((deep + 1, LANES, LANES))
    for y in range(deep):
        fit = min(wide, LANES - wide * y)
        along[y, :: LANES // az, wide * y : wide * y + fit] = part_z[:fit].T
    along[deep, :: LANES // az, : wide - fit] = part_z[fit:].T
    return np.concatenate((high, low)), along.reshape(-1, LANES).astype(jnp.bfloat16)


def lift_line(n):
    whole = np.zeros((n, n + 2))
    cells = np.eye(n + 2)
    even, odd = cells[0:n:2], cells[1:n:2]
    after = np.concatenate((even[1:], cells[n + 1 :]))
    detail = odd - 0.5 * (even + after)
    before = np.concatenate((cells[n : n + 1] - 0.5 * even[:1], detail[:-1]))
    whole[0::2] = even + 0.25 * (before + detail)
    whole[1::2] = detail
    return whole

def line_tables(n):
    lift = lift_line(n)
    own = lift[:, :n]
    sent = np.zeros((4, n))
    sent[0, n - 1], sent[0, n - 2] = 1.0, -0.5
    sent[1] = own[n - 2] - 0.5 * own[n - 4]
    sent[2, 0] = 1.0
    sent[3] = own[0]
    first = np.zeros((n + 2, n + 4))
    first[:n, :n] = own
    first[:n, n], first[:n, n + 2] = lift[:, n], lift[:, n + 1]
    first[n, n + 1], first[n, 0] = 1.0, lift[n - 2, n + 1]
    first[n + 1, n + 3] = 1.0
    first[n + 1, :n] = lift[0, n] * sent[0]
    return sent, first, lift_line(n // 2)


def fine_tables(px):
    q = LANES // px
    ends = np.zeros((2, px))
    ends[0, px - 1], ends[0, px - 2], ends[1, 0] = 1.0, -0.5, 1.0
    edges = np.zeros((8, LANES))
    place = np.zeros((16, LANES))
    for z in range(2):
        for x in range(2):
            edges[2 * z + x, 1 + z :: q] = ends[x]
            for part in range(3):
                place[4 * part + 2 * z + x, (LANES - q) * x + 1 + z] = 1.0
    result = (lift_line(LANES)[:, :LANES].T, edges, place)
    return tuple(table.astype(jnp.bfloat16) for table in result)


def middle_tables(ax, ay, az):
    step = LANES // az
    sent_x, first_x, second_x = line_tables(ax)
    sent_y, first_y, second_y = line_tables(ay)
    sent_z, first_z, second_z = line_tables(az)
    own = [(x, y) for x in range(ax) for y in range(ay)]
    corners = [(x, 2 * g + y) for g in range(2) for x in range(4) for y in range(2)]
    extra = [(ax + k, y) for k in range(4) for y in range(ay)]
    extra += [(x, ay + k) for k in range(4) for x in range(ax)]
    extra += [(ax + x, ay + y) for x, y in corners]
    taken = np.array(own + extra)
    given = own + [(ax + k, y) for k in range(2) for y in range(0, ay, 2)]
    given += [(x, ay + k) for k in range(2) for x in range(0, ax, 2)]
    given += [(ax + x, ay + y) for x in range(2) for y in range(2)]
    height = -(-len(given) // 16) * 16

    whole_x, whole_y = np.concatenate((np.eye(ax), sent_x)), np.concatenate((np.eye(ay), sent_y))
    ex, ey = np.array(extra).T
    ox, oy = np.array(own).T
    send_rows = whole_x[np.ix_(ex, ox)] * whole_y[np.ix_(ey, oy)]
    gx, gy = np.array(given).T
    tx, ty = taken.T
    rows = np.zeros((height, len(taken)))
    rows[: len(given)] = first_x[np.ix_(gx, tx)] * first_y[np.ix_(gy, ty)]

    def spot(at, n):
        return np.where(at >= n, n // 2 + at - n, at // 2)

    half = np.array([(x, y) for x in range(ax // 2) for y in range(ay // 2)])
    use = ((gx % 2 == 0) | (gx >= ax)) & ((gy % 2 == 0) | (gy >= ay))
    last = np.zeros((len(half), height))
    pick_x = second_x[np.ix_(half[:, 0], spot(gx, ax))]
    pick_y = second_y[np.ix_(half[:, 1], spot(gy, ay))]
    last[:, : len(given)] = pick_x * pick_y * use

    lanes = np.arange(az) * step
    out = np.concatenate((lanes, [1, step + 1]))
    send_lanes = np.zeros((8, LANES))
    send_lanes[np.ix_(np.arange(4), lanes)] = sent_z
    along = np.zeros((LANES, LANES))
    along[np.ix_(lanes, out)] = first_z[:, :az].T
    rim = np.zeros((16, LANES))
    for part in range(3):
        rim[np.ix_(4 * part + np.arange(4), out)] = first_z[:, az:].T
    along_last = np.zeros((LANES, LANES))
    source = np.concatenate((lanes[0::2], [1, step + 1]))
    along_last[np.ix_(source, lanes[0::2])] = second_z.T
    result = (send_rows, rows, last, send_lanes, along, rim, along_last)
    return tuple(table.astype(jnp.bfloat16) for table in result)


def iota(shape, axis):
    return lax.broadcasted_iota(jnp.int32, shape, axis)


def roll(values, shift, axis):
    return pltpu.roll(values, shift % values.shape[axis], axis)


def lift_rows(v, low, high):
    n = v.shape[0]
    row = iota(v.shape, 0)
    odd = row % 2 == 1
    up = jnp.where(row == n - 1, high, roll(v, -1, 0))
    w = jnp.where(odd, v - 0.5 * (roll(v, 1, 0) + up), v)
    down = jnp.where(row == 0, low - 0.5 * v, roll(w, 1, 0))
    return jnp.where(odd, w, w + 0.25 * (down + roll(w, -1, 0)))


def lift_groups(v, rim, s):
    lane = iota(v.shape, 1)
    odd = (lane // s) % 2 == 1
    up = jnp.where(lane >= LANES - s, rim, roll(v, -s, 1))
    w = jnp.where(odd, v - 0.5 * (roll(v, s, 1) + up), v)
    down = jnp.where(lane < s, rim - 0.5 * v, roll(w, s, 1))
    return jnp.where(odd, w, w + 0.25 * (down + roll(w, -s, 1)))


def shrink(v, thresh):
    return v - jnp.clip(v, -thresh, thresh)


def three(v):
    parts = []
    for _ in range(3):
        parts.append(v.astype(jnp.bfloat16))
        v = v - parts[-1].astype(jnp.float32)
    return parts


def mix(a, b, dims):
    return lax.dot_general(a, b, (dims, ((), ())), preferred_element_type=jnp.float32)


def mix_rows(table, v):
    wide = mix(table, jnp.concatenate(three(v), axis=1), ((1,), (0,)))
    return wide[:, :LANES] + wide[:, LANES : 2 * LANES] + wide[:, 2 * LANES :]


def mix_lanes(v, table):
    return mix(jnp.concatenate(three(v), axis=1), jnp.concatenate([table] * 3, axis=0), ((1,), (0,)))


def total(v):
    return jnp.sum(jnp.sum(v, axis=0, keepdims=True), axis=1, keepdims=True)


def kernel(sizes, cells, exps_in, field_in, rows_in, lanes_in, *rest):
    tables_in, (out, stats), scratch = rest[:TABLES], rest[TABLES : TABLES + 2], rest[TABLES + 2 :]
    nx, ny, nz = sizes
    ndev = nx * ny * nz
    scratch = list(scratch)
    tables = scratch[-TABLES:]
    scratch = scratch[:-TABLES]
    field, exps, k_s, l_s, in_sem = scratch[-5:]
    scratch = scratch[:-5]
    pairs = [(field_in, field), (exps_in, exps), *zip(tables_in, tables), (rows_in, k_s), (lanes_in, l_s)]
    loads = [pltpu.make_async_copy(a, b, in_sem.at[i]) for i, (a, b) in enumerate(pairs)]
    me = (lax.axis_index("gx"), lax.axis_index("gy"), lax.axis_index("gz"))

    def device(dx, dy, dz):
        return (
            lax.rem(me[0] + (dx + nx), nx),
            lax.rem(me[1] + (dy + ny), ny),
            lax.rem(me[2] + (dz + nz), nz),
        )

    def distance(spot):
        return sum(min(d, size - d) for d, size in zip(spot, sizes))

    def thresh(level):
        return jnp.exp2(jnp.full((1, LANES), exps[level].astype(jnp.float32)))

    def split(j):
        return j // (ny * nz), (j // nz) % ny, j % nz

    def launch(copies, send_sem, recv_sem):
        flights = [
            pltpu.make_async_remote_copy(
                src_ref=f, dst_ref=t, send_sem=send_sem, recv_sem=recv_sem,
                device_id=device(*d), device_id_type=MESH,
            )
            for f, t, d in copies
        ]
        for flight in flights:
            flight.start()
        return sum(t.size for _, t, _ in copies) // LANES

    def settle(span, send_sem, recv_sem):
        for sem in (recv_sem, send_sem):
            pltpu.make_async_copy(span, span, sem).wait()

    barrier = pltpu.get_barrier_semaphore()

    near = max(sizes) // 2 <= ROUNDS
    greeted = {
        tuple((d + size - 1) % size if near else d for d, size in zip(spot, sizes))
        for spot in np.ndindex(*(3, 3, 3) if near else sizes)
    } - {(0, 0, 0)}
    for spot in sorted(greeted, key=lambda spot: (-distance(spot), spot)):
        pl.semaphore_signal(barrier, inc=1, device_id=device(*spot), device_id_type=MESH)
    for load in loads:
        load.start()
    gath, msg, parts_s, final_s, tally_s, tallies, g_send, g_recv, t_send, t_recv = scratch[-10:]
    loads[0].wait()
    loads[1].wait()
    step_to = (1, -1)
    alone = nx == 2
    ways = (0,) if alone else (0, 1)
    (xs, xr, ys, yr, es, er, yl, zs, zr, ds, dr, ts, txr, tcr, rim, work, send_sem, recv_sem) = scratch[:BUFFERS]
    grown, sent, side, hz, t2r, t3r, o1s, o2s, m_send, m_recv = scratch[BUFFERS : BUFFERS + 10]
    fine_lanes, fine_edges, fine_place, reach_rows, reach_lanes, *tables = tables
    src = field.at[0]
    px, n = src.shape[0], src.shape[1]
    half, q = n // 2, LANES // px
    lane = iota((n, LANES), 1)
    row8 = iota((8, LANES), 0)

    def ends(v):
        return v[n - 1 : n] - 0.5 * v[n - 2 : n - 1], v[0:1]

    def under(pair):
        return jnp.where(row8 == 0, pair[0], jnp.where(row8 == 1, pair[1], 0.0))

    planes = (src[px - 1] - 0.5 * src[px - 2], src[0])
    ys[0] = src[:, n - 1, :] - 0.5 * src[:, n - 2, :]
    ys[1] = src[:, 0, :]
    for gx in (0, 1):
        xs[gx] = planes[gx]
        es[2 * gx], es[2 * gx + 1] = ends(planes[gx])
    packed = jnp.zeros((n, LANES), jnp.float32)
    for x in range(px):
        packed = jnp.where(lane // q == x, roll(src[x], q * x + 2, 1), packed)
    packed = jnp.where(lane % q == 1, packed - 0.5 * roll(packed, 1, 1), packed)
    zs[...] = packed
    ds[0], ds[1] = ends(packed)
    for load in loads[2:5]:
        load.wait()
    edges = sum(
        mix(fine_edges[...], part, ((1,), (1,)))
        for part in three(jnp.concatenate((packed, under(ends(packed))), axis=0))
    )
    ts[...] = jnp.zeros(ts.shape, jnp.float32)
    for g in (0, 1):
        ts[g, :, pl.ds(0, n + 8)] = edges[2 * g : 2 * g + 2]

    pl.semaphore_wait(barrier, len(greeted))
    copies = []
    for g in (0, 1):
        dz = step_to[g]
        for gx in ways:
            for gy in (0, 1):
                copies.append((ts.at[g], tcr.at[g, gy, gx], (step_to[gx], step_to[gy], dz)))
            copies.append((ts.at[g], txr.at[g, gx], (step_to[gx], 0, dz)))
        for gy in (0, 1):
            copies.append((ds.at[gy], dr.at[2 * g + gy], (0, step_to[gy], dz)))
    for gx in (0, 1):
        for gy in (0, 1):
            copies.append((es.at[2 * gx + gy], er.at[2 * gx + gy], (step_to[gx], step_to[gy], 0)))
    for g in (0, 1):
        copies.append((xs.at[g], xr.at[g], (step_to[g], 0, 0)))
    for g in (0, 1):
        copies.append((ys.at[g], yr.at[g], (0, step_to[g], 0)))
    for g in (0, 1):
        copies.append((zs, zr.at[g], (0, 0, step_to[g])))
    sent_rows = launch(copies, send_sem, recv_sem)
    settle(grown.at[pl.ds(0, sent_rows)], send_sem, recv_sem)

    lane2, row2 = iota((2, LANES), 1), iota((2, LANES), 0)
    for g in (0, 1):
        yl[g] = lift_rows(yr[g], er[g], er[2 + g])

    def both(ref):
        return ref[0] if alone else jnp.where(row2 == 0, ref[0], ref[1])

    def columns(top, table):
        pieces = [part.astype(jnp.float32) for part in three(top)]
        pieces.append(jnp.zeros_like(top))
        return mix(jnp.concatenate(pieces, axis=0).astype(jnp.bfloat16), table, ((0,), (0,)))

    tops = []
    for g in (0, 1):
        v = jnp.where(lane2 == n, both(tcr.at[g, 0]), both(tcr.at[g, 1]))
        v = jnp.where(lane2 < n, both(txr.at[g]), v)
        tops.append(jnp.where(lane2 < n + 2, v, 0.0))
    beside = columns(jnp.concatenate(tops, axis=0), fine_place[...])[0 : n + 8]

    def kinds(a, b):
        return jnp.where(iota(a.shape, 1) % q == 1, a, b)

    lower = under((kinds(dr[0], dr[2]), kinds(dr[1], dr[3])))
    v = lift_groups(jnp.concatenate((kinds(zr[0], zr[1]), lower), axis=0), beside, q)
    v = lift_rows(v[0:n], v[n : n + 1], v[n + 1 : n + 2])
    v = jnp.where(lane % q == 2, roll(v, 1, 1), jnp.where(lane % q == 1, roll(v, -1, 1), roll(v, -2, 1)))
    rim[...] = v
    border = jnp.concatenate((rim[pl.ds(0, half, stride=2), :], rim[pl.ds(1, half, stride=2), :]), axis=0)
    share = jnp.where(lane == LANES - 1, -0.5, jnp.where(lane == LANES - 2, -0.125, jnp.where(lane == 0, 0.25, 0.0)))
    level_thresh = thresh(0)
    inner = (iota((n, LANES), 0) < half) & (lane % 2 == 0)
    row = iota((half, LANES), 0)

    def halves(ref, x):
        return [ref[x, pl.ds(start, half, stride=2), :] for start in (0, 1)]

    def lift_halves(v, x):
        even, odd = v
        after = jnp.where(row == half - 1, yl[1, x : x + 1, :], roll(even, -1, 0))
        detail = odd - 0.5 * (even + after)
        before = jnp.where(row == 0, yl[0, x : x + 1, :] - 0.5 * even, roll(detail, 1, 0))
        return [even + 0.25 * (before + detail), detail]

    even = halves(src, 0)
    before = [p - 0.5 * e for p, e in zip(halves(xr, 0), even)]
    stack = []
    for k in range(px // 2):
        after = halves(src, 2 * k + 2) if 2 * k + 2 < px else halves(xr, 1)
        detail = [o - 0.5 * (e + a) for o, e, a in zip(halves(src, 2 * k + 1), even, after)]
        smooth = [e + 0.25 * (b + d) for e, b, d in zip(even, before, detail)]
        stack += lift_halves(smooth, 2 * k) + lift_halves(detail, 2 * k + 1)
        even, before = after, detail
        if len(stack) == 2 * BATCH:
            wide = mix_lanes(jnp.concatenate(stack, axis=0), fine_lanes[...])
            for i in range(BATCH):
                x = 2 * k + 2 - BATCH + i
                v = wide[n * i : n * i + n] + roll(border, LANES - 2 - q * x, 1) * share
                work[x] = v
                if x % 2 == 0:
                    grown[pl.ds(x // 2 * half, half), :] = v[0:half]
            stack = []

    def finish():
        energy = kept = jnp.zeros((n, LANES), jnp.float32)
        for x in range(px):
            v = work[x]
            small = shrink(v, level_thresh)
            if x % 2 == 0:
                energy += jnp.where(inner, 0.0, v * v)
                kept += jnp.where(inner, 0.0, jnp.abs(small))
            else:
                energy += v * v
                kept += jnp.abs(small)
            for start in (0, 1):
                out[0, x, pl.ds(start, half, stride=2), :] = small[half * start : half * start + half]
        return [total(energy), total(kept)]

    ax, ay = px // 2, n // 2
    own = ax * ay
    send_rows, rows1, rows2, send_lanes, lanes1, rim1, lanes2 = tables
    for load in loads[5 : 2 + TABLES]:
        load.wait()
    here = grown[0:own]
    halo = mix_rows(send_rows[...], here)
    sent[...] = halo
    edges = sum(
        mix(send_lanes[...], part, ((1,), (1,)))
        for part in three(jnp.concatenate((here, halo), axis=0))
    )
    extra = halo.shape[0]
    for g in (0, 1):
        side[g, :, pl.ds(own, 2 * LANES)] = jnp.zeros((2, 2 * LANES), jnp.float32)
        side[g, :, pl.ds(0, own + extra)] = edges[2 * g : 2 * g + 2]

    px_rows, py_rows = 4 * ay, 4 * ax
    copies = []
    for g in (0, 1):
        dz = step_to[g]
        tail = pl.ds(own + LANES, LANES)
        for gy in (0, 1):
            for gx in ways:
                copies.append((side.at[g, :, tail], t3r.at[g, gy, gx], (step_to[gx], step_to[gy], dz)))
        middle = pl.ds(own, LANES)
        for gx in ways:
            copies.append((side.at[g, :, middle], t2r.at[g, gx], (step_to[gx], 0, dz)))
        for gy in (0, 1):
            copies.append((side.at[g, :, middle], t2r.at[g, 2 + gy], (0, step_to[gy], dz)))
        copies.append((side.at[g, :, pl.ds(0, own)], hz.at[g, :, pl.ds(0, own)], (0, 0, dz)))

    def rows_copy(start, size, to):
        copies.append((sent.at[pl.ds(start, size)], grown.at[pl.ds(own + start, size)], to))

    parts = len(ways)
    for gy in (0, 1):
        for gx in ways:
            rows_copy(px_rows + py_rows + 8 * gy + 4 * gx, 8 // parts, (step_to[gx], step_to[gy], 0))
    for gx in ways:
        rows_copy(px_rows // 2 * gx, px_rows // parts, (step_to[gx], 0, 0))
    for gy in (0, 1):
        rows_copy(px_rows + py_rows // 2 * gy, py_rows // 2, (0, step_to[gy], 0))
    sent_rows = launch(copies, m_send, m_recv)

    spots = nx * ny
    slot = (me[2] * nx + me[0]) * ny + me[1]
    cx, cy, cz = ax // 4, ay // 4, LANES // 2**FINE
    step = 2**FINE
    count = cx * cy
    long, deep, reach = cx + 3, cy + 3, cz + 3
    cut = LANES - reach * (deep - 1)
    rest = reach - cut

    def spread(source, target, send_sem, recv_sem):
        def post(j):
            return pltpu.make_async_remote_copy(
                src_ref=source, dst_ref=target, send_sem=send_sem, recv_sem=recv_sem,
                device_id=device(*split(j)), device_id_type=MESH,
            )

        def send(j, carry):
            post(j).start()
            return carry

        if ndev <= 32:
            for j in sorted(range(1, ndev), key=lambda j: (-distance(split(j)), j)):
                post(j).start()
        else:
            lax.fori_loop(1, ndev, send, 0)

    pieces = mix_rows(reach_rows[...], here)
    pieces = pieces[0 : 8 * deep] + pieces[8 * deep :]
    blocks = [part.astype(jnp.float32) for part in three(pieces)]

    def stack(first, last):
        rows = [jnp.concatenate([b[8 * y : 8 * y + 8] for y in range(first, last)], axis=1) for b in blocks]
        return jnp.concatenate(rows + [jnp.zeros_like(rows[0])], axis=0).astype(jnp.bfloat16)

    def fold(v):
        return v[0:8] + v[8:16] + v[16:24]

    sheet = fold(mix(stack(0, deep), reach_lanes[pl.ds(0, deep * LANES), :], ((1,), (0,))))
    loose = fold(mix(stack(deep - 1, deep), reach_lanes[pl.ds(deep * LANES, LANES), :], ((1,), (0,))))
    spare = loose[0:1]
    for x in range(1, long):
        spare += roll(loose[x : x + 1], rest * x, 1)
    msg[...] = jnp.where(row8 == long, spare, sheet)
    spread(msg, gath.at[slot], g_send, g_recv)
    gath[slot] = msg[...]
    sums = finish()
    settle(grown.at[pl.ds(0, sent_rows)], m_send, m_recv)

    for g in (0, 1):
        v = jnp.where(lane2 < px_rows // 2, t2r[g, 0], t2r[g, 0 if alone else 1])
        v = jnp.where(lane2 < px_rows, v, jnp.where(lane2 < px_rows + py_rows // 2, t2r[g, 2], t2r[g, 3]))
        hz[g, :, pl.ds(own, LANES)] = v
        u = []
        for gy in (0, 1):
            u.append(jnp.where(lane2 % 8 < 4, t3r[g, gy, 0], t3r[g, gy, 0 if alone else 1]))
        v = jnp.where(lane2 < 8, u[0], u[1])
        hz[g, :, pl.ds(own + LANES, LANES)] = jnp.where(lane2 < 16, v, 0.0)
    rim_rows = columns(jnp.concatenate((hz[0], hz[1]), axis=0), rim1[...])
    wide = mix_lanes(grown[...], lanes1[...]) + rim_rows[0 : own + extra]
    first = mix_rows(rows1[...], wide)
    second = mix_lanes(mix_rows(rows2[...], first), lanes2[...])
    o1s[...] = first[0:own]
    o2s[...] = second.reshape(o2s.shape)

    def tally(v, level, ny):
        s = 2**level
        row, at = iota(v.shape, 0), iota(v.shape, 1)
        smooth = ((row // ny) % 2 == 0) & (row % 2 == 0) & (at % (2 * s) == 0)
        use = (at % s == 0) & ~smooth
        small = shrink(v, thresh(level))
        return [total(jnp.where(use, v * v, 0.0)), total(jnp.where(use, jnp.abs(small), 0.0))]

    sums += tally(first[0:own], 1, ay) + tally(second, 2, ay // 2)

    def place(source, level):
        s = 2**level
        small_y = ay >> (level - 1)
        keep = iota((small_y, LANES), 1) % s == 0
        for x in range(ax >> (level - 1)):
            spot = (0, s * x, pl.ds(0, small_y, stride=s), slice(None))
            out[spot] = jnp.where(keep, shrink(source(x), thresh(level)), out[spot])

    one = iota((1, LANES), 1)
    tail = jnp.zeros((1, LANES), jnp.float32)
    for i, whole in enumerate(sums):
        tail = jnp.where(one == i, whole, tail)
    tally_s[...] = tail
    spread(tally_s, tallies.at[slot], t_send, t_recv)
    tallies[slot] = tail
    place(lambda x: o1s[pl.ds(x * ay, ay), :], 1)
    place(lambda x: o2s[x], 2)
    settle(gath.at[pl.ds(0, ndev - 1)], g_send, g_recv)

    at = iota((spots, LANES), 1)
    spares = [gath[pl.ds(z * spots, spots), long, :] for z in range(nz)]

    def window(v, source, start, size):
        moved = roll(v, start - source, 1)
        return jnp.where((at >= start) & (at < start + size), moved, 0.0)

    for x in range(long):
        boxes = [gath[pl.ds(z * spots, spots), x, :] for z in range(nz)]
        for y in range(deep):
            fit = reach if y < deep - 1 else cut
            v = sum(window(boxes[z], reach * y, cz * z, fit) for z in range(nz))
            if fit < reach:
                v += sum(window(spares[z], rest * x, cz * z + cut, rest) for z in range(nz))
            parts_s[pl.ds((y * long + x) * spots, spots), :] = v

    def dot(a, b):
        return jnp.dot(a, b, precision=lax.Precision.HIGHEST, preferred_element_type=jnp.float32)

    grid = parts_s[...]
    loads[2 + TABLES].wait()
    loads[3 + TABLES].wait()
    half3, half4 = dot(k_s[0], grid), dot(k_s[1], grid)
    grid, grid4 = dot(half3, l_s[0]), dot(half4, l_s[1])
    row = iota(grid.shape, 0)
    lane = iota(grid.shape, 1)
    inner_row = row % count
    gx, gy, gz = inner_row // cy, inner_row % cy, lane // step
    valid = lane % step < nz
    even3 = (gx % 2 == 0) & (gy % 2 == 0) & (gz % 2 == 0)
    even4 = (gx % 4 == 0) & (gy % 4 == 0) & (gz % 4 == 0)
    det3 = valid & ~even3
    det4 = valid & even3 & ~even4
    small3 = shrink(grid, thresh(FINE))
    small4 = shrink(grid4, thresh(FINE + 1))
    final_s[...] = jnp.where(even3, jnp.where(even4, grid4, small4), small3)

    def masked(mask, v):
        return total(jnp.where(mask, v, 0.0))

    coarse = ((masked(det3, grid * grid), masked(det3, jnp.abs(small3))),
              (masked(det4, grid4 * grid4), masked(det4, jnp.abs(small4))))
    first = pl.multiple_of((me[0] * ny + me[1]) * count, count)
    mine = pltpu.roll(final_s[pl.ds(first, count), :], lax.rem(LANES - me[2], LANES), 1)
    keep = iota((cy, LANES), 1) % step == 0
    for x in range(cx):
        spot = (0, step * x, pl.ds(0, cy, stride=step), slice(None))
        out[spot] = jnp.where(keep, mine[x * cy : x * cy + cy], out[spot])

    settle(tallies.at[pl.ds(0, ndev - 1)], t_send, t_recv)
    tail = jnp.sum(tallies[...], axis=0)
    for q in (0, 1):
        line = jnp.zeros((1, LANES), jnp.float32)
        for level in range(LEVELS):
            weight = 8.0 ** (level + 1) / (7.0 * cells)
            if level < FINE:
                value = jnp.sum(jnp.where(one == 2 * level + q, tail, 0.0), axis=1, keepdims=True)
            else:
                value = coarse[level - FINE][q]
            line = jnp.where(one == level, value * weight, line)
        stats[q] = line[:, 0:LEVELS]


def deliver(held, held_stats, out, stats, sem):
    rows = held.shape[1] // CHUNKS
    copies = [pltpu.make_async_copy(held_stats, stats, sem.at[CHUNKS])]
    for i in range(CHUNKS):
        part = pl.ds(i * rows, rows)
        copies.append(pltpu.make_async_copy(held.at[:, part], out.at[:, part], sem.at[i]))
    for copy in copies:
        copy.start()
    for copy in copies:
        copy.wait()


def shards(sizes, fields, exponents):
    nx, ny, nz = sizes
    ndev = nx * ny * nz
    _, lx, ly, lz = fields.shape
    cells = fields.size * ndev
    step = 2**FINE
    coarse = (lx // step, ly // step, lz // step)
    count = coarse[0] * coarse[1]
    tables = coarse_matrices(sizes, coarse)
    middle = middle_tables(lx // 2, ly // 2, lz // 2)
    own, extra = lx // 2 * (ly // 2), middle[0].shape[0]
    middle = fine_tables(lx) + reach_tables(lx // 2, ly // 2, lz // 2) + middle
    scratch = [
        *(pltpu.VMEM(shape, jnp.float32) for shape in (
            (2, ly, LANES), (2, ly, LANES), (2, lx, LANES), (2, lx, LANES), (4, 1, LANES), (4, 1, LANES),
            (2, lx, LANES), (ly, LANES), (2, ly, LANES), (2, 1, LANES), (4, 1, LANES), (2, 2, LANES),
            (2, 2, 2, LANES), (2, 2, 2, 2, LANES), (ly, LANES), (lx, ly, LANES),
        )),
        pltpu.SemaphoreType.DMA,
        pltpu.SemaphoreType.DMA,
        *(pltpu.VMEM(shape, jnp.float32) for shape in (
            (own + extra, LANES), (extra, LANES), (2, 2, own + 2 * LANES), (2, 2, own + 2 * LANES),
            (2, 4, 2, LANES), (2, 2, 2, 2, LANES), (own, LANES), (lx // 4, ly // 4, LANES),
        )),
        pltpu.SemaphoreType.DMA,
        pltpu.SemaphoreType.DMA,
    ]
    scratch += [
        pltpu.VMEM((ndev, 8, LANES), jnp.float32),
        pltpu.VMEM((8, LANES), jnp.float32),
        pltpu.VMEM((tables[0].shape[2], LANES), jnp.float32),
        pltpu.VMEM((nx * ny * count, LANES), jnp.float32),
        pltpu.VMEM((1, LANES), jnp.float32),
        pltpu.VMEM((ndev, 1, LANES), jnp.float32),
        *[pltpu.SemaphoreType.DMA] * 4,
        pltpu.VMEM(fields.shape, jnp.float32),
        pltpu.SMEM(exponents.shape, jnp.int32),
        pltpu.VMEM(tables[0].shape, jnp.float32),
        pltpu.VMEM(tables[1].shape, jnp.float32),
        pltpu.SemaphoreType.DMA((4 + TABLES,)),
        *(pltpu.VMEM(table.shape, table.dtype) for table in middle),
    ]
    vmem = pl.BlockSpec(memory_space=pltpu.VMEM)
    held = pl.pallas_call(
        functools.partial(kernel, sizes, cells),
        out_shape=(
            pltpu.VMEM(fields.shape, jnp.float32),
            pltpu.VMEM((2, 1, LEVELS), jnp.float32),
        ),
        in_specs=[pl.BlockSpec(memory_space=pltpu.HBM)] * (4 + TABLES),
        out_specs=(vmem, vmem),
        scratch_shapes=scratch,
        compiler_params=pltpu.CompilerParams(
            collective_id=0, has_side_effects=True, vmem_limit_bytes=VMEM_LIMIT
        ),
    )(*(pltpu.with_memory_space_constraint(x, pltpu.HBM) for x in (exponents, fields, *map(jnp.asarray, (*tables, *middle)))))
    hbm = pl.BlockSpec(memory_space=pltpu.HBM)
    return pl.pallas_call(
        deliver,
        out_shape=(
            jax.ShapeDtypeStruct(fields.shape, jnp.float32),
            jax.ShapeDtypeStruct((2, 1, LEVELS), jnp.float32),
        ),
        in_specs=(vmem, vmem),
        out_specs=(hbm, hbm),
        scratch_shapes=[pltpu.SemaphoreType.DMA((CHUNKS + 1,))],
    )(*(pltpu.with_memory_space_constraint(x, pltpu.VMEM) for x in held))


def solution(mesh):
    sizes = tuple(mesh.shape[name] for name in ("gx", "gy", "gz"))
    placed = (P(None, "gx", "gy", "gz"), P())
    return jax.shard_map(
        functools.partial(shards, sizes),
        mesh=mesh,
        in_specs=placed,
        out_specs=placed,
        check_vma=False,
    )
```

```python
import functools

import numpy as np

import jax
import jax.numpy as jnp
from jax import lax
from jax.experimental import pallas as pl
from jax.experimental.pallas import tpu as pltpu
from jax.sharding import PartitionSpec as P

FINE = 3
LEVELS = 5
LANES = 128
CHUNKS = 4
BUFFERS = 18
TABLES = 12
BATCH = 8
ROUNDS = 2
VMEM_LIMIT = 58_720_256
MESH = pl.DeviceIdType.MESH


def periodic_lift(length):
    eye = np.eye(length)
    even, odd = eye[0::2], eye[1::2]
    detail = odd - 0.5 * (even + np.roll(even, -1, 0))
    smooth = even + 0.25 * (np.roll(detail, 1, 0) + detail)
    whole = np.zeros((length, length))
    whole[0::2] = smooth
    whole[1::2] = detail
    return whole


def second_lift(length):
    whole = np.zeros((length, length))
    whole[0::2, 0::2] = periodic_lift(length // 2)
    return whole


def coarse_matrices(sizes, coarse):
    nx, ny, nz = sizes
    cx, cy, cz = coarse
    rows = np.arange(nx * ny * cx * cy)
    dev, inner = rows // (cx * cy), rows % (cx * cy)
    gx = (dev // ny) * cx + inner // cy
    gy = (dev % ny) * cy + inner % cy
    step = LANES // cz
    lanes = np.array([z * step + d for d in range(nz) for z in range(cz)])
    reach_y, reach_x, spot = np.indices((cy + 3, cx + 3, nx * ny)).reshape(3, -1)
    from_x = (spot // ny * cx + reach_x - 1) % (nx * cx)
    from_y = (spot % ny * cy + reach_y - 1) % (ny * cy)
    from_z = np.arange(-1, nz * cz + 2) % (nz * cz)
    result = []
    for both_levels in (False, True):
        mx, my, mz = periodic_lift(nx * cx), periodic_lift(ny * cy), periodic_lift(nz * cz)
        if both_levels:
            mx, my, mz = second_lift(nx * cx) @ mx, second_lift(ny * cy) @ my, second_lift(nz * cz) @ mz
        both = mx[gx[:, None], from_x[None]] * my[gy[:, None], from_y[None]]
        along = np.zeros((LANES, LANES))
        along[np.ix_(np.arange(len(from_z)), lanes)] = mz[:, from_z].T
        result.append((both.astype(np.float32), along.astype(np.float32)))
    return [np.stack(pair) for pair in zip(*result)]


def cut_table(table):
    high = table.astype(jnp.bfloat16)
    low = (table - high.astype(np.float64)).astype(jnp.bfloat16)
    return high, low


def reach_line(n):
    twice = periodic_lift(3 * n // 2)[0::2] @ periodic_lift(3 * n)[0::2]
    return twice[n // 4 - 1 : n // 2 + 2, n : 2 * n]


def reach_tables(ax, ay, az):
    part_x, part_y, part_z = reach_line(ax), reach_line(ay), reach_line(az)
    wide, deep = len(part_z), len(part_y)
    rows = np.zeros((deep, 8, ax * ay))
    rows[:, : len(part_x)] = np.einsum("yb,xa->yxab", part_y, part_x).reshape(deep, -1, ax * ay)
    rows = rows.reshape(8 * deep, -1)
    along = np.zeros((deep + 1, LANES, LANES))
    for y in range(deep):
        fit = min(wide, LANES - wide * y)
        along[y, :: LANES // az, wide * y : wide * y + fit] = part_z[:fit].T
    along[deep, :: LANES // az, : wide - fit] = part_z[fit:].T
    return np.concatenate(cut_table(rows)), along.reshape(-1, LANES).astype(jnp.bfloat16)


def lift_line(n):
    whole = np.zeros((n, n + 2))
    cells = np.eye(n + 2)
    even, odd = cells[0:n:2], cells[1:n:2]
    after = np.concatenate((even[1:], cells[n + 1 :]))
    detail = odd - 0.5 * (even + after)
    before = np.concatenate((cells[n : n + 1] - 0.5 * even[:1], detail[:-1]))
    whole[0::2] = even + 0.25 * (before + detail)
    whole[1::2] = detail
    return whole

def line_tables(n):
    lift = lift_line(n)
    own = lift[:, :n]
    sent = np.zeros((4, n))
    sent[0, n - 1], sent[0, n - 2] = 1.0, -0.5
    sent[1] = own[n - 2] - 0.5 * own[n - 4]
    sent[2, 0] = 1.0
    sent[3] = own[0]
    first = np.zeros((n + 2, n + 4))
    first[:n, :n] = own
    first[:n, n], first[:n, n + 2] = lift[:, n], lift[:, n + 1]
    first[n, n + 1], first[n, 0] = 1.0, lift[n - 2, n + 1]
    first[n + 1, n + 3] = 1.0
    first[n + 1, :n] = lift[0, n] * sent[0]
    return sent, first, lift_line(n // 2)


def fine_tables(px):
    q = LANES // px
    ends = np.zeros((2, px))
    ends[0, px - 1], ends[0, px - 2], ends[1, 0] = 1.0, -0.5, 1.0
    edges = np.zeros((8, LANES))
    place = np.zeros((16, LANES))
    for z in range(2):
        for x in range(2):
            edges[2 * z + x, 1 + z :: q] = ends[x]
            for part in range(3):
                place[4 * part + 2 * z + x, (LANES - q) * x + 1 + z] = 1.0
    result = (lift_line(LANES)[:, :LANES].T, edges, place)
    return tuple(table.astype(jnp.bfloat16) for table in result)


def middle_tables(ax, ay, az):
    step = LANES // az
    sent_x, first_x, second_x = line_tables(ax)
    sent_y, first_y, second_y = line_tables(ay)
    sent_z, first_z, second_z = line_tables(az)
    own = [(x, y) for x in range(ax) for y in range(ay)]
    corners = [(x, 2 * g + y) for g in range(2) for x in range(4) for y in range(2)]
    extra = []
    for start in range(2):
        extra += [(ax + k, y) for k in (start, start + 2) for y in range(ay)]
        extra += [(x, ay + k) for k in (start, start + 2) for x in range(ax)]
    extra += [(ax + x, ay + y) for x, y in corners]
    taken = np.array(own + extra)
    given = own + [(ax + k, y) for k in range(2) for y in range(0, ay, 2)]
    given += [(x, ay + k) for k in range(2) for x in range(0, ax, 2)]
    given += [(ax + x, ay + y) for x in range(2) for y in range(2)]
    height = -(-len(given) // 16) * 16

    whole_x, whole_y = np.concatenate((np.eye(ax), sent_x)), np.concatenate((np.eye(ay), sent_y))
    ex, ey = np.array(extra).T
    ox, oy = np.array(own).T
    send_rows = whole_x[np.ix_(ex, ox)] * whole_y[np.ix_(ey, oy)]
    gx, gy = np.array(given).T
    tx, ty = taken.T
    rows = np.zeros((height, len(taken)))
    rows[: len(given)] = first_x[np.ix_(gx, tx)] * first_y[np.ix_(gy, ty)]

    def spot(at, n):
        return np.where(at >= n, n // 2 + at - n, at // 2)

    half = np.array([(x, y) for x in range(ax // 2) for y in range(ay // 2)])
    use = ((gx % 2 == 0) | (gx >= ax)) & ((gy % 2 == 0) | (gy >= ay))
    last = np.zeros((len(half), height))
    pick_x = second_x[np.ix_(half[:, 0], spot(gx, ax))]
    pick_y = second_y[np.ix_(half[:, 1], spot(gy, ay))]
    last[:, : len(given)] = pick_x * pick_y * use

    lanes = np.arange(az) * step
    out = np.concatenate((lanes, [1, step + 1]))
    send_lanes = np.zeros((8, LANES))
    send_lanes[np.ix_(np.arange(4), lanes)] = sent_z
    along = np.zeros((LANES, LANES))
    along[np.ix_(lanes, out)] = first_z[:, :az].T
    rim = np.zeros((16, LANES))
    for part in range(3):
        rim[np.ix_(4 * part + np.arange(4), out)] = first_z[:, az:].T
    along_last = np.zeros((LANES, LANES))
    source = np.concatenate((lanes[0::2], [1, step + 1]))
    along_last[np.ix_(source, lanes[0::2])] = second_z.T
    last = np.concatenate(cut_table(last @ rows))
    along = np.concatenate((along, along @ along_last), axis=1)
    rim = np.concatenate((rim, rim @ along_last), axis=1)
    result = (send_rows, rows[: len(own)], last, send_lanes, along, np.roll(along, 1, 0), rim)
    return tuple(table.astype(jnp.bfloat16) for table in result)


def iota(shape, axis):
    return lax.broadcasted_iota(jnp.int32, shape, axis)


def roll(values, shift, axis):
    return pltpu.roll(values, shift % values.shape[axis], axis)


def lift_rows(v, low, high):
    n = v.shape[0]
    row = iota(v.shape, 0)
    odd = row % 2 == 1
    up = jnp.where(row == n - 1, high, roll(v, -1, 0))
    w = jnp.where(odd, v - 0.5 * (roll(v, 1, 0) + up), v)
    down = jnp.where(row == 0, low - 0.5 * v, roll(w, 1, 0))
    return jnp.where(odd, w, w + 0.25 * (down + roll(w, -1, 0)))


def lift_groups(v, rim, s):
    lane = iota(v.shape, 1)
    odd = (lane // s) % 2 == 1
    up = jnp.where(lane >= LANES - s, rim, roll(v, -s, 1))
    w = jnp.where(odd, v - 0.5 * (roll(v, s, 1) + up), v)
    down = jnp.where(lane < s, rim - 0.5 * v, roll(w, s, 1))
    return jnp.where(odd, w, w + 0.25 * (down + roll(w, -s, 1)))


def shrink(v, thresh):
    return v - jnp.clip(v, -thresh, thresh)


def three(v):
    parts = []
    for _ in range(3):
        parts.append(v.astype(jnp.bfloat16))
        v = v - parts[-1].astype(jnp.float32)
    return parts


def mix(a, b, dims):
    return lax.dot_general(a, b, (dims, ((), ())), preferred_element_type=jnp.float32)


def mix_rows(table, v):
    wide = mix(table, jnp.concatenate(three(v), axis=1), ((1,), (0,)))
    return wide[:, :LANES] + wide[:, LANES : 2 * LANES] + wide[:, 2 * LANES :]


def doubled(v, n):
    return v[0:n] + v[n:]


def mix_lanes(v, table):
    return mix(jnp.concatenate(three(v), axis=1), jnp.concatenate([table] * 3, axis=0), ((1,), (0,)))


def total(v):
    return jnp.sum(jnp.sum(v, axis=0, keepdims=True), axis=1, keepdims=True)


def kernel(sizes, cells, exps_in, field_in, rows_in, lanes_in, *rest):
    tables_in, (out, stats), scratch = rest[:TABLES], rest[TABLES : TABLES + 2], rest[TABLES + 2 :]
    nx, ny, nz = sizes
    ndev = nx * ny * nz
    scratch = list(scratch)
    tables = scratch[-TABLES:]
    scratch = scratch[:-TABLES]
    field, exps, k_s, l_s, in_sem = scratch[-5:]
    scratch = scratch[:-5]
    pairs = [(field_in, field), (exps_in, exps), *zip(tables_in, tables), (rows_in, k_s), (lanes_in, l_s)]
    loads = [pltpu.make_async_copy(a, b, in_sem.at[i]) for i, (a, b) in enumerate(pairs)]
    me = (lax.axis_index("gx"), lax.axis_index("gy"), lax.axis_index("gz"))

    def device(dx, dy, dz):
        return (
            lax.rem(me[0] + (dx + nx), nx),
            lax.rem(me[1] + (dy + ny), ny),
            lax.rem(me[2] + (dz + nz), nz),
        )

    def distance(spot):
        return sum(min(d, size - d) for d, size in zip(spot, sizes))

    def thresh(level):
        return jnp.exp2(jnp.full((1, LANES), exps[level].astype(jnp.float32)))

    def split(j):
        return j // (ny * nz), (j // nz) % ny, j % nz

    def launch(copies, send_sem, recv_sem):
        flights = [
            pltpu.make_async_remote_copy(
                src_ref=f, dst_ref=t, send_sem=send_sem, recv_sem=recv_sem,
                device_id=device(*d), device_id_type=MESH,
            )
            for f, t, d in copies
        ]
        for flight in flights:
            flight.start()
        return sum(t.size for _, t, _ in copies) // LANES

    def settle(span, send_sem, recv_sem):
        for sem in (recv_sem, send_sem):
            pltpu.make_async_copy(span, span, sem).wait()

    barrier = pltpu.get_barrier_semaphore()

    near = max(sizes) // 2 <= ROUNDS
    greeted = {
        tuple((d + size - 1) % size if near else d for d, size in zip(spot, sizes))
        for spot in np.ndindex(*(3, 3, 3) if near else sizes)
    } - {(0, 0, 0)}
    for spot in sorted(greeted, key=lambda spot: (-distance(spot), spot)):
        pl.semaphore_signal(barrier, inc=1, device_id=device(*spot), device_id_type=MESH)
    for load in loads:
        load.start()
    gath, msg, parts_s, final_s, tally_s, tallies, g_send, g_recv, t_send, t_recv = scratch[-10:]
    loads[0].wait()
    loads[1].wait()
    step_to = (1, -1)
    alone = nx == 2
    ways = (0,) if alone else (0, 1)
    (xs, xr, ys, yr, es, er, yl, zs, zr, ds, dr, ts, txr, tcr, rim, work, send_sem, recv_sem) = scratch[:BUFFERS]
    grown, sent, side, hz, t2r, t3r, o1s, o2s, m_send, m_recv = scratch[BUFFERS : BUFFERS + 10]
    fine_lanes, fine_edges, fine_place, reach_rows, reach_lanes, *tables = tables
    src = field.at[0]
    px, n = src.shape[0], src.shape[1]
    half, q = n // 2, LANES // px
    lane = iota((n, LANES), 1)
    row8 = iota((8, LANES), 0)

    def ends(v):
        return v[n - 1 : n] - 0.5 * v[n - 2 : n - 1], v[0:1]

    def under(pair):
        return jnp.where(row8 == 0, pair[0], jnp.where(row8 == 1, pair[1], 0.0))

    planes = (src[px - 1] - 0.5 * src[px - 2], src[0])
    ys[0] = src[:, n - 1, :] - 0.5 * src[:, n - 2, :]
    ys[1] = src[:, 0, :]
    for gx in (0, 1):
        xs[gx] = planes[gx]
        es[2 * gx], es[2 * gx + 1] = ends(planes[gx])
    packed = jnp.zeros((n, LANES), jnp.float32)
    for x in range(px):
        packed = jnp.where(lane // q == x, roll(src[x], q * x + 2, 1), packed)
    packed = jnp.where(lane % q == 1, packed - 0.5 * roll(packed, 1, 1), packed)
    zs[...] = packed
    ds[0], ds[1] = ends(packed)
    for load in loads[2:5]:
        load.wait()
    edges = sum(
        mix(fine_edges[...], part, ((1,), (1,)))
        for part in three(jnp.concatenate((packed, under(ends(packed))), axis=0))
    )
    ts[...] = jnp.zeros(ts.shape, jnp.float32)
    for g in (0, 1):
        ts[g, :, pl.ds(0, n + 8)] = edges[2 * g : 2 * g + 2]

    pl.semaphore_wait(barrier, len(greeted))
    copies = []
    for g in (0, 1):
        dz = step_to[g]
        for gx in ways:
            for gy in (0, 1):
                copies.append((ts.at[g], tcr.at[g, gy, gx], (step_to[gx], step_to[gy], dz)))
            copies.append((ts.at[g], txr.at[g, gx], (step_to[gx], 0, dz)))
        for gy in (0, 1):
            copies.append((ds.at[gy], dr.at[2 * g + gy], (0, step_to[gy], dz)))
    for gx in (0, 1):
        for gy in (0, 1):
            copies.append((es.at[2 * gx + gy], er.at[2 * gx + gy], (step_to[gx], step_to[gy], 0)))
    for g in (0, 1):
        copies.append((xs.at[g], xr.at[g], (step_to[g], 0, 0)))
    for g in (0, 1):
        copies.append((ys.at[g], yr.at[g], (0, step_to[g], 0)))
    for g in (0, 1):
        copies.append((zs, zr.at[g], (0, 0, step_to[g])))
    sent_rows = launch(copies, send_sem, recv_sem)
    settle(grown.at[pl.ds(0, sent_rows)], send_sem, recv_sem)

    lane2, row2 = iota((2, LANES), 1), iota((2, LANES), 0)
    for g in (0, 1):
        yl[g] = lift_rows(yr[g], er[g], er[2 + g])

    def both(ref):
        return ref[0] if alone else jnp.where(row2 == 0, ref[0], ref[1])

    def columns(top, table):
        pieces = [part.astype(jnp.float32) for part in three(top)]
        pieces.append(jnp.zeros_like(top))
        return mix(jnp.concatenate(pieces, axis=0).astype(jnp.bfloat16), table, ((0,), (0,)))

    tops = []
    for g in (0, 1):
        v = jnp.where(lane2 == n, both(tcr.at[g, 0]), both(tcr.at[g, 1]))
        v = jnp.where(lane2 < n, both(txr.at[g]), v)
        tops.append(jnp.where(lane2 < n + 2, v, 0.0))
    beside = columns(jnp.concatenate(tops, axis=0), fine_place[...])[0 : n + 8]

    def kinds(a, b):
        return jnp.where(iota(a.shape, 1) % q == 1, a, b)

    lower = under((kinds(dr[0], dr[2]), kinds(dr[1], dr[3])))
    v = lift_groups(jnp.concatenate((kinds(zr[0], zr[1]), lower), axis=0), beside, q)
    v = lift_rows(v[0:n], v[n : n + 1], v[n + 1 : n + 2])
    v = jnp.where(lane % q == 2, roll(v, 1, 1), jnp.where(lane % q == 1, roll(v, -1, 1), roll(v, -2, 1)))
    rim[...] = v
    border = jnp.concatenate((rim[pl.ds(0, half, stride=2), :], rim[pl.ds(1, half, stride=2), :]), axis=0)
    share = jnp.where(lane == LANES - 1, -0.5, jnp.where(lane == LANES - 2, -0.125, jnp.where(lane == 0, 0.25, 0.0)))
    level_thresh = thresh(0)
    inner = (iota((n, LANES), 0) < half) & (lane % 2 == 0)
    row = iota((half, LANES), 0)

    def halves(ref, x):
        return [ref[x, pl.ds(start, half, stride=2), :] for start in (0, 1)]

    def lift_halves(v, x):
        even, odd = v
        after = jnp.where(row == half - 1, yl[1, x : x + 1, :], roll(even, -1, 0))
        detail = odd - 0.5 * (even + after)
        before = jnp.where(row == 0, yl[0, x : x + 1, :] - 0.5 * even, roll(detail, 1, 0))
        return [even + 0.25 * (before + detail), detail]

    even = halves(src, 0)
    before = [p - 0.5 * e for p, e in zip(halves(xr, 0), even)]
    stack = []
    for k in range(px // 2):
        after = halves(src, 2 * k + 2) if 2 * k + 2 < px else halves(xr, 1)
        detail = [o - 0.5 * (e + a) for o, e, a in zip(halves(src, 2 * k + 1), even, after)]
        smooth = [e + 0.25 * (b + d) for e, b, d in zip(even, before, detail)]
        stack += lift_halves(smooth, 2 * k) + lift_halves(detail, 2 * k + 1)
        even, before = after, detail
        if len(stack) == 2 * BATCH:
            wide = mix_lanes(jnp.concatenate(stack, axis=0), fine_lanes[...])
            for i in range(BATCH):
                x = 2 * k + 2 - BATCH + i
                v = wide[n * i : n * i + n] + roll(border, LANES - 2 - q * x, 1) * share
                work[x] = v
                if x % 2 == 0:
                    grown[pl.ds(x // 2 * half, half), :] = v[0:half]
            stack = []

    def finish():
        energy = kept = jnp.zeros((n, LANES), jnp.float32)
        for x in range(px):
            v = work[x]
            small = shrink(v, level_thresh)
            if x % 2 == 0:
                energy += jnp.where(inner, 0.0, v * v)
                kept += jnp.where(inner, 0.0, jnp.abs(small))
            else:
                energy += v * v
                kept += jnp.abs(small)
            for start in (0, 1):
                out[0, x, pl.ds(start, half, stride=2), :] = small[half * start : half * start + half]
        return [total(energy), total(kept)]

    ax, ay = px // 2, n // 2
    own = ax * ay
    send_rows, rows1, rows2, send_lanes, lanes12, odd_lanes12, rim12 = tables
    for load in loads[5 : 2 + TABLES]:
        load.wait()
    here = grown[0:own]
    halo = mix_rows(send_rows[...], here)
    px_rows, py_rows = 2 * ay, 2 * ax
    pair = px_rows + py_rows
    second_kind = roll(halo[pair : 2 * pair], 1, 1)
    sent[0:pair] = jnp.where(iota(second_kind.shape, 1) % 2 == 0, halo[0:pair], second_kind)
    sent[pair:] = halo[2 * pair :]
    edges = sum(
        mix(send_lanes[...], part, ((1,), (1,)))
        for part in three(jnp.concatenate((here, halo), axis=0))
    )
    extra = halo.shape[0]
    for g in (0, 1):
        side[g, :, pl.ds(own, 2 * LANES)] = jnp.zeros((2, 2 * LANES), jnp.float32)
        side[g, :, pl.ds(0, own + extra)] = edges[2 * g : 2 * g + 2]

    copies = []
    for g in (0, 1):
        dz = step_to[g]
        tail = pl.ds(own + LANES, LANES)
        for gy in (0, 1):
            for gx in ways:
                copies.append((side.at[g, :, tail], t3r.at[g, gy, gx], (step_to[gx], step_to[gy], dz)))
        middle = pl.ds(own, LANES)
        for gx in ways:
            copies.append((side.at[g, :, middle], t2r.at[g, gx], (step_to[gx], 0, dz)))
        for gy in (0, 1):
            copies.append((side.at[g, :, middle], t2r.at[g, 2 + gy], (0, step_to[gy], dz)))
        copies.append((side.at[g, :, pl.ds(0, own)], hz.at[g, :, pl.ds(0, own)], (0, 0, dz)))

    def rows_copy(start, size, to):
        copies.append((sent.at[pl.ds(start, size)], grown.at[pl.ds(own + start, size)], to))

    parts = len(ways)
    for gy in (0, 1):
        for gx in ways:
            rows_copy(pair + 8 * gy + 4 * gx, 8 // parts, (step_to[gx], step_to[gy], 0))
    for gx in ways:
        rows_copy(px_rows // 2 * gx, px_rows // parts, (step_to[gx], 0, 0))
    for gy in (0, 1):
        rows_copy(px_rows + py_rows // 2 * gy, py_rows // 2, (0, step_to[gy], 0))
    sent_rows = launch(copies, m_send, m_recv)

    spots = nx * ny
    slot = (me[2] * nx + me[0]) * ny + me[1]
    cx, cy, cz = ax // 4, ay // 4, LANES // 2**FINE
    step = 2**FINE
    count = cx * cy
    long, deep, reach = cx + 3, cy + 3, cz + 3
    cut = LANES - reach * (deep - 1)
    rest = reach - cut

    def spread(source, target, send_sem, recv_sem):
        def post(j):
            return pltpu.make_async_remote_copy(
                src_ref=source, dst_ref=target, send_sem=send_sem, recv_sem=recv_sem,
                device_id=device(*split(j)), device_id_type=MESH,
            )

        def send(j, carry):
            post(j).start()
            return carry

        if ndev <= 32:
            for j in sorted(range(1, ndev), key=lambda j: (-distance(split(j)), j)):
                post(j).start()
        else:
            lax.fori_loop(1, ndev, send, 0)

    pieces = mix_rows(reach_rows[...], here)
    pieces = doubled(pieces, 8 * deep)
    blocks = [part.astype(jnp.float32) for part in three(pieces)]

    def stack(first, last):
        rows = [jnp.concatenate([b[8 * y : 8 * y + 8] for y in range(first, last)], axis=1) for b in blocks]
        return jnp.concatenate(rows + [jnp.zeros_like(rows[0])], axis=0).astype(jnp.bfloat16)

    def fold(v):
        return v[0:8] + v[8:16] + v[16:24]

    sheet = fold(mix(stack(0, deep), reach_lanes[pl.ds(0, deep * LANES), :], ((1,), (0,))))
    loose = fold(mix(stack(deep - 1, deep), reach_lanes[pl.ds(deep * LANES, LANES), :], ((1,), (0,))))
    spare = loose[0:1]
    for x in range(1, long):
        spare += roll(loose[x : x + 1], rest * x, 1)
    msg[...] = jnp.where(row8 == long, spare, sheet)
    spread(msg, gath.at[slot], g_send, g_recv)
    gath[slot] = msg[...]
    sums = finish()
    quarter = own // 4

    def level_rows(v, columns):
        return (
            mix_rows(rows1[:, columns], v[:, 0:LANES]),
            doubled(mix_rows(rows2[:, columns], v[:, LANES:]), quarter),
        )

    o1s[...], early = level_rows(mix_lanes(here, lanes12[...]), pl.ds(0, own))
    o2s[...] = early.reshape(o2s.shape)
    settle(grown.at[pl.ds(0, sent_rows)], m_send, m_recv)

    for g in (0, 1):
        place_in = lane2 % pair
        v = jnp.where(place_in < ay, t2r[g, 0], t2r[g, 0 if alone else 1])
        v = jnp.where(place_in < px_rows, v, jnp.where(place_in < px_rows + ax, t2r[g, 2], t2r[g, 3]))
        hz[g, :, pl.ds(own, LANES)] = v
        u = []
        for gy in (0, 1):
            u.append(jnp.where(lane2 % 8 < 4, t3r[g, gy, 0], t3r[g, gy, 0 if alone else 1]))
        v = jnp.where(lane2 < 8, u[0], u[1])
        hz[g, :, pl.ds(own + LANES, LANES)] = jnp.where(lane2 < 16, v, 0.0)
    rim_rows = columns(jnp.concatenate((hz[0], hz[1]), axis=0), rim12[...])
    got = grown[pl.ds(own, pair + 16), :]
    outer = mix_lanes(got, lanes12[...])
    outer = (outer[0:pair], mix_lanes(got[0:pair], odd_lanes12[...]), outer[pair:])
    outer = jnp.concatenate(outer, axis=0) + rim_rows[own : own + extra]
    late = level_rows(jnp.concatenate((rim_rows[0:own], outer), axis=0), pl.ds(0, own + extra))
    first = o1s[...] + late[0]
    second = o2s[...].reshape(quarter, LANES) + late[1]
    o1s[...] = first
    o2s[...] = second.reshape(o2s.shape)

    def tally(v, level, ny):
        s = 2**level
        row, at = iota(v.shape, 0), iota(v.shape, 1)
        smooth = ((row // ny) % 2 == 0) & (row % 2 == 0) & (at % (2 * s) == 0)
        use = (at % s == 0) & ~smooth
        small = shrink(v, thresh(level))
        return [total(jnp.where(use, v * v, 0.0)), total(jnp.where(use, jnp.abs(small), 0.0))]

    sums += tally(first, 1, ay) + tally(second, 2, ay // 2)

    def place(source, level):
        s = 2**level
        small_y = ay >> (level - 1)
        keep = iota((small_y, LANES), 1) % s == 0
        for x in range(ax >> (level - 1)):
            spot = (0, s * x, pl.ds(0, small_y, stride=s), slice(None))
            out[spot] = jnp.where(keep, shrink(source(x), thresh(level)), out[spot])

    one = iota((1, LANES), 1)
    tail = jnp.zeros((1, LANES), jnp.float32)
    for i, whole in enumerate(sums):
        tail = jnp.where(one == i, whole, tail)
    tally_s[...] = tail
    spread(tally_s, tallies.at[slot], t_send, t_recv)
    tallies[slot] = tail
    place(lambda x: o1s[pl.ds(x * ay, ay), :], 1)
    place(lambda x: o2s[x], 2)
    settle(gath.at[pl.ds(0, ndev - 1)], g_send, g_recv)

    at = iota((spots, LANES), 1)
    spares = [gath[pl.ds(z * spots, spots), long, :] for z in range(nz)]

    def window(v, source, start, size):
        moved = roll(v, start - source, 1)
        return jnp.where((at >= start) & (at < start + size), moved, 0.0)

    for x in range(long):
        boxes = [gath[pl.ds(z * spots, spots), x, :] for z in range(nz)]
        for y in range(deep):
            fit = reach if y < deep - 1 else cut
            v = sum(window(boxes[z], reach * y, cz * z, fit) for z in range(nz))
            if fit < reach:
                v += sum(window(spares[z], rest * x, cz * z + cut, rest) for z in range(nz))
            parts_s[pl.ds((y * long + x) * spots, spots), :] = v

    def dot(a, b):
        return jnp.dot(a, b, precision=lax.Precision.HIGHEST, preferred_element_type=jnp.float32)

    grid = parts_s[...]
    loads[2 + TABLES].wait()
    loads[3 + TABLES].wait()
    half3, half4 = dot(k_s[0], grid), dot(k_s[1], grid)
    grid, grid4 = dot(half3, l_s[0]), dot(half4, l_s[1])
    row = iota(grid.shape, 0)
    lane = iota(grid.shape, 1)
    inner_row = row % count
    gx, gy, gz = inner_row // cy, inner_row % cy, lane // step
    valid = lane % step < nz
    even3 = (gx % 2 == 0) & (gy % 2 == 0) & (gz % 2 == 0)
    even4 = (gx % 4 == 0) & (gy % 4 == 0) & (gz % 4 == 0)
    det3 = valid & ~even3
    det4 = valid & even3 & ~even4
    small3 = shrink(grid, thresh(FINE))
    small4 = shrink(grid4, thresh(FINE + 1))
    final_s[...] = jnp.where(even3, jnp.where(even4, grid4, small4), small3)

    def masked(mask, v):
        return total(jnp.where(mask, v, 0.0))

    coarse = ((masked(det3, grid * grid), masked(det3, jnp.abs(small3))),
              (masked(det4, grid4 * grid4), masked(det4, jnp.abs(small4))))
    first = pl.multiple_of((me[0] * ny + me[1]) * count, count)
    mine = pltpu.roll(final_s[pl.ds(first, count), :], lax.rem(LANES - me[2], LANES), 1)
    keep = iota((cy, LANES), 1) % step == 0
    for x in range(cx):
        spot = (0, step * x, pl.ds(0, cy, stride=step), slice(None))
        out[spot] = jnp.where(keep, mine[x * cy : x * cy + cy], out[spot])

    settle(tallies.at[pl.ds(0, ndev - 1)], t_send, t_recv)
    tail = jnp.sum(tallies[...], axis=0)
    for q in (0, 1):
        line = jnp.zeros((1, LANES), jnp.float32)
        for level in range(LEVELS):
            weight = 8.0 ** (level + 1) / (7.0 * cells)
            if level < FINE:
                value = jnp.sum(jnp.where(one == 2 * level + q, tail, 0.0), axis=1, keepdims=True)
            else:
                value = coarse[level - FINE][q]
            line = jnp.where(one == level, value * weight, line)
        stats[q] = line[:, 0:LEVELS]


def deliver(held, held_stats, out, stats, sem):
    rows = held.shape[1] // CHUNKS
    copies = [pltpu.make_async_copy(held_stats, stats, sem.at[CHUNKS])]
    for i in range(CHUNKS):
        part = pl.ds(i * rows, rows)
        copies.append(pltpu.make_async_copy(held.at[:, part], out.at[:, part], sem.at[i]))
    for copy in copies:
        copy.start()
    for copy in copies:
        copy.wait()


def shards(sizes, fields, exponents):
    nx, ny, nz = sizes
    ndev = nx * ny * nz
    _, lx, ly, lz = fields.shape
    cells = fields.size * ndev
    step = 2**FINE
    coarse = (lx // step, ly // step, lz // step)
    count = coarse[0] * coarse[1]
    tables = coarse_matrices(sizes, coarse)
    middle = middle_tables(lx // 2, ly // 2, lz // 2)
    own, extra = lx // 2 * (ly // 2), middle[0].shape[0]
    middle = fine_tables(lx) + reach_tables(lx // 2, ly // 2, lz // 2) + middle
    scratch = [
        *(pltpu.VMEM(shape, jnp.float32) for shape in (
            (2, ly, LANES), (2, ly, LANES), (2, lx, LANES), (2, lx, LANES), (4, 1, LANES), (4, 1, LANES),
            (2, lx, LANES), (ly, LANES), (2, ly, LANES), (2, 1, LANES), (4, 1, LANES), (2, 2, LANES),
            (2, 2, 2, LANES), (2, 2, 2, 2, LANES), (ly, LANES), (lx, ly, LANES),
        )),
        pltpu.SemaphoreType.DMA,
        pltpu.SemaphoreType.DMA,
        *(pltpu.VMEM(shape, jnp.float32) for shape in (
            (own + lx + ly + 16, LANES), (lx + ly + 16, LANES), (2, 2, own + 2 * LANES), (2, 2, own + 2 * LANES),
            (2, 4, 2, LANES), (2, 2, 2, 2, LANES), (own, LANES), (lx // 4, ly // 4, LANES),
        )),
        pltpu.SemaphoreType.DMA,
        pltpu.SemaphoreType.DMA,
    ]
    scratch += [
        pltpu.VMEM((ndev, 8, LANES), jnp.float32),
        pltpu.VMEM((8, LANES), jnp.float32),
        pltpu.VMEM((tables[0].shape[2], LANES), jnp.float32),
        pltpu.VMEM((nx * ny * count, LANES), jnp.float32),
        pltpu.VMEM((1, LANES), jnp.float32),
        pltpu.VMEM((ndev, 1, LANES), jnp.float32),
        *[pltpu.SemaphoreType.DMA] * 4,
        pltpu.VMEM(fields.shape, jnp.float32),
        pltpu.SMEM(exponents.shape, jnp.int32),
        pltpu.VMEM(tables[0].shape, jnp.float32),
        pltpu.VMEM(tables[1].shape, jnp.float32),
        pltpu.SemaphoreType.DMA((4 + TABLES,)),
        *(pltpu.VMEM(table.shape, table.dtype) for table in middle),
    ]
    vmem = pl.BlockSpec(memory_space=pltpu.VMEM)
    held = pl.pallas_call(
        functools.partial(kernel, sizes, cells),
        out_shape=(
            pltpu.VMEM(fields.shape, jnp.float32),
            pltpu.VMEM((2, 1, LEVELS), jnp.float32),
        ),
        in_specs=[pl.BlockSpec(memory_space=pltpu.HBM)] * (4 + TABLES),
        out_specs=(vmem, vmem),
        scratch_shapes=scratch,
        compiler_params=pltpu.CompilerParams(
            collective_id=0, has_side_effects=True, vmem_limit_bytes=VMEM_LIMIT
        ),
    )(*(pltpu.with_memory_space_constraint(x, pltpu.HBM) for x in (exponents, fields, *map(jnp.asarray, (*tables, *middle)))))
    hbm = pl.BlockSpec(memory_space=pltpu.HBM)
    return pl.pallas_call(
        deliver,
        out_shape=(
            jax.ShapeDtypeStruct(fields.shape, jnp.float32),
            jax.ShapeDtypeStruct((2, 1, LEVELS), jnp.float32),
        ),
        in_specs=(vmem, vmem),
        out_specs=(hbm, hbm),
        scratch_shapes=[pltpu.SemaphoreType.DMA((CHUNKS + 1,))],
    )(*(pltpu.with_memory_space_constraint(x, pltpu.VMEM) for x in held))


def solution(mesh):
    sizes = tuple(mesh.shape[name] for name in ("gx", "gy", "gz"))
    placed = (P(None, "gx", "gy", "gz"), P())
    return jax.shard_map(
        functools.partial(shards, sizes),
        mesh=mesh,
        in_specs=placed,
        out_specs=placed,
        check_vma=False,
    )
```

```python
import functools

import numpy as np

import jax
import jax.numpy as jnp
from jax import lax
from jax.experimental import pallas as pl
from jax.experimental.pallas import tpu as pltpu
from jax.sharding import PartitionSpec as P

FINE = 3
LEVELS = 5
LANES = 128
CHUNKS = 4
BUFFERS = 18
TABLES = 14
BATCH = 8
ROUNDS = 2
VMEM_LIMIT = 58_720_256
MESH = pl.DeviceIdType.MESH


def periodic_lift(length):
    eye = np.eye(length)
    even, odd = eye[0::2], eye[1::2]
    detail = odd - 0.5 * (even + np.roll(even, -1, 0))
    smooth = even + 0.25 * (np.roll(detail, 1, 0) + detail)
    whole = np.zeros((length, length))
    whole[0::2] = smooth
    whole[1::2] = detail
    return whole


def second_lift(length):
    whole = np.zeros((length, length))
    whole[0::2, 0::2] = periodic_lift(length // 2)
    return whole


def coarse_matrices(sizes, coarse):
    nx, ny, nz = sizes
    cx, cy, cz = coarse
    rows = np.arange(nx * ny * cx * cy)
    dev, inner = rows // (cx * cy), rows % (cx * cy)
    gx = (dev // ny) * cx + inner // cy
    gy = (dev % ny) * cy + inner % cy
    step = LANES // cz
    lanes = np.array([z * step + d for d in range(nz) for z in range(cz)])
    reach_y, reach_x, spot = np.indices((cy + 3, cx + 3, nx * ny)).reshape(3, -1)
    from_x = (spot // ny * cx + reach_x - 1) % (nx * cx)
    from_y = (spot % ny * cy + reach_y - 1) % (ny * cy)
    from_z = np.arange(-1, nz * cz + 2) % (nz * cz)
    result = []
    for both_levels in (False, True):
        mx, my, mz = periodic_lift(nx * cx), periodic_lift(ny * cy), periodic_lift(nz * cz)
        if both_levels:
            mx, my, mz = second_lift(nx * cx) @ mx, second_lift(ny * cy) @ my, second_lift(nz * cz) @ mz
        both = mx[gx[:, None], from_x[None]] * my[gy[:, None], from_y[None]]
        along = np.zeros((LANES, LANES))
        along[np.ix_(np.arange(len(from_z)), lanes)] = mz[:, from_z].T
        result.append((both.astype(np.float32), along.astype(np.float32)))
    return [np.stack(pair) for pair in zip(*result)]


def cut_table(table):
    high = table.astype(jnp.bfloat16)
    low = (table - high.astype(np.float64)).astype(jnp.bfloat16)
    return high, low


def reach_line(n):
    twice = periodic_lift(3 * n // 2)[0::2] @ periodic_lift(3 * n)[0::2]
    return twice[n // 4 - 1 : n // 2 + 2, n : 2 * n]


def reach_tables(ax, ay, az):
    part_x, part_y, part_z = reach_line(ax), reach_line(ay), reach_line(az)
    wide, deep = len(part_z), len(part_y)
    rows = np.zeros((deep, 8, ax * ay))
    rows[:, : len(part_x)] = np.einsum("yb,xa->yxab", part_y, part_x).reshape(deep, -1, ax * ay)
    rows = rows.reshape(8 * deep, -1)
    along = np.zeros((deep + 1, LANES, LANES))
    for y in range(deep):
        fit = min(wide, LANES - wide * y)
        along[y, :: LANES // az, wide * y : wide * y + fit] = part_z[:fit].T
    along[deep, :: LANES // az, : wide - fit] = part_z[fit:].T
    return np.concatenate(cut_table(rows)), along.reshape(-1, LANES).astype(jnp.bfloat16)


def lift_line(n):
    whole = np.zeros((n, n + 2))
    cells = np.eye(n + 2)
    even, odd = cells[0:n:2], cells[1:n:2]
    after = np.concatenate((even[1:], cells[n + 1 :]))
    detail = odd - 0.5 * (even + after)
    before = np.concatenate((cells[n : n + 1] - 0.5 * even[:1], detail[:-1]))
    whole[0::2] = even + 0.25 * (before + detail)
    whole[1::2] = detail
    return whole

def line_tables(n):
    lift = lift_line(n)
    own = lift[:, :n]
    sent = np.zeros((4, n))
    sent[0, n - 1], sent[0, n - 2] = 1.0, -0.5
    sent[1] = own[n - 2] - 0.5 * own[n - 4]
    sent[2, 0] = 1.0
    sent[3] = own[0]
    first = np.zeros((n + 2, n + 4))
    first[:n, :n] = own
    first[:n, n], first[:n, n + 2] = lift[:, n], lift[:, n + 1]
    first[n, n + 1], first[n, 0] = 1.0, lift[n - 2, n + 1]
    first[n + 1, n + 3] = 1.0
    first[n + 1, :n] = lift[0, n] * sent[0]
    return sent, first, lift_line(n // 2)


def fine_tables(px):
    q = LANES // px
    ends = np.zeros((2, px))
    ends[0, px - 1], ends[0, px - 2], ends[1, 0] = 1.0, -0.5, 1.0
    edges = np.zeros((8, LANES))
    place = np.zeros((16, LANES))
    for z in range(2):
        for x in range(2):
            edges[2 * z + x, 2 - 2 * z :: q] = ends[x]
            for lane in ((2,), (0, 1))[z]:
                place[2 * z + x : 12 : 4, (LANES - q) * x + lane] = 1.0
    result = (lift_line(LANES)[:, :LANES].T, edges, place)
    return tuple(table.astype(jnp.bfloat16) for table in result)


def middle_tables(ax, ay, az):
    step = LANES // az
    sent_x, first_x, second_x = line_tables(ax)
    sent_y, first_y, second_y = line_tables(ay)
    sent_z, first_z, second_z = line_tables(az)
    finer = lift_line(2 * ay)
    low, high = finer[0, 2 * ay], finer[2 * ay - 2, 2 * ay + 1]
    after = sent_y[2, 0] * first_y[:, ay + 2] + sent_y[3, 0] * first_y[:, ay + 3]
    before = sent_y[0, ay - 1] * first_y[:, ay] + sent_y[1, ay - 1] * first_y[:, ay + 1]
    first_y = np.concatenate((first_y, np.stack((low * after, high * before), axis=1)), axis=1)
    own = [(x, y) for x in range(ax) for y in range(ay)]
    corners = [(x, 2 * g + y) for g in range(2) for x in range(4) for y in range(2)]
    extra = []
    for start in range(2):
        extra += [(ax + k, y) for k in (start, start + 2) for y in range(ay)]
        extra += [(x, ay + k) for k in (start, start + 2) for x in range(ax)]
    extra += [(ax + x, ay + y) for x, y in corners]
    pair = 2 * ax + 2 * ay
    by_x = extra[: 2 * ay] + extra[pair : pair + 2 * ay]
    by_y = extra[2 * ay : pair] + extra[pair + 2 * ay :]
    extra += [(x, ay + 4 + k) for k in range(2) for x in range(ax)]
    extra += [(ax + x, ay + 4 + k) for x in range(4) for k in range(2)]
    taken = np.array(own + extra)
    given = own + [(ax + k, y) for k in range(2) for y in range(0, ay, 2)]
    given += [(x, ay + k) for k in range(2) for x in range(0, ax, 2)]
    given += [(ax + x, ay + y) for x in range(2) for y in range(2)]
    height = -(-len(given) // 16) * 16

    whole_x, whole_y = np.concatenate((np.eye(ax), sent_x)), np.concatenate((np.eye(ay), sent_y))
    ox, oy = np.array(own).T
    sends = []
    for kinds in (by_y, by_x):
        ex, ey = np.array(kinds).T
        sends.append(whole_x[np.ix_(ex, ox)] * whole_y[np.ix_(ey, oy)])
    sends.append(np.zeros((16, 2 * ax)))
    sends[2][:8] = np.kron(sent_x, np.eye(2)).reshape(8, ax, 2).transpose(0, 2, 1).reshape(8, -1)
    gx, gy = np.array(given).T
    tx, ty = taken.T
    rows = np.zeros((height, len(taken) + 8))
    rows[: len(given), : len(taken)] = first_x[np.ix_(gx, tx)] * first_y[np.ix_(gy, ty)]

    def spot(at, n):
        return np.where(at >= n, n // 2 + at - n, at // 2)

    half = np.array([(x, y) for x in range(ax // 2) for y in range(ay // 2)])
    use = ((gx % 2 == 0) | (gx >= ax)) & ((gy % 2 == 0) | (gy >= ay))
    last = np.zeros((len(half), height))
    pick_x = second_x[np.ix_(half[:, 0], spot(gx, ax))]
    pick_y = second_y[np.ix_(half[:, 1], spot(gy, ay))]
    last[:, : len(given)] = pick_x * pick_y * use

    lanes = np.arange(az) * step
    out = np.concatenate((lanes, [1, step + 1]))
    send_lanes = np.zeros((8, LANES))
    send_lanes[np.ix_(np.arange(4), lanes)] = sent_z
    along = np.zeros((LANES, LANES))
    along[np.ix_(lanes, out)] = first_z[:, :az].T
    rim = np.zeros((16, LANES))
    for part in range(3):
        rim[np.ix_(4 * part + np.arange(4), out)] = first_z[:, az:].T
    along_last = np.zeros((LANES, LANES))
    source = np.concatenate((lanes[0::2], [1, step + 1]))
    along_last[np.ix_(source, lanes[0::2])] = second_z.T
    last = np.concatenate(cut_table(last @ rows))
    along = np.concatenate((along, along @ along_last), axis=1)
    rim = np.concatenate((rim, rim @ along_last), axis=1)
    result = (*sends, rows[: len(own)], last, send_lanes, along, np.roll(along, 1, 0), rim)
    return tuple(table.astype(jnp.bfloat16) for table in result)


def iota(shape, axis):
    return lax.broadcasted_iota(jnp.int32, shape, axis)


def roll(values, shift, axis):
    return pltpu.roll(values, shift % values.shape[axis], axis)


def lift_rows(v, low, high):
    n = v.shape[0]
    row = iota(v.shape, 0)
    odd = row % 2 == 1
    up = jnp.where(row == n - 1, high, roll(v, -1, 0))
    w = jnp.where(odd, v - 0.5 * (roll(v, 1, 0) + up), v)
    down = jnp.where(row == 0, low - 0.5 * v, roll(w, 1, 0))
    return jnp.where(odd, w, w + 0.25 * (down + roll(w, -1, 0)))


def lift_groups(v, rim, s):
    lane = iota(v.shape, 1)
    odd = (lane // s) % 2 == 1
    up = jnp.where(lane >= LANES - s, rim, roll(v, -s, 1))
    w = jnp.where(odd, v - 0.5 * (roll(v, s, 1) + up), v)
    down = jnp.where(lane < s, rim - 0.5 * v, roll(w, s, 1))
    return jnp.where(odd, w, w + 0.25 * (down + roll(w, -s, 1)))


def shrink(v, thresh):
    return v - jnp.clip(v, -thresh, thresh)


def three(v):
    parts = []
    for _ in range(3):
        parts.append(v.astype(jnp.bfloat16))
        v = v - parts[-1].astype(jnp.float32)
    return parts


def mix(a, b, dims):
    return lax.dot_general(a, b, (dims, ((), ())), preferred_element_type=jnp.float32)


def mix_rows(table, v):
    wide = mix(table, jnp.concatenate(three(v), axis=1), ((1,), (0,)))
    return wide[:, :LANES] + wide[:, LANES : 2 * LANES] + wide[:, 2 * LANES :]


def doubled(v, n):
    return v[0:n] + v[n:]


def mix_lanes(v, table):
    return mix(jnp.concatenate(three(v), axis=1), jnp.concatenate([table] * 3, axis=0), ((1,), (0,)))


def total(v):
    return jnp.sum(jnp.sum(v, axis=0, keepdims=True), axis=1, keepdims=True)


def kernel(sizes, cells, exps_in, field_in, rows_in, lanes_in, *rest):
    tables_in, (out, stats), scratch = rest[:TABLES], rest[TABLES : TABLES + 2], rest[TABLES + 2 :]
    nx, ny, nz = sizes
    ndev = nx * ny * nz
    scratch = list(scratch)
    tables = scratch[-TABLES:]
    scratch = scratch[:-TABLES]
    field, exps, k_s, l_s, in_sem = scratch[-5:]
    scratch = scratch[:-5]
    pairs = [(field_in, field), (exps_in, exps), *zip(tables_in, tables), (rows_in, k_s), (lanes_in, l_s)]
    loads = [pltpu.make_async_copy(a, b, in_sem.at[i]) for i, (a, b) in enumerate(pairs)]
    me = (lax.axis_index("gx"), lax.axis_index("gy"), lax.axis_index("gz"))

    def device(dx, dy, dz):
        return (
            lax.rem(me[0] + (dx + nx), nx),
            lax.rem(me[1] + (dy + ny), ny),
            lax.rem(me[2] + (dz + nz), nz),
        )

    def distance(spot):
        return sum(min(d, size - d) for d, size in zip(spot, sizes))

    def thresh(level):
        return jnp.exp2(jnp.full((1, LANES), exps[level].astype(jnp.float32)))

    def split(j):
        return j // (ny * nz), (j // nz) % ny, j % nz

    def launch(copies, send_sem, recv_sem):
        flights = [
            pltpu.make_async_remote_copy(
                src_ref=f, dst_ref=t, send_sem=send_sem, recv_sem=recv_sem,
                device_id=device(*d), device_id_type=MESH,
            )
            for f, t, d in copies
        ]
        for flight in flights:
            flight.start()
        return sum(t.size for _, t, _ in copies) // LANES

    def settle(span, send_sem, recv_sem):
        for sem in (recv_sem, send_sem):
            pltpu.make_async_copy(span, span, sem).wait()

    barrier = pltpu.get_barrier_semaphore()

    near = max(sizes) // 2 <= ROUNDS
    greeted = {
        tuple((d + size - 1) % size if near else d for d, size in zip(spot, sizes))
        for spot in np.ndindex(*(3, 3, 3) if near else sizes)
    } - {(0, 0, 0)}
    for spot in sorted(greeted, key=lambda spot: (-distance(spot), spot)):
        pl.semaphore_signal(barrier, inc=1, device_id=device(*spot), device_id_type=MESH)
    for load in loads:
        load.start()
    gath, msg, parts_s, final_s, tally_s, tallies, g_send, g_recv, t_send, t_recv = scratch[-10:]
    loads[0].wait()
    loads[1].wait()
    step_to = (1, -1)
    alone = nx == 2
    ways = (0,) if alone else (0, 1)
    (xs, xr, ys, yr, es, er, yl, zs, zr, ds, dr, ts, txr, tcr, rim, work, send_sem, recv_sem) = scratch[:BUFFERS]
    middle = scratch[BUFFERS : BUFFERS + 15]
    grown, ghost, sent, edge1, side, hz, xzr, t2r, t3r, o1s, o2s, m_send, m_recv, y_send, y_recv = middle
    fine_lanes, fine_edges, fine_place, reach_rows, reach_lanes, *tables = tables
    src = field.at[0]
    px, n = src.shape[0], src.shape[1]
    half, q = n // 2, LANES // px
    lane = iota((n, LANES), 1)
    row8 = iota((8, LANES), 0)

    def ends(v):
        return v[n - 1 : n] - 0.5 * v[n - 2 : n - 1], v[0:1]

    def under(pair):
        return jnp.where(row8 == 0, pair[0], jnp.where(row8 == 1, pair[1], 0.0))

    planes = (src[px - 1] - 0.5 * src[px - 2], src[0])
    ys[0] = src[:, n - 1, :] - 0.5 * src[:, n - 2, :]
    ys[1] = src[:, 0, :]
    for gx in (0, 1):
        xs[gx] = planes[gx]
        es[2 * gx], es[2 * gx + 1] = ends(planes[gx])
    packed = jnp.zeros((n, LANES), jnp.float32)
    for x in range(px):
        packed = jnp.where(lane // q == x, roll(src[x], q * x + 2, 1), packed)
    odd_end = roll(packed - 0.5 * roll(packed, 1, 1), 1, 1)
    even_end = jnp.where(lane % q == 1, roll(packed, -1, 1), roll(packed, -2, 1))
    packed = jnp.where(lane % q == 2, odd_end, even_end)
    zs[...] = packed
    ds[0], ds[1] = ends(packed)
    for load in loads[2:5]:
        load.wait()
    edges = sum(
        mix(fine_edges[...], part, ((1,), (1,)))
        for part in three(jnp.concatenate((packed, under(ends(packed))), axis=0))
    )
    ts[...] = jnp.zeros(ts.shape, jnp.float32)
    for g in (0, 1):
        ts[g, :, pl.ds(0, n + 8)] = edges[2 * g : 2 * g + 2]

    pl.semaphore_wait(barrier, len(greeted))
    along_y, others = [], []
    for g in (0, 1):
        dz = step_to[g]
        for gx in ways:
            for gy in (0, 1):
                along_y.append((ts.at[g], tcr.at[g, gy, gx], (step_to[gx], step_to[gy], dz)))
            others.append((ts.at[g], txr.at[g, gx], (step_to[gx], 0, dz)))
        for gy in (0, 1):
            along_y.append((ds.at[gy], dr.at[2 * g + gy], (0, step_to[gy], dz)))
    for gx in (0, 1):
        for gy in (0, 1):
            along_y.append((es.at[2 * gx + gy], er.at[2 * gx + gy], (step_to[gx], step_to[gy], 0)))
    for g in (0, 1):
        along_y.append((ys.at[g], yr.at[g], (0, step_to[g], 0)))
    for g in (0, 1):
        others.append((xs.at[g], xr.at[g], (step_to[g], 0, 0)))
    for g in (0, 1):
        others.append((zs, zr.at[g], (0, 0, step_to[g])))
    y_rows = launch(along_y, y_send, y_recv)
    sent_rows = launch(others, send_sem, recv_sem)
    settle(grown.at[pl.ds(0, sent_rows)], send_sem, recv_sem)

    lane2, row2 = iota((2, LANES), 1), iota((2, LANES), 0)

    def both(ref):
        return ref[0] if alone else jnp.where(row2 == 0, ref[0], ref[1])

    def columns(top, table):
        pieces = [part.astype(jnp.float32) for part in three(top)]
        pieces.append(jnp.zeros_like(top))
        return mix(jnp.concatenate(pieces, axis=0).astype(jnp.bfloat16), table, ((0,), (0,)))

    def kinds(a, b):
        return jnp.where(iota(a.shape, 1) % q == 2, a, b)

    lane_half = iota((half, LANES), 1)
    share = jnp.where(lane_half == LANES - 2, -0.125, jnp.where(lane_half == 0, 0.25, 0.0))
    share = jnp.where(lane_half == LANES - 1, -0.5, share)
    level_thresh = thresh(0)
    row = iota((half, LANES), 0)
    ax, ay = px // 2, half
    own = ax * ay
    px_rows, py_rows = 2 * ay, 2 * ax
    pair = px_rows + py_rows
    send_y, send_x, send_q, rows1, rows2, send_lanes, lanes12, odd_lanes12, rim12 = tables
    none = jnp.zeros((1, LANES), jnp.float32)

    def halves(ref, x):
        return [ref[x, pl.ds(start, half, stride=2), :] for start in (0, 1)]

    def stored(x):
        return [work[x, 0:half], work[x, half:]]

    def lift_halves(v, below, above):
        even, odd = v
        after = jnp.where(row == half - 1, above, roll(even, -1, 0))
        detail = odd - 0.5 * (even + after)
        before = jnp.where(row == 0, below - 0.5 * even, roll(detail, 1, 0))
        return [even + 0.25 * (before + detail), detail]

    def lift_last(stack, border):
        whole = mix_lanes(jnp.concatenate([v for v, _, _ in stack], axis=0), fine_lanes[...])
        for i, (_, x, kind) in enumerate(stack):
            yield x, kind, whole[half * i : half * i + half] + roll(border[kind], LANES - 2 - q * x, 1) * share

    def sideways(parts, target):
        edges = sum(mix(send_lanes[...], part, ((1,), (1,))) for part in three(jnp.concatenate(parts, axis=0)))
        for g in (0, 1):
            target[g, :, pl.ds(target.shape[2] - LANES, LANES)] = jnp.zeros((2, LANES), jnp.float32)
            target[g, :, pl.ds(0, edges.shape[1])] = edges[2 * g : 2 * g + 2]

    def both_kinds(a, b):
        return jnp.where(iota(a.shape, 1) % 2 == 0, a, roll(b, 1, 1))

    for load in loads[5 : 2 + TABLES]:
        load.wait()
    tops = [jnp.where(lane2 < n, both(txr.at[g]), 0.0) for g in (0, 1)]
    beside = columns(jnp.concatenate(tops, axis=0), fine_place[...])[0:n]
    v = lift_groups(kinds(zr[0], zr[1]), beside, q)
    outer_rims = ends(v)
    rim[...] = lift_rows(v, none, none)
    border = [rim[pl.ds(0, half, stride=2), :]]
    even = halves(src, 0)
    before = [p - 0.5 * e for p, e in zip(halves(xr, 0), even)]
    stack = []
    for k in range(px // 2):
        after = halves(src, 2 * k + 2) if 2 * k + 2 < px else halves(xr, 1)
        detail = [o - 0.5 * (e + a) for o, e, a in zip(halves(src, 2 * k + 1), even, after)]
        smooth = [e + 0.25 * (b + d) for e, b, d in zip(even, before, detail)]
        work[2 * k, 0:half], work[2 * k, half:] = smooth
        work[2 * k + 1, 0:half], work[2 * k + 1, half:] = detail
        stack.append((lift_halves(smooth, none, none)[0], 2 * k, 0))
        even, before = after, detail
        if len(stack) == BATCH:
            for x, _, v in lift_last(stack, border):
                ghost[pl.ds(x // 2 * half, half), :] = v
            stack = []
    beyond = [ends(xr[g]) for g in (0, 1)]
    raw = []
    for g in (0, 1):
        yl[g] = lift_rows(ys[g], beyond[0][g], beyond[1][g])
        raw.append(yl[g, pl.ds(0, ax, stride=2), :])
    raw = mix_lanes(jnp.concatenate(raw, axis=0), fine_lanes[...])
    turned = []
    for v in outer_rims:
        v = jnp.broadcast_to(v, (8, LANES))
        for start in range(0, ax, 8):
            tile = jnp.zeros((8, LANES), jnp.float32)
            for i in range(8):
                tile = jnp.where(row8 == i, roll(v, LANES - 2 - 2 * q * (start + i), 1), tile)
            turned.append(tile)
    raw = raw + jnp.concatenate(turned, axis=0) * share[0:1]
    grown[pl.ds(own + pair + 16, py_rows), :] = raw
    grown[pl.ds(own + pair + 24 + py_rows, 8), :] = jnp.zeros((8, LANES), jnp.float32)

    halo = mix_rows(send_y[...], ghost[...])
    halo = (halo[0:py_rows], halo[py_rows : 2 * py_rows], halo[2 * py_rows :])
    sent[px_rows:pair] = both_kinds(halo[0], halo[1])
    sent[pair : pair + 16] = halo[2]
    blank = jnp.zeros((px_rows, LANES), jnp.float32)
    sideways((blank, halo[0], blank, halo[1], halo[2]), edge1)
    copies = []

    def rows_copy(start, size, to):
        copies.append((sent.at[pl.ds(start, size)], grown.at[pl.ds(own + start, size)], to))

    parts = len(ways)
    for g in (0, 1):
        for gy in (0, 1):
            for gx in ways:
                copies.append((edge1.at[g, :, pl.ds(LANES, LANES)], t3r.at[g, gy, gx], (step_to[gx], step_to[gy], step_to[g])))
            copies.append((edge1.at[g, :, pl.ds(0, LANES)], t2r.at[g, gy], (0, step_to[gy], step_to[g])))
    for gy in (0, 1):
        for gx in ways:
            rows_copy(pair + 8 * gy + 4 * gx, 8 // parts, (step_to[gx], step_to[gy], 0))
    for gy in (0, 1):
        rows_copy(px_rows + ax * gy, ax, (0, step_to[gy], 0))
    sent_rows = launch(copies, m_send, m_recv)
    settle(grown.at[pl.ds(0, y_rows)], y_send, y_recv)

    tops = []
    for g in (0, 1):
        yl[g] = lift_rows(yr[g], er[g], er[2 + g])
        v = jnp.where(lane2 == n, both(tcr.at[g, 0]), both(tcr.at[g, 1]))
        v = jnp.where(lane2 < n, both(txr.at[g]), v)
        tops.append(jnp.where(lane2 < n + 2, v, 0.0))
    beside = columns(jnp.concatenate(tops, axis=0), fine_place[...])[0 : n + 8]
    lower = under((kinds(dr[0], dr[2]), kinds(dr[1], dr[3])))
    v = lift_groups(jnp.concatenate((kinds(zr[0], zr[1]), lower), axis=0), beside, q)
    v = lift_rows(v[0:n], v[n : n + 1], v[n + 1 : n + 2])
    rim[...] = v
    border = [rim[pl.ds(start, half, stride=2), :] for start in (0, 1)]
    stack = []
    for x in range(0, px, 2):
        smooth = lift_halves(stored(x), yl[0, x : x + 1, :], yl[1, x : x + 1, :])
        work[x, half:] = smooth[1]
        stack.append((smooth[0], x, 0))
        if len(stack) == BATCH:
            for at, _, v in lift_last(stack, border):
                work[at, 0:half] = v
                grown[pl.ds(at // 2 * half, half), :] = v
            stack = []

    def finish():
        energy = kept = jnp.zeros((half, LANES), jnp.float32)
        for start in range(0, px, 4):
            stack, ready = [], []
            for x in range(start, start + 4, 2):
                ready.append((x, 0, work[x, 0:half]))
                stack.append((work[x, half:], x, 1))
                lifted = lift_halves(stored(x + 1), yl[0, x + 1 : x + 2, :], yl[1, x + 1 : x + 2, :])
                stack += [(lifted[0], x + 1, 0), (lifted[1], x + 1, 1)]
            for x, kind, v in (*ready, *lift_last(stack, border)):
                small = shrink(v, level_thresh)
                out[0, x, pl.ds(kind, half, stride=2), :] = small
                square, size = v * v, jnp.abs(small)
                if x % 2 == 0 and kind == 0:
                    square, size = (jnp.where(lane_half % 2 == 0, 0.0, u) for u in (square, size))
                energy += square
                kept += size
        return [total(energy), total(kept)]

    here = grown[0:own]
    halo = mix_rows(send_x[...], here)
    corner = mix_rows(send_q[...], raw)[0:8]
    sent[0:px_rows] = both_kinds(halo[0:px_rows], halo[px_rows:])
    sent[pair + 16 :] = corner
    blank = jnp.zeros((py_rows, LANES), jnp.float32)
    filled = jnp.zeros((16, LANES), jnp.float32)
    sideways((here, halo[0:px_rows], blank, halo[px_rows:], blank, filled, raw, corner, filled[0:8]), side)
    copies = []
    for g in (0, 1):
        for gx in ways:
            copies.append((side.at[g, :, pl.ds(own, 2 * LANES)], xzr.at[g, gx], (step_to[gx], 0, step_to[g])))
        copies.append((side.at[g], hz.at[g], (0, 0, step_to[g])))
    for gx in ways:
        size = 8 // parts
        at = own + pair + 16 + py_rows + size * gx
        copies.append((sent.at[pl.ds(pair + 16 + size * gx, size)], grown.at[pl.ds(at, size)], (step_to[gx], 0, 0)))
        rows_copy(ay * gx, px_rows // parts, (step_to[gx], 0, 0))
    sent_rows += launch(copies, m_send, m_recv)
    extra = 2 * pair + 16 + py_rows + 16

    spots = nx * ny
    slot = (me[2] * nx + me[0]) * ny + me[1]
    cx, cy, cz = ax // 4, ay // 4, LANES // 2**FINE
    step = 2**FINE
    count = cx * cy
    long, deep, reach = cx + 3, cy + 3, cz + 3
    cut = LANES - reach * (deep - 1)
    rest = reach - cut

    def spread(source, target, send_sem, recv_sem):
        def post(j):
            return pltpu.make_async_remote_copy(
                src_ref=source, dst_ref=target, send_sem=send_sem, recv_sem=recv_sem,
                device_id=device(*split(j)), device_id_type=MESH,
            )

        def send(j, carry):
            post(j).start()
            return carry

        if ndev <= 32:
            for j in sorted(range(1, ndev), key=lambda j: (-distance(split(j)), j)):
                post(j).start()
        else:
            lax.fori_loop(1, ndev, send, 0)

    pieces = mix_rows(reach_rows[...], here)
    pieces = doubled(pieces, 8 * deep)
    blocks = [part.astype(jnp.float32) for part in three(pieces)]

    def stack(first, last):
        rows = [jnp.concatenate([b[8 * y : 8 * y + 8] for y in range(first, last)], axis=1) for b in blocks]
        return jnp.concatenate(rows + [jnp.zeros_like(rows[0])], axis=0).astype(jnp.bfloat16)

    def fold(v):
        return v[0:8] + v[8:16] + v[16:24]

    sheet = fold(mix(stack(0, deep), reach_lanes[pl.ds(0, deep * LANES), :], ((1,), (0,))))
    loose = fold(mix(stack(deep - 1, deep), reach_lanes[pl.ds(deep * LANES, LANES), :], ((1,), (0,))))
    spare = loose[0:1]
    for x in range(1, long):
        spare += roll(loose[x : x + 1], rest * x, 1)
    msg[...] = jnp.where(row8 == long, spare, sheet)
    spread(msg, gath.at[slot], g_send, g_recv)
    gath[slot] = msg[...]
    sums = finish()
    quarter = own // 4

    def level_rows(v, columns):
        return (
            mix_rows(rows1[:, columns], v[:, 0:LANES]),
            doubled(mix_rows(rows2[:, columns], v[:, LANES:]), quarter),
        )

    o1s[...], early = level_rows(mix_lanes(here, lanes12[...]), pl.ds(0, own))
    o2s[...] = early.reshape(o2s.shape)
    settle(grown.at[pl.ds(0, sent_rows)], m_send, m_recv)

    for g in (0, 1):
        across = (xzr.at[g, 0], xzr.at[g, 0 if alone else 1])
        place_in = lane2 % pair
        v = jnp.where(place_in < ay, across[0][:, 0:LANES], across[1][:, 0:LANES])
        v = jnp.where(place_in < px_rows, v, jnp.where(place_in < px_rows + ax, t2r[g, 0], t2r[g, 1]))
        hz[g, :, pl.ds(own, LANES)] = v
        u = []
        for gy in (0, 1):
            u.append(jnp.where(lane2 % 8 < 4, t3r[g, gy, 0], t3r[g, gy, 0 if alone else 1]))
        v = jnp.where(lane2 < 8, u[0], u[1])
        w = jnp.where(lane2 < 20 + py_rows, across[0][:, LANES:], across[1][:, LANES:])
        w = jnp.where(lane2 < 16 + py_rows, hz[g, :, pl.ds(own + LANES, LANES)], w)
        v = jnp.where(lane2 < 16, v, jnp.where(lane2 < 24 + py_rows, w, 0.0))
        hz[g, :, pl.ds(own + LANES, LANES)] = v
    rim_rows = columns(jnp.concatenate((hz[0], hz[1]), axis=0), rim12[...])
    got = grown[pl.ds(own, extra - pair), :]
    outer = mix_lanes(got, lanes12[...])
    outer = (outer[0:pair], mix_lanes(got[0:pair], odd_lanes12[...]), outer[pair:])
    outer = jnp.concatenate(outer, axis=0) + rim_rows[own : own + extra]
    late = level_rows(jnp.concatenate((rim_rows[0:own], outer), axis=0), pl.ds(0, own + extra))
    first = o1s[...] + late[0]
    second = o2s[...].reshape(quarter, LANES) + late[1]
    o1s[...] = first
    o2s[...] = second.reshape(o2s.shape)

    def tally(v, level, ny):
        s = 2**level
        row, at = iota(v.shape, 0), iota(v.shape, 1)
        smooth = ((row // ny) % 2 == 0) & (row % 2 == 0) & (at % (2 * s) == 0)
        use = (at % s == 0) & ~smooth
        small = shrink(v, thresh(level))
        return [total(jnp.where(use, v * v, 0.0)), total(jnp.where(use, jnp.abs(small), 0.0))]

    sums += tally(first, 1, ay) + tally(second, 2, ay // 2)

    def place(source, level):
        s = 2**level
        small_y = ay >> (level - 1)
        keep = iota((small_y, LANES), 1) % s == 0
        for x in range(ax >> (level - 1)):
            spot = (0, s * x, pl.ds(0, small_y, stride=s), slice(None))
            out[spot] = jnp.where(keep, shrink(source(x), thresh(level)), out[spot])

    one = iota((1, LANES), 1)
    tail = jnp.zeros((1, LANES), jnp.float32)
    for i, whole in enumerate(sums):
        tail = jnp.where(one == i, whole, tail)
    tally_s[...] = tail
    spread(tally_s, tallies.at[slot], t_send, t_recv)
    tallies[slot] = tail
    place(lambda x: o1s[pl.ds(x * ay, ay), :], 1)
    place(lambda x: o2s[x], 2)
    settle(gath.at[pl.ds(0, ndev - 1)], g_send, g_recv)

    at = iota((spots, LANES), 1)
    spares = [gath[pl.ds(z * spots, spots), long, :] for z in range(nz)]

    def window(v, source, start, size):
        moved = roll(v, start - source, 1)
        return jnp.where((at >= start) & (at < start + size), moved, 0.0)

    for x in range(long):
        boxes = [gath[pl.ds(z * spots, spots), x, :] for z in range(nz)]
        for y in range(deep):
            fit = reach if y < deep - 1 else cut
            v = sum(window(boxes[z], reach * y, cz * z, fit) for z in range(nz))
            if fit < reach:
                v += sum(window(spares[z], rest * x, cz * z + cut, rest) for z in range(nz))
            parts_s[pl.ds((y * long + x) * spots, spots), :] = v

    def dot(a, b):
        return jnp.dot(a, b, precision=lax.Precision.HIGHEST, preferred_element_type=jnp.float32)

    grid = parts_s[...]
    loads[2 + TABLES].wait()
    loads[3 + TABLES].wait()
    half3, half4 = dot(k_s[0], grid), dot(k_s[1], grid)
    grid, grid4 = dot(half3, l_s[0]), dot(half4, l_s[1])
    row = iota(grid.shape, 0)
    lane = iota(grid.shape, 1)
    inner_row = row % count
    gx, gy, gz = inner_row // cy, inner_row % cy, lane // step
    valid = lane % step < nz
    even3 = (gx % 2 == 0) & (gy % 2 == 0) & (gz % 2 == 0)
    even4 = (gx % 4 == 0) & (gy % 4 == 0) & (gz % 4 == 0)
    det3 = valid & ~even3
    det4 = valid & even3 & ~even4
    small3 = shrink(grid, thresh(FINE))
    small4 = shrink(grid4, thresh(FINE + 1))
    final_s[...] = jnp.where(even3, jnp.where(even4, grid4, small4), small3)

    def masked(mask, v):
        return total(jnp.where(mask, v, 0.0))

    coarse = ((masked(det3, grid * grid), masked(det3, jnp.abs(small3))),
              (masked(det4, grid4 * grid4), masked(det4, jnp.abs(small4))))
    first = pl.multiple_of((me[0] * ny + me[1]) * count, count)
    mine = pltpu.roll(final_s[pl.ds(first, count), :], lax.rem(LANES - me[2], LANES), 1)
    keep = iota((cy, LANES), 1) % step == 0
    for x in range(cx):
        spot = (0, step * x, pl.ds(0, cy, stride=step), slice(None))
        out[spot] = jnp.where(keep, mine[x * cy : x * cy + cy], out[spot])

    settle(tallies.at[pl.ds(0, ndev - 1)], t_send, t_recv)
    tail = jnp.sum(tallies[...], axis=0)
    for q in (0, 1):
        line = jnp.zeros((1, LANES), jnp.float32)
        for level in range(LEVELS):
            weight = 8.0 ** (level + 1) / (7.0 * cells)
            if level < FINE:
                value = jnp.sum(jnp.where(one == 2 * level + q, tail, 0.0), axis=1, keepdims=True)
            else:
                value = coarse[level - FINE][q]
            line = jnp.where(one == level, value * weight, line)
        stats[q] = line[:, 0:LEVELS]


def deliver(held, held_stats, out, stats, sem):
    rows = held.shape[1] // CHUNKS
    copies = [pltpu.make_async_copy(held_stats, stats, sem.at[CHUNKS])]
    for i in range(CHUNKS):
        part = pl.ds(i * rows, rows)
        copies.append(pltpu.make_async_copy(held.at[:, part], out.at[:, part], sem.at[i]))
    for copy in copies:
        copy.start()
    for copy in copies:
        copy.wait()


def shards(sizes, fields, exponents):
    nx, ny, nz = sizes
    ndev = nx * ny * nz
    _, lx, ly, lz = fields.shape
    cells = fields.size * ndev
    step = 2**FINE
    coarse = (lx // step, ly // step, lz // step)
    count = coarse[0] * coarse[1]
    tables = coarse_matrices(sizes, coarse)
    middle = middle_tables(lx // 2, ly // 2, lz // 2)
    own, extra = lx // 2 * (ly // 2), middle[0].shape[0]
    middle = fine_tables(lx) + reach_tables(lx // 2, ly // 2, lz // 2) + middle
    scratch = [
        *(pltpu.VMEM(shape, jnp.float32) for shape in (
            (2, ly, LANES), (2, ly, LANES), (2, lx, LANES), (2, lx, LANES), (4, 1, LANES), (4, 1, LANES),
            (2, lx, LANES), (ly, LANES), (2, ly, LANES), (2, 1, LANES), (4, 1, LANES), (2, 2, LANES),
            (2, 2, 2, LANES), (2, 2, 2, 2, LANES), (ly, LANES), (lx, ly, LANES),
        )),
        pltpu.SemaphoreType.DMA,
        pltpu.SemaphoreType.DMA,
        *(pltpu.VMEM(shape, jnp.float32) for shape in (
            (own + 2 * lx + ly + 32, LANES), (own, LANES), (lx + ly + 24, LANES), (2, 2, 2 * LANES),
            (2, 2, own + 2 * LANES), (2, 2, own + 2 * LANES), (2, 2, 2, 2 * LANES), (2, 2, 2, LANES),
            (2, 2, 2, 2, LANES), (own, LANES), (lx // 4, ly // 4, LANES),
        )),
        pltpu.SemaphoreType.DMA,
        pltpu.SemaphoreType.DMA,
        pltpu.SemaphoreType.DMA,
        pltpu.SemaphoreType.DMA,
    ]
    scratch += [
        pltpu.VMEM((ndev, 8, LANES), jnp.float32),
        pltpu.VMEM((8, LANES), jnp.float32),
        pltpu.VMEM((tables[0].shape[2], LANES), jnp.float32),
        pltpu.VMEM((nx * ny * count, LANES), jnp.float32),
        pltpu.VMEM((1, LANES), jnp.float32),
        pltpu.VMEM((ndev, 1, LANES), jnp.float32),
        *[pltpu.SemaphoreType.DMA] * 4,
        pltpu.VMEM(fields.shape, jnp.float32),
        pltpu.SMEM(exponents.shape, jnp.int32),
        pltpu.VMEM(tables[0].shape, jnp.float32),
        pltpu.VMEM(tables[1].shape, jnp.float32),
        pltpu.SemaphoreType.DMA((4 + TABLES,)),
        *(pltpu.VMEM(table.shape, table.dtype) for table in middle),
    ]
    vmem = pl.BlockSpec(memory_space=pltpu.VMEM)
    held = pl.pallas_call(
        functools.partial(kernel, sizes, cells),
        out_shape=(
            pltpu.VMEM(fields.shape, jnp.float32),
            pltpu.VMEM((2, 1, LEVELS), jnp.float32),
        ),
        in_specs=[pl.BlockSpec(memory_space=pltpu.HBM)] * (4 + TABLES),
        out_specs=(vmem, vmem),
        scratch_shapes=scratch,
        compiler_params=pltpu.CompilerParams(
            collective_id=0, has_side_effects=True, vmem_limit_bytes=VMEM_LIMIT
        ),
    )(*(pltpu.with_memory_space_constraint(x, pltpu.HBM) for x in (exponents, fields, *map(jnp.asarray, (*tables, *middle)))))
    hbm = pl.BlockSpec(memory_space=pltpu.HBM)
    return pl.pallas_call(
        deliver,
        out_shape=(
            jax.ShapeDtypeStruct(fields.shape, jnp.float32),
            jax.ShapeDtypeStruct((2, 1, LEVELS), jnp.float32),
        ),
        in_specs=(vmem, vmem),
        out_specs=(hbm, hbm),
        scratch_shapes=[pltpu.SemaphoreType.DMA((CHUNKS + 1,))],
    )(*(pltpu.with_memory_space_constraint(x, pltpu.VMEM) for x in held))


def solution(mesh):
    sizes = tuple(mesh.shape[name] for name in ("gx", "gy", "gz"))
    placed = (P(None, "gx", "gy", "gz"), P())
    return jax.shard_map(
        functools.partial(shards, sizes),
        mesh=mesh,
        in_specs=placed,
        out_specs=placed,
        check_vma=False,
    )
```

```python
import functools

import numpy as np

import jax
import jax.numpy as jnp
from jax import lax
from jax.experimental import pallas as pl
from jax.experimental.pallas import tpu as pltpu
from jax.sharding import PartitionSpec as P

FINE = 3
LEVELS = 5
LANES = 128
CHUNKS = 4
BUFFERS = 20
TABLES = 14
BATCH = 8
ROUNDS = 2
VMEM_LIMIT = 58_720_256
MESH = pl.DeviceIdType.MESH


def periodic_lift(length):
    eye = np.eye(length)
    even, odd = eye[0::2], eye[1::2]
    detail = odd - 0.5 * (even + np.roll(even, -1, 0))
    smooth = even + 0.25 * (np.roll(detail, 1, 0) + detail)
    whole = np.zeros((length, length))
    whole[0::2] = smooth
    whole[1::2] = detail
    return whole


def second_lift(length):
    whole = np.zeros((length, length))
    whole[0::2, 0::2] = periodic_lift(length // 2)
    return whole


def coarse_matrices(sizes, coarse):
    nx, ny, nz = sizes
    cx, cy, cz = coarse
    rows = np.arange(nx * ny * cx * cy)
    dev, inner = rows // (cx * cy), rows % (cx * cy)
    gx = (dev // ny) * cx + inner // cy
    gy = (dev % ny) * cy + inner % cy
    step = LANES // cz
    lanes = np.array([z * step + d for d in range(nz) for z in range(cz)])
    reach_y, reach_x, spot = np.indices((cy + 3, cx + 3, nx * ny)).reshape(3, -1)
    from_x = (spot // ny * cx + reach_x - 1) % (nx * cx)
    from_y = (spot % ny * cy + reach_y - 1) % (ny * cy)
    from_z = np.arange(-1, nz * cz + 2) % (nz * cz)
    result = []
    for both_levels in (False, True):
        mx, my, mz = periodic_lift(nx * cx), periodic_lift(ny * cy), periodic_lift(nz * cz)
        if both_levels:
            mx, my, mz = second_lift(nx * cx) @ mx, second_lift(ny * cy) @ my, second_lift(nz * cz) @ mz
        both = mx[gx[:, None], from_x[None]] * my[gy[:, None], from_y[None]]
        along = np.zeros((LANES, LANES))
        along[np.ix_(np.arange(len(from_z)), lanes)] = mz[:, from_z].T
        result.append((np.pad(both, ((0, 0), (0, -both.shape[1] % 16))), along.astype(jnp.bfloat16)))
    (one, along_one), (two, along_two) = result
    rows = np.concatenate((one.astype(jnp.bfloat16), *cut_table(two)))
    return rows, np.stack((along_one, along_two))


def cut_table(table):
    high = table.astype(jnp.bfloat16)
    low = (table - high.astype(np.float64)).astype(jnp.bfloat16)
    return high, low


def reach_line(n):
    twice = periodic_lift(3 * n // 2)[0::2] @ periodic_lift(3 * n)[0::2]
    return twice[n // 4 - 1 : n // 2 + 2, n : 2 * n]


def reach_tables(ax, ay, az):
    part_x, part_y, part_z = reach_line(ax), reach_line(ay), reach_line(az)
    wide, deep = len(part_z), len(part_y)
    rows = np.zeros((deep, 8, ax * ay))
    rows[:, : len(part_x)] = np.einsum("yb,xa->yxab", part_y, part_x).reshape(deep, -1, ax * ay)
    rows = rows.reshape(8 * deep, -1)
    along = np.zeros((deep + 1, LANES, LANES))
    for y in range(deep):
        fit = min(wide, LANES - wide * y)
        along[y, :: LANES // az, wide * y : wide * y + fit] = part_z[:fit].T
    along[deep, :: LANES // az, : wide - fit] = part_z[fit:].T
    return np.concatenate(cut_table(rows)), along.reshape(-1, LANES).astype(jnp.bfloat16)


def lift_line(n):
    whole = np.zeros((n, n + 2))
    cells = np.eye(n + 2)
    even, odd = cells[0:n:2], cells[1:n:2]
    after = np.concatenate((even[1:], cells[n + 1 :]))
    detail = odd - 0.5 * (even + after)
    before = np.concatenate((cells[n : n + 1] - 0.5 * even[:1], detail[:-1]))
    whole[0::2] = even + 0.25 * (before + detail)
    whole[1::2] = detail
    return whole

def line_tables(n):
    lift = lift_line(n)
    own = lift[:, :n]
    sent = np.zeros((4, n))
    sent[0, n - 1], sent[0, n - 2] = 1.0, -0.5
    sent[1] = own[n - 2] - 0.5 * own[n - 4]
    sent[2, 0] = 1.0
    sent[3] = own[0]
    first = np.zeros((n + 2, n + 4))
    first[:n, :n] = own
    first[:n, n], first[:n, n + 2] = lift[:, n], lift[:, n + 1]
    first[n, n + 1], first[n, 0] = 1.0, lift[n - 2, n + 1]
    first[n + 1, n + 3] = 1.0
    first[n + 1, :n] = lift[0, n] * sent[0]
    return sent, first, lift_line(n // 2)


def fine_tables(px):
    q = LANES // px
    ends = np.zeros((2, px))
    ends[0, px - 1], ends[0, px - 2], ends[1, 0] = 1.0, -0.5, 1.0
    edges = np.zeros((8, LANES))
    place = np.zeros((16, LANES))
    for z in range(2):
        for x in range(2):
            edges[2 * z + x, 2 - 2 * z :: q] = ends[x]
            for lane in ((2,), (0, 1))[z]:
                place[2 * z + x : 12 : 4, (LANES - q) * x + lane] = 1.0
    result = (lift_line(LANES)[:, :LANES].T, edges, place)
    return tuple(table.astype(jnp.bfloat16) for table in result)


def middle_tables(ax, ay, az):
    step = LANES // az
    sent_x, first_x, second_x = line_tables(ax)
    sent_y, first_y, second_y = line_tables(ay)
    sent_z, first_z, second_z = line_tables(az)
    finer = lift_line(2 * ay)
    low, high = finer[0, 2 * ay], finer[2 * ay - 2, 2 * ay + 1]
    after = sent_y[2, 0] * first_y[:, ay + 2] + sent_y[3, 0] * first_y[:, ay + 3]
    before = sent_y[0, ay - 1] * first_y[:, ay] + sent_y[1, ay - 1] * first_y[:, ay + 1]
    first_y = np.concatenate((first_y, np.stack((low * after, high * before), axis=1)), axis=1)
    own = [(x, y) for x in range(ax) for y in range(ay)]
    corners = [(x, 2 * g + y) for g in range(2) for x in range(4) for y in range(2)]
    extra = []
    for start in range(2):
        extra += [(ax + k, y) for k in (start, start + 2) for y in range(ay)]
        extra += [(x, ay + k) for k in (start, start + 2) for x in range(ax)]
    extra += [(ax + x, ay + y) for x, y in corners]
    pair = 2 * ax + 2 * ay
    by_x = extra[: 2 * ay] + extra[pair : pair + 2 * ay]
    by_y = extra[2 * ay : pair] + extra[pair + 2 * ay :]
    extra += [(x, ay + 4 + k) for k in range(2) for x in range(ax)]
    extra += [(ax + x, ay + 4 + k) for x in range(4) for k in range(2)]
    taken = np.array(own + extra)
    given = own + [(ax + k, y) for k in range(2) for y in range(0, ay, 2)]
    given += [(x, ay + k) for k in range(2) for x in range(0, ax, 2)]
    given += [(ax + x, ay + y) for x in range(2) for y in range(2)]
    height = -(-len(given) // 16) * 16

    whole_x, whole_y = np.concatenate((np.eye(ax), sent_x)), np.concatenate((np.eye(ay), sent_y))
    ox, oy = np.array(own).T
    sends = []
    for kinds in (by_y, by_x):
        ex, ey = np.array(kinds).T
        sends.append(whole_x[np.ix_(ex, ox)] * whole_y[np.ix_(ey, oy)])
    sends.append(np.zeros((16, 2 * ax)))
    sends[2][:8] = np.kron(sent_x, np.eye(2)).reshape(8, ax, 2).transpose(0, 2, 1).reshape(8, -1)
    gx, gy = np.array(given).T
    tx, ty = taken.T
    rows = np.zeros((height, len(taken) + 8))
    rows[: len(given), : len(taken)] = first_x[np.ix_(gx, tx)] * first_y[np.ix_(gy, ty)]

    def spot(at, n):
        return np.where(at >= n, n // 2 + at - n, at // 2)

    half = np.array([(x, y) for x in range(ax // 2) for y in range(ay // 2)])
    use = ((gx % 2 == 0) | (gx >= ax)) & ((gy % 2 == 0) | (gy >= ay))
    last = np.zeros((len(half), height))
    pick_x = second_x[np.ix_(half[:, 0], spot(gx, ax))]
    pick_y = second_y[np.ix_(half[:, 1], spot(gy, ay))]
    last[:, : len(given)] = pick_x * pick_y * use

    lanes = np.arange(az) * step
    out = np.concatenate((lanes, [1, step + 1]))
    send_lanes = np.zeros((8, LANES))
    send_lanes[np.ix_(np.arange(4), lanes)] = sent_z
    along = np.zeros((LANES, LANES))
    along[np.ix_(lanes, out)] = first_z[:, :az].T
    rim = np.zeros((16, LANES))
    for part in range(3):
        rim[np.ix_(4 * part + np.arange(4), out)] = first_z[:, az:].T
    along_last = np.zeros((LANES, LANES))
    source = np.concatenate((lanes[0::2], [1, step + 1]))
    along_last[np.ix_(source, lanes[0::2])] = second_z.T
    last = np.concatenate(cut_table(last @ rows))
    along = np.concatenate((along, along @ along_last), axis=1)
    rim = np.concatenate((rim, rim @ along_last), axis=1)
    result = (*sends, rows[: len(own)], last, send_lanes, along, np.roll(along, 1, 0), rim)
    return tuple(table.astype(jnp.bfloat16) for table in result)


def iota(shape, axis):
    return lax.broadcasted_iota(jnp.int32, shape, axis)


def roll(values, shift, axis):
    return pltpu.roll(values, shift % values.shape[axis], axis)


def lift_rows(v, low, high):
    n = v.shape[0]
    row = iota(v.shape, 0)
    odd = row % 2 == 1
    up = jnp.where(row == n - 1, high, roll(v, -1, 0))
    w = jnp.where(odd, v - 0.5 * (roll(v, 1, 0) + up), v)
    down = jnp.where(row == 0, low - 0.5 * v, roll(w, 1, 0))
    return jnp.where(odd, w, w + 0.25 * (down + roll(w, -1, 0)))


def lift_groups(v, rim, s):
    lane = iota(v.shape, 1)
    odd = (lane // s) % 2 == 1
    up = jnp.where(lane >= LANES - s, rim, roll(v, -s, 1))
    w = jnp.where(odd, v - 0.5 * (roll(v, s, 1) + up), v)
    down = jnp.where(lane < s, rim - 0.5 * v, roll(w, s, 1))
    return jnp.where(odd, w, w + 0.25 * (down + roll(w, -s, 1)))


def shrink(v, thresh):
    return v - jnp.clip(v, -thresh, thresh)


def three(v):
    parts = []
    for _ in range(3):
        parts.append(v.astype(jnp.bfloat16))
        v = v - parts[-1].astype(jnp.float32)
    return parts


def mix(a, b, dims):
    return lax.dot_general(a, b, (dims, ((), ())), preferred_element_type=jnp.float32)


def mix_rows(table, v):
    wide = mix(table, jnp.concatenate(three(v), axis=1), ((1,), (0,)))
    return wide[:, :LANES] + wide[:, LANES : 2 * LANES] + wide[:, 2 * LANES :]


def doubled(v, n):
    return v[0:n] + v[n:]


def mix_lanes(v, table):
    return mix(jnp.concatenate(three(v), axis=1), jnp.concatenate([table] * 3, axis=0), ((1,), (0,)))


def total(v):
    return jnp.sum(jnp.sum(v, axis=0, keepdims=True), axis=1, keepdims=True)


def kernel(sizes, cells, exps_in, field_in, rows_in, lanes_in, *rest):
    tables_in, (out, stats), scratch = rest[:TABLES], rest[TABLES : TABLES + 2], rest[TABLES + 2 :]
    nx, ny, nz = sizes
    ndev = nx * ny * nz
    scratch = list(scratch)
    tables = scratch[-TABLES:]
    scratch = scratch[:-TABLES]
    field, exps, k_s, l_s, in_sem = scratch[-5:]
    scratch = scratch[:-5]
    pairs = [(field_in, field), (exps_in, exps), *zip(tables_in, tables), (rows_in, k_s), (lanes_in, l_s)]
    loads = [pltpu.make_async_copy(a, b, in_sem.at[i]) for i, (a, b) in enumerate(pairs)]
    me = (lax.axis_index("gx"), lax.axis_index("gy"), lax.axis_index("gz"))

    def device(dx, dy, dz):
        return (
            lax.rem(me[0] + (dx + nx), nx),
            lax.rem(me[1] + (dy + ny), ny),
            lax.rem(me[2] + (dz + nz), nz),
        )

    def distance(spot):
        return sum(min(d, size - d) for d, size in zip(spot, sizes))

    def thresh(level):
        return jnp.exp2(jnp.full((1, LANES), exps[level].astype(jnp.float32)))

    def split(j):
        return j // (ny * nz), (j // nz) % ny, j % nz

    def launch(copies, send_sem, recv_sem):
        flights = [
            pltpu.make_async_remote_copy(
                src_ref=f, dst_ref=t, send_sem=send_sem, recv_sem=recv_sem,
                device_id=device(*d), device_id_type=MESH,
            )
            for f, t, d in copies
        ]
        for flight in flights:
            flight.start()
        return sum(t.size for _, t, _ in copies) // LANES

    def settle(span, send_sem, recv_sem):
        for sem in (recv_sem, send_sem):
            pltpu.make_async_copy(span, span, sem).wait()

    barrier = pltpu.get_barrier_semaphore()

    near = max(sizes) // 2 <= ROUNDS
    greeted = {
        tuple((d + size - 1) % size if near else d for d, size in zip(spot, sizes))
        for spot in np.ndindex(*(3, 3, 3) if near else sizes)
    } - {(0, 0, 0)}
    for spot in sorted(greeted, key=lambda spot: (-distance(spot), spot)):
        pl.semaphore_signal(barrier, inc=1, device_id=device(*spot), device_id_type=MESH)
    for load in loads:
        load.start()
    gath, msg, parts_s, final_s, tally_s, tallies, g_send, g_recv, t_send, t_recv = scratch[-10:]
    loads[0].wait()
    loads[1].wait()
    step_to = (1, -1)
    alone = nx == 2
    ways = (0,) if alone else (0, 1)
    (xs, xh, xe, xr, ys, yr, es, er, yl, zs, zr, ds, dr, ts, txr, tcr, rim, work, send_sem, recv_sem) = scratch[:BUFFERS]
    middle = scratch[BUFFERS : BUFFERS + 15]
    grown, lifted, sent, edge1, side, hz, xzr, t2r, t3r, o1s, o2s, m_send, m_recv, y_send, y_recv = middle
    fine_lanes, fine_edges, fine_place, reach_rows, reach_lanes, *tables = tables
    src = field.at[0]
    px, n = src.shape[0], src.shape[1]
    half, q = n // 2, LANES // px
    lane = iota((n, LANES), 1)
    row8 = iota((8, LANES), 0)

    def ends(v):
        return v[n - 1 : n] - 0.5 * v[n - 2 : n - 1], v[0:1]

    def under(pair):
        return jnp.where(row8 == 0, pair[0], jnp.where(row8 == 1, pair[1], 0.0))

    lane_half = iota((half, LANES), 1)
    share = jnp.where(lane_half == LANES - 2, -0.125, jnp.where(lane_half == 0, 0.25, 0.0))
    share = jnp.where(lane_half == LANES - 1, -0.5, share)
    level_thresh = thresh(0)
    row = iota((half, LANES), 0)
    ax, ay = px // 2, half
    own = ax * ay
    px_rows, py_rows = 2 * ay, 2 * ax
    pair = px_rows + py_rows
    send_y, send_x, send_q, rows1, rows2, send_lanes, lanes12, odd_lanes12, rim12 = tables
    none = jnp.zeros((1, LANES), jnp.float32)

    def halves(ref, x):
        return [ref[x, pl.ds(start, half, stride=2), :] for start in (0, 1)]

    def stored(x):
        return [work[x, 0:half], work[x, half:]]

    def lift_halves(v, below, above):
        even, odd = v
        after = jnp.where(row == half - 1, above, roll(even, -1, 0))
        detail = odd - 0.5 * (even + after)
        before = jnp.where(row == 0, below - 0.5 * even, roll(detail, 1, 0))
        return [even + 0.25 * (before + detail), detail]

    def lift_last(stack, border):
        whole = mix_lanes(jnp.concatenate([v for v, _, _ in stack], axis=0), fine_lanes[...])
        for i, (_, x, kind) in enumerate(stack):
            yield x, kind, whole[half * i : half * i + half] + roll(border[kind], LANES - 2 - q * x, 1) * share

    def sideways(parts, target):
        edges = sum(mix(send_lanes[...], part, ((1,), (1,))) for part in three(jnp.concatenate(parts, axis=0)))
        for g in (0, 1):
            target[g, :, pl.ds(target.shape[2] - LANES, LANES)] = jnp.zeros((2, LANES), jnp.float32)
            target[g, :, pl.ds(0, edges.shape[1])] = edges[2 * g : 2 * g + 2]

    def both_kinds(a, b):
        return jnp.where(iota(a.shape, 1) % 2 == 0, a, roll(b, 1, 1))

    planes = (src[px - 1] - 0.5 * src[px - 2], src[0])
    ys[0] = src[:, n - 1, :] - 0.5 * src[:, n - 2, :]
    ys[1] = src[:, 0, :]
    for gx in (0, 1):
        xs[gx] = planes[gx]
        xh[gx, 0:half], xh[gx, half:] = lift_halves(halves(xs, gx), none, none)
        es[2 * gx], es[2 * gx + 1] = ends(planes[gx])
    packed = jnp.zeros((n, LANES), jnp.float32)
    for x in range(px):
        packed = jnp.where(lane // q == x, roll(src[x], q * x + 2, 1), packed)
    odd_end = roll(packed - 0.5 * roll(packed, 1, 1), 1, 1)
    even_end = jnp.where(lane % q == 1, roll(packed, -1, 1), roll(packed, -2, 1))
    packed = jnp.where(lane % q == 2, odd_end, even_end)
    zs[...] = packed
    ds[0], ds[1] = ends(packed)
    for load in loads[2:5]:
        load.wait()
    edges = sum(
        mix(fine_edges[...], part, ((1,), (1,)))
        for part in three(jnp.concatenate((packed, under(ends(packed))), axis=0))
    )
    ts[...] = jnp.zeros(ts.shape, jnp.float32)
    for g in (0, 1):
        ts[g, :, pl.ds(0, n + 8)] = edges[2 * g : 2 * g + 2]

    pl.semaphore_wait(barrier, len(greeted))
    along_y, others = [], []
    for g in (0, 1):
        dz = step_to[g]
        for gx in ways:
            for gy in (0, 1):
                along_y.append((ts.at[g], tcr.at[g, gy, gx], (step_to[gx], step_to[gy], dz)))
            others.append((ts.at[g], txr.at[g, gx], (step_to[gx], 0, dz)))
        for gy in (0, 1):
            along_y.append((ds.at[gy], dr.at[2 * g + gy], (0, step_to[gy], dz)))
    for gx in (0, 1):
        for gy in (0, 1):
            along_y.append((es.at[2 * gx + gy], er.at[2 * gx + gy], (step_to[gx], step_to[gy], 0)))
    for g in (0, 1):
        along_y.append((ys.at[g], yr.at[g], (0, step_to[g], 0)))
    for g in (0, 1):
        ends_of = pl.ds(2 * g, 2)
        others.append((es.at[ends_of], xe.at[ends_of], (step_to[g], 0, 0)))
    for g in (0, 1):
        others.append((xh.at[g, pl.ds(0, half)], xr.at[g, pl.ds(0, half)], (step_to[g], 0, 0)))
        along_y.append((xh.at[g, pl.ds(half, half)], xr.at[g, pl.ds(half, half)], (step_to[g], 0, 0)))
    for g in (0, 1):
        others.append((zs, zr.at[g], (0, 0, step_to[g])))
    y_rows = launch(along_y[:-2], y_send, y_recv)
    sent_rows = launch(others, send_sem, recv_sem)
    y_rows += launch(along_y[-2:], y_send, y_recv)

    for load in loads[5 : 2 + TABLES]:
        load.wait()
    even = halves(src, 0)
    before = [-0.5 * e for e in even]
    stack = []
    for k in range(px // 2):
        after = halves(src, 2 * k + 2) if 2 * k + 2 < px else [0.0, 0.0]
        detail = [o - 0.5 * (e + a) for o, e, a in zip(halves(src, 2 * k + 1), even, after)]
        smooth = [e + 0.25 * (b + d) for e, b, d in zip(even, before, detail)]
        for x, v in ((2 * k, smooth), (2 * k + 1, detail)):
            work[x, 0:half], work[x, half:] = lift_halves(v, none, none)
        even, before = after, detail
    for start in range(0, px, 2 * BATCH):
        block = jnp.concatenate([work[x, 0:half] for x in range(start, start + 2 * BATCH, 2)], axis=0)
        grown[pl.ds(start // 2 * half, BATCH * half), :] = mix_lanes(block, fine_lanes[...])
    settle(grown.at[pl.ds(0, sent_rows)], send_sem, recv_sem)

    lane2, row2 = iota((2, LANES), 1), iota((2, LANES), 0)

    def both(ref):
        return ref[0] if alone else jnp.where(row2 == 0, ref[0], ref[1])

    def columns(top, table):
        pieces = [part.astype(jnp.float32) for part in three(top)]
        pieces.append(jnp.zeros_like(top))
        return mix(jnp.concatenate(pieces, axis=0).astype(jnp.bfloat16), table, ((0,), (0,)))

    def kinds(a, b):
        return jnp.where(iota(a.shape, 1) % q == 2, a, b)

    tops = [jnp.where(lane2 < n, both(txr.at[g]), 0.0) for g in (0, 1)]
    beside = columns(jnp.concatenate(tops, axis=0), fine_place[...])[0:n]
    v = lift_groups(kinds(zr[0], zr[1]), beside, q)
    outer_rims = ends(v)
    lifted[...] = v
    rim[...] = lift_rows(v, none, none)
    border = [rim[pl.ds(0, half, stride=2), :]]
    near_x = mix_lanes(jnp.concatenate((xr[0, 0:half], xr[1, 0:half]), axis=0), fine_lanes[...])
    terms = {0: 0.25 * near_x[0:half], px - 2: -0.125 * near_x[half:]}
    for x in range(0, px, 2):
        spot = (pl.ds(x // 2 * half, half), slice(None))
        v = roll(border[0], LANES - 2 - q * x, 1) * share
        grown[spot] = grown[spot] + (v + terms[x] if x in terms else v)
    halo = mix_rows(send_y[...], grown[0:own])
    halo = (halo[0:py_rows], halo[py_rows : 2 * py_rows], halo[2 * py_rows :])
    sent[px_rows:pair] = both_kinds(halo[0], halo[1])
    sent[pair : pair + 16] = halo[2]
    blank = jnp.zeros((px_rows, LANES), jnp.float32)
    sideways((blank, halo[0], blank, halo[1], halo[2]), edge1)
    copies = []

    def rows_copy(start, size, to):
        copies.append((sent.at[pl.ds(start, size)], grown.at[pl.ds(own + start, size)], to))

    parts = len(ways)
    for g in (0, 1):
        for gy in (0, 1):
            for gx in ways:
                copies.append((edge1.at[g, :, pl.ds(LANES, LANES)], t3r.at[g, gy, gx], (step_to[gx], step_to[gy], step_to[g])))
            copies.append((edge1.at[g, :, pl.ds(0, LANES)], t2r.at[g, gy], (0, step_to[gy], step_to[g])))
    for gy in (0, 1):
        for gx in ways:
            rows_copy(pair + 8 * gy + 4 * gx, 8 // parts, (step_to[gx], step_to[gy], 0))
    for gy in (0, 1):
        rows_copy(px_rows + ax * gy, ax, (0, step_to[gy], 0))
    sent_rows = launch(copies, m_send, m_recv)
    def along_x(rims):
        rows = jnp.concatenate([yl[g, pl.ds(0, ax, stride=2), :] for g in (0, 1)], axis=0)
        turned = []
        for v in rims:
            v = jnp.broadcast_to(v, (8, LANES))
            for start in range(0, ax, 8):
                tile = jnp.zeros((8, LANES), jnp.float32)
                for i in range(8):
                    tile = jnp.where(row8 == i, roll(v, LANES - 2 - 2 * q * (start + i), 1), tile)
                turned.append(tile)
        return mix_lanes(rows, fine_lanes[...]) + jnp.concatenate(turned, axis=0) * share[0:1]

    beyond = [(xe[2 * g], xe[2 * g + 1]) for g in (0, 1)]
    for g in (0, 1):
        yl[g] = lift_rows(ys[g], beyond[0][g], beyond[1][g])
    raw = along_x(outer_rims)
    grown[pl.ds(own + pair + 16, py_rows), :] = raw
    grown[pl.ds(own + pair + 24 + py_rows, 8), :] = jnp.zeros((8, LANES), jnp.float32)
    settle(grown.at[pl.ds(0, y_rows)], y_send, y_recv)

    tops = []
    for g in (0, 1):
        yl[g] = lift_rows(yr[g], er[g], er[2 + g])
        v = jnp.where(lane2 == n, both(tcr.at[g, 0]), both(tcr.at[g, 1]))
        tops.append(jnp.where(lane2 // 2 == n // 2, v, 0.0))
    beside = columns(jnp.concatenate(tops, axis=0), fine_place[...])[n : n + 8]
    lower = lift_groups(under((kinds(dr[0], dr[2]), kinds(dr[1], dr[3]))), beside, q)
    lower = (lower[0:1], lower[1:2])
    late = along_x(lower)
    for at, scale, v in ((0, 0.25, late[0:ax]), (ay - 1, -0.125, late[ax:])):
        spot = (pl.ds(at, ax, stride=ay), slice(None))
        grown[spot] = grown[spot] + scale * v

    def finish():
        energy = kept = jnp.zeros((half, LANES), jnp.float32)
        rim[...] = lift_rows(lifted[...], *lower)
        border = [rim[pl.ds(start, half, stride=2), :] for start in (0, 1)]

        def fixed(x):
            smooth, detail = stored(x)
            for plane, kind, scale in ((0, 0, 0.25), (px - 2, 1, -0.125), (px - 1, 1, -0.5)):
                if x == plane:
                    smooth = smooth + scale * xr[kind, 0:half]
                    detail = detail + scale * xr[kind, half:]
            below, above = yl[0, x : x + 1, :], yl[1, x : x + 1, :]
            smooth = smooth + jnp.where(row == 0, 0.25 * below, jnp.where(row == half - 1, -0.125 * above, 0.0))
            return smooth, detail + jnp.where(row == half - 1, -0.5 * above, 0.0)

        for start in range(0, px, 4):
            stack, ready = [], []
            for x in range(start, start + 4, 2):
                ready.append((x, 0, grown[pl.ds(x // 2 * half, half), :]))
                stack.append((fixed(x)[1], x, 1))
                whole = fixed(x + 1)
                stack += [(whole[0], x + 1, 0), (whole[1], x + 1, 1)]
            for x, kind, v in (*ready, *lift_last(stack, border)):
                small = shrink(v, level_thresh)
                out[0, x, pl.ds(kind, half, stride=2), :] = small
                square, size = v * v, jnp.abs(small)
                if x % 2 == 0 and kind == 0:
                    square, size = (jnp.where(lane_half % 2 == 0, 0.0, u) for u in (square, size))
                energy += square
                kept += size
        return [total(energy), total(kept)]

    here = grown[0:own]
    halo = mix_rows(send_x[...], here)
    corner = mix_rows(send_q[...], raw)[0:8]
    sent[0:px_rows] = both_kinds(halo[0:px_rows], halo[px_rows:])
    sent[pair + 16 :] = corner
    blank = jnp.zeros((py_rows, LANES), jnp.float32)
    filled = jnp.zeros((16, LANES), jnp.float32)
    sideways((here, halo[0:px_rows], blank, halo[px_rows:], blank, filled, raw, corner, filled[0:8]), side)
    copies = []
    for g in (0, 1):
        for gx in ways:
            copies.append((side.at[g, :, pl.ds(own, 2 * LANES)], xzr.at[g, gx], (step_to[gx], 0, step_to[g])))
        copies.append((side.at[g], hz.at[g], (0, 0, step_to[g])))
    for gx in ways:
        size = 8 // parts
        at = own + pair + 16 + py_rows + size * gx
        copies.append((sent.at[pl.ds(pair + 16 + size * gx, size)], grown.at[pl.ds(at, size)], (step_to[gx], 0, 0)))
        rows_copy(ay * gx, px_rows // parts, (step_to[gx], 0, 0))
    sent_rows += launch(copies, m_send, m_recv)
    extra = 2 * pair + 16 + py_rows + 16

    spots = nx * ny
    slot = (me[2] * nx + me[0]) * ny + me[1]
    cx, cy, cz = ax // 4, ay // 4, LANES // 2**FINE
    step = 2**FINE
    count = cx * cy
    long, deep, reach = cx + 3, cy + 3, cz + 3
    cut = LANES - reach * (deep - 1)
    rest = reach - cut

    def spread(source, target, send_sem, recv_sem, first=0, last=None):
        def post(j):
            return pltpu.make_async_remote_copy(
                src_ref=source, dst_ref=target, send_sem=send_sem, recv_sem=recv_sem,
                device_id=device(*split(j)), device_id_type=MESH,
            )

        def send(j, carry):
            post(j).start()
            return carry

        if ndev <= 32:
            order = sorted(range(1, ndev), key=lambda j: (-distance(split(j)), j))
            for j in order[first:last]:
                post(j).start()
        elif first == 0:
            lax.fori_loop(1, ndev, send, 0)

    pieces = mix_rows(reach_rows[...], here)
    pieces = doubled(pieces, 8 * deep)
    blocks = [part.astype(jnp.float32) for part in three(pieces)]

    def stack(first, last):
        rows = [jnp.concatenate([b[8 * y : 8 * y + 8] for y in range(first, last)], axis=1) for b in blocks]
        return jnp.concatenate(rows + [jnp.zeros_like(rows[0])], axis=0).astype(jnp.bfloat16)

    def fold(v):
        return v[0:8] + v[8:16] + v[16:24]

    sheet = fold(mix(stack(0, deep), reach_lanes[pl.ds(0, deep * LANES), :], ((1,), (0,))))
    loose = fold(mix(stack(deep - 1, deep), reach_lanes[pl.ds(deep * LANES, LANES), :], ((1,), (0,))))
    spare = loose[0:1]
    for x in range(1, long):
        spare += roll(loose[x : x + 1], rest * x, 1)
    msg[...] = jnp.where(row8 == long, spare, sheet)
    spread(msg, gath.at[slot], g_send, g_recv, 0, ndev // 2)
    gath[slot] = msg[...]
    sums = finish()
    quarter = own // 4

    def level_rows(v, columns):
        return (
            mix_rows(rows1[:, columns], v[:, 0:LANES]),
            doubled(mix_rows(rows2[:, columns], v[:, LANES:]), quarter),
        )

    o1s[...], early = level_rows(mix_lanes(here, lanes12[...]), pl.ds(0, own))
    o2s[...] = early.reshape(o2s.shape)
    spread(msg, gath.at[slot], g_send, g_recv, ndev // 2)
    settle(grown.at[pl.ds(0, sent_rows)], m_send, m_recv)

    for g in (0, 1):
        across = (xzr.at[g, 0], xzr.at[g, 0 if alone else 1])
        place_in = lane2 % pair
        v = jnp.where(place_in < ay, across[0][:, 0:LANES], across[1][:, 0:LANES])
        v = jnp.where(place_in < px_rows, v, jnp.where(place_in < px_rows + ax, t2r[g, 0], t2r[g, 1]))
        hz[g, :, pl.ds(own, LANES)] = v
        u = []
        for gy in (0, 1):
            u.append(jnp.where(lane2 % 8 < 4, t3r[g, gy, 0], t3r[g, gy, 0 if alone else 1]))
        v = jnp.where(lane2 < 8, u[0], u[1])
        w = jnp.where(lane2 < 20 + py_rows, across[0][:, LANES:], across[1][:, LANES:])
        w = jnp.where(lane2 < 16 + py_rows, hz[g, :, pl.ds(own + LANES, LANES)], w)
        v = jnp.where(lane2 < 16, v, jnp.where(lane2 < 24 + py_rows, w, 0.0))
        hz[g, :, pl.ds(own + LANES, LANES)] = v
    rim_rows = columns(jnp.concatenate((hz[0], hz[1]), axis=0), rim12[...])
    got = grown[pl.ds(own, extra - pair), :]
    outer = mix_lanes(got, lanes12[...])
    outer = (outer[0:pair], mix_lanes(got[0:pair], odd_lanes12[...]), outer[pair:])
    outer = jnp.concatenate(outer, axis=0) + rim_rows[own : own + extra]
    late = level_rows(jnp.concatenate((rim_rows[0:own], outer), axis=0), pl.ds(0, own + extra))
    first = o1s[...] + late[0]
    second = o2s[...].reshape(quarter, LANES) + late[1]
    o1s[...] = first
    o2s[...] = second.reshape(o2s.shape)

    def tally(v, level, ny):
        s = 2**level
        row, at = iota(v.shape, 0), iota(v.shape, 1)
        smooth = ((row // ny) % 2 == 0) & (row % 2 == 0) & (at % (2 * s) == 0)
        use = (at % s == 0) & ~smooth
        small = shrink(v, thresh(level))
        return [total(jnp.where(use, v * v, 0.0)), total(jnp.where(use, jnp.abs(small), 0.0))]

    sums += tally(first, 1, ay) + tally(second, 2, ay // 2)

    def place(source, level):
        s = 2**level
        small_y = ay >> (level - 1)
        keep = iota((small_y, LANES), 1) % s == 0
        for x in range(ax >> (level - 1)):
            spot = (0, s * x, pl.ds(0, small_y, stride=s), slice(None))
            out[spot] = jnp.where(keep, shrink(source(x), thresh(level)), out[spot])

    one = iota((1, LANES), 1)
    tail = jnp.zeros((1, LANES), jnp.float32)
    for i, whole in enumerate(sums):
        tail = jnp.where(one == i, whole, tail)
    tally_s[...] = tail
    spread(tally_s, tallies.at[slot], t_send, t_recv)
    tallies[slot] = tail
    place(lambda x: o1s[pl.ds(x * ay, ay), :], 1)
    place(lambda x: o2s[x], 2)
    settle(gath.at[pl.ds(0, ndev - 1)], g_send, g_recv)

    at = iota((spots, LANES), 1)
    spares = [gath[pl.ds(z * spots, spots), long, :] for z in range(nz)]

    def window(v, source, start, size):
        moved = roll(v, start - source, 1)
        return jnp.where((at >= start) & (at < start + size), moved, 0.0)

    for x in range(long):
        boxes = [gath[pl.ds(z * spots, spots), x, :] for z in range(nz)]
        for y in range(deep):
            fit = reach if y < deep - 1 else cut
            v = sum(window(boxes[z], reach * y, cz * z, fit) for z in range(nz))
            if fit < reach:
                v += sum(window(spares[z], rest * x, cz * z + cut, rest) for z in range(nz))
            parts_s[pl.ds((y * long + x) * spots, spots), :] = v

    filled = long * deep * spots
    spare_rows = parts_s.shape[0] - filled
    if spare_rows:
        parts_s[pl.ds(filled, spare_rows), :] = jnp.zeros((spare_rows, LANES), jnp.float32)
    grid = parts_s[...]
    loads[2 + TABLES].wait()
    loads[3 + TABLES].wait()
    cells_in = spots * count
    grid = mix_rows(k_s[...], grid)
    half3, half4 = grid[0:cells_in], doubled(grid[cells_in:], cells_in)
    grid, grid4 = mix_lanes(half3, l_s[0]), mix_lanes(half4, l_s[1])
    row = iota(grid.shape, 0)
    lane = iota(grid.shape, 1)
    inner_row = row % count
    gx, gy, gz = inner_row // cy, inner_row % cy, lane // step
    valid = lane % step < nz
    even3 = (gx % 2 == 0) & (gy % 2 == 0) & (gz % 2 == 0)
    even4 = (gx % 4 == 0) & (gy % 4 == 0) & (gz % 4 == 0)
    det3 = valid & ~even3
    det4 = valid & even3 & ~even4
    small3 = shrink(grid, thresh(FINE))
    small4 = shrink(grid4, thresh(FINE + 1))
    final_s[...] = jnp.where(even3, jnp.where(even4, grid4, small4), small3)

    def masked(mask, v):
        return total(jnp.where(mask, v, 0.0))

    coarse = ((masked(det3, grid * grid), masked(det3, jnp.abs(small3))),
              (masked(det4, grid4 * grid4), masked(det4, jnp.abs(small4))))
    first = pl.multiple_of((me[0] * ny + me[1]) * count, count)
    mine = pltpu.roll(final_s[pl.ds(first, count), :], lax.rem(LANES - me[2], LANES), 1)
    keep = iota((cy, LANES), 1) % step == 0
    for x in range(cx):
        spot = (0, step * x, pl.ds(0, cy, stride=step), slice(None))
        out[spot] = jnp.where(keep, mine[x * cy : x * cy + cy], out[spot])

    settle(tallies.at[pl.ds(0, ndev - 1)], t_send, t_recv)
    tail = jnp.sum(tallies[...], axis=0)
    for q in (0, 1):
        line = jnp.zeros((1, LANES), jnp.float32)
        for level in range(LEVELS):
            weight = 8.0 ** (level + 1) / (7.0 * cells)
            if level < FINE:
                value = jnp.sum(jnp.where(one == 2 * level + q, tail, 0.0), axis=1, keepdims=True)
            else:
                value = coarse[level - FINE][q]
            line = jnp.where(one == level, value * weight, line)
        stats[q] = line[:, 0:LEVELS]


def deliver(held, held_stats, out, stats, sem):
    rows = held.shape[1] // CHUNKS
    copies = [pltpu.make_async_copy(held_stats, stats, sem.at[CHUNKS])]
    for i in range(CHUNKS):
        part = pl.ds(i * rows, rows)
        copies.append(pltpu.make_async_copy(held.at[:, part], out.at[:, part], sem.at[i]))
    for copy in copies:
        copy.start()
    for copy in copies:
        copy.wait()


def shards(sizes, fields, exponents):
    nx, ny, nz = sizes
    ndev = nx * ny * nz
    _, lx, ly, lz = fields.shape
    cells = fields.size * ndev
    step = 2**FINE
    coarse = (lx // step, ly // step, lz // step)
    count = coarse[0] * coarse[1]
    tables = coarse_matrices(sizes, coarse)
    middle = middle_tables(lx // 2, ly // 2, lz // 2)
    own, extra = lx // 2 * (ly // 2), middle[0].shape[0]
    middle = fine_tables(lx) + reach_tables(lx // 2, ly // 2, lz // 2) + middle
    scratch = [
        *(pltpu.VMEM(shape, jnp.float32) for shape in (
            (2, ly, LANES), (2, ly, LANES), (4, 1, LANES), (2, ly, LANES), (2, lx, LANES), (2, lx, LANES),
            (4, 1, LANES), (4, 1, LANES),
            (2, lx, LANES), (ly, LANES), (2, ly, LANES), (2, 1, LANES), (4, 1, LANES), (2, 2, LANES),
            (2, 2, 2, LANES), (2, 2, 2, 2, LANES), (ly, LANES), (lx, ly, LANES),
        )),
        pltpu.SemaphoreType.DMA,
        pltpu.SemaphoreType.DMA,
        *(pltpu.VMEM(shape, jnp.float32) for shape in (
            (own + 2 * lx + ly + 32, LANES), (ly, LANES), (lx + ly + 24, LANES), (2, 2, 2 * LANES),
            (2, 2, own + 2 * LANES), (2, 2, own + 2 * LANES), (2, 2, 2, 2 * LANES), (2, 2, 2, LANES),
            (2, 2, 2, 2, LANES), (own, LANES), (lx // 4, ly // 4, LANES),
        )),
        pltpu.SemaphoreType.DMA,
        pltpu.SemaphoreType.DMA,
        pltpu.SemaphoreType.DMA,
        pltpu.SemaphoreType.DMA,
    ]
    scratch += [
        pltpu.VMEM((ndev, 8, LANES), jnp.float32),
        pltpu.VMEM((8, LANES), jnp.float32),
        pltpu.VMEM((tables[0].shape[1], LANES), jnp.float32),
        pltpu.VMEM((nx * ny * count, LANES), jnp.float32),
        pltpu.VMEM((1, LANES), jnp.float32),
        pltpu.VMEM((ndev, 1, LANES), jnp.float32),
        *[pltpu.SemaphoreType.DMA] * 4,
        pltpu.VMEM(fields.shape, jnp.float32),
        pltpu.SMEM(exponents.shape, jnp.int32),
        pltpu.VMEM(tables[0].shape, jnp.bfloat16),
        pltpu.VMEM(tables[1].shape, jnp.bfloat16),
        pltpu.SemaphoreType.DMA((4 + TABLES,)),
        *(pltpu.VMEM(table.shape, table.dtype) for table in middle),
    ]
    vmem = pl.BlockSpec(memory_space=pltpu.VMEM)
    held = pl.pallas_call(
        functools.partial(kernel, sizes, cells),
        out_shape=(
            pltpu.VMEM(fields.shape, jnp.float32),
            pltpu.VMEM((2, 1, LEVELS), jnp.float32),
        ),
        in_specs=[pl.BlockSpec(memory_space=pltpu.HBM)] * (4 + TABLES),
        out_specs=(vmem, vmem),
        scratch_shapes=scratch,
        compiler_params=pltpu.CompilerParams(
            collective_id=0, has_side_effects=True, vmem_limit_bytes=VMEM_LIMIT
        ),
    )(*(pltpu.with_memory_space_constraint(x, pltpu.HBM) for x in (exponents, fields, *map(jnp.asarray, (*tables, *middle)))))
    hbm = pl.BlockSpec(memory_space=pltpu.HBM)
    return pl.pallas_call(
        deliver,
        out_shape=(
            jax.ShapeDtypeStruct(fields.shape, jnp.float32),
            jax.ShapeDtypeStruct((2, 1, LEVELS), jnp.float32),
        ),
        in_specs=(vmem, vmem),
        out_specs=(hbm, hbm),
        scratch_shapes=[pltpu.SemaphoreType.DMA((CHUNKS + 1,))],
    )(*(pltpu.with_memory_space_constraint(x, pltpu.VMEM) for x in held))


def solution(mesh):
    sizes = tuple(mesh.shape[name] for name in ("gx", "gy", "gz"))
    placed = (P(None, "gx", "gy", "gz"), P())
    return jax.shard_map(
        functools.partial(shards, sizes),
        mesh=mesh,
        in_specs=placed,
        out_specs=placed,
        check_vma=False,
    )
```

```python
import functools

import numpy as np

import jax
import jax.numpy as jnp
from jax import lax
from jax.experimental import pallas as pl
from jax.experimental.pallas import tpu as pltpu
from jax.sharding import PartitionSpec as P

FINE = 3
LEVELS = 5
LANES = 128
CHUNKS = 4
BUFFERS = 20
BATCH = 8
ROUNDS = 2
VMEM_LIMIT = 58_720_256
MESH = pl.DeviceIdType.MESH


def periodic_lift(length):
    eye = np.eye(length)
    even, odd = eye[0::2], eye[1::2]
    detail = odd - 0.5 * (even + np.roll(even, -1, 0))
    smooth = even + 0.25 * (np.roll(detail, 1, 0) + detail)
    whole = np.zeros((length, length))
    whole[0::2] = smooth
    whole[1::2] = detail
    return whole


def second_lift(length):
    whole = np.zeros((length, length))
    whole[0::2, 0::2] = periodic_lift(length // 2)
    return whole


def coarse_matrices(sizes, coarse):
    nx, ny, nz = sizes
    cx, cy, cz = coarse
    rows = np.arange(nx * ny * cx * cy)
    dev, inner = rows // (cx * cy), rows % (cx * cy)
    gx = (dev // ny) * cx + inner // cy
    gy = (dev % ny) * cy + inner % cy
    step = LANES // cz
    lanes = np.array([z * step + d for d in range(nz) for z in range(cz)])
    reach_y, reach_x, spot = np.indices((cy + 3, cx + 3, nx * ny)).reshape(3, -1)
    from_x = (spot // ny * cx + reach_x - 1) % (nx * cx)
    from_y = (spot % ny * cy + reach_y - 1) % (ny * cy)
    from_z = np.arange(-1, nz * cz + 2) % (nz * cz)
    result = []
    for both_levels in (False, True):
        mx, my, mz = periodic_lift(nx * cx), periodic_lift(ny * cy), periodic_lift(nz * cz)
        if both_levels:
            mx, my, mz = second_lift(nx * cx) @ mx, second_lift(ny * cy) @ my, second_lift(nz * cz) @ mz
        both = mx[gx[:, None], from_x[None]] * my[gy[:, None], from_y[None]]
        along = np.zeros((LANES, LANES))
        along[np.ix_(np.arange(len(from_z)), lanes)] = mz[:, from_z].T
        result.append((np.pad(both, ((0, 0), (0, -both.shape[1] % 16))), along.astype(jnp.bfloat16)))
    (one, along_one), (two, along_two) = result
    rows = np.concatenate((one.astype(jnp.bfloat16), *cut_table(two)))
    return rows, np.stack((along_one, along_two))


def cut_table(table):
    high = table.astype(jnp.bfloat16)
    low = (table - high.astype(np.float64)).astype(jnp.bfloat16)
    return high, low


def reach_line(n):
    twice = periodic_lift(3 * n // 2)[0::2] @ periodic_lift(3 * n)[0::2]
    return twice[n // 4 - 1 : n // 2 + 2, n : 2 * n]


def reach_tables(ax, ay, az):
    part_x, part_y, part_z = reach_line(ax), reach_line(ay), reach_line(az)
    wide, deep = len(part_z), len(part_y)
    rows = np.zeros((deep, 8, ax * ay))
    rows[:, : len(part_x)] = np.einsum("yb,xa->yxab", part_y, part_x).reshape(deep, -1, ax * ay)
    rows = rows.reshape(8 * deep, -1)
    along = np.zeros((deep + 1, LANES, LANES))
    for y in range(deep):
        fit = min(wide, LANES - wide * y)
        along[y, :: LANES // az, wide * y : wide * y + fit] = part_z[:fit].T
    along[deep, :: LANES // az, : wide - fit] = part_z[fit:].T
    return np.concatenate(cut_table(rows)), along.reshape(-1, LANES).astype(jnp.bfloat16)


def lift_line(n):
    whole = np.zeros((n, n + 2))
    cells = np.eye(n + 2)
    even, odd = cells[0:n:2], cells[1:n:2]
    after = np.concatenate((even[1:], cells[n + 1 :]))
    detail = odd - 0.5 * (even + after)
    before = np.concatenate((cells[n : n + 1] - 0.5 * even[:1], detail[:-1]))
    whole[0::2] = even + 0.25 * (before + detail)
    whole[1::2] = detail
    return whole

def line_tables(n):
    lift = lift_line(n)
    own = lift[:, :n]
    sent = np.zeros((4, n))
    sent[0, n - 1], sent[0, n - 2] = 1.0, -0.5
    sent[1] = own[n - 2] - 0.5 * own[n - 4]
    sent[2, 0] = 1.0
    sent[3] = own[0]
    first = np.zeros((n + 2, n + 4))
    first[:n, :n] = own
    first[:n, n], first[:n, n + 2] = lift[:, n], lift[:, n + 1]
    first[n, n + 1], first[n, 0] = 1.0, lift[n - 2, n + 1]
    first[n + 1, n + 3] = 1.0
    first[n + 1, :n] = lift[0, n] * sent[0]
    return sent, first, lift_line(n // 2)


def fine_tables(px):
    q = LANES // px
    ends = np.zeros((2, px))
    ends[0, px - 1], ends[0, px - 2], ends[1, 0] = 1.0, -0.5, 1.0
    edges = np.zeros((8, LANES))
    place = np.zeros((16, LANES))
    for z in range(2):
        for x in range(2):
            edges[2 * z + x, 2 - 2 * z :: q] = ends[x]
            for lane in ((2,), (0, 1))[z]:
                place[2 * z + x : 12 : 4, (LANES - q) * x + lane] = 1.0
    result = (lift_line(LANES)[:, :LANES].T, edges, place)
    return tuple(table.astype(jnp.bfloat16) for table in result)


def middle_tables(ax, ay, az):
    step = LANES // az
    sent_x, first_x, second_x = line_tables(ax)
    sent_y, first_y, second_y = line_tables(ay)
    sent_z, first_z, second_z = line_tables(az)
    finer = lift_line(2 * ay)
    low, high = finer[0, 2 * ay], finer[2 * ay - 2, 2 * ay + 1]
    after = sent_y[2, 0] * first_y[:, ay + 2] + sent_y[3, 0] * first_y[:, ay + 3]
    before = sent_y[0, ay - 1] * first_y[:, ay] + sent_y[1, ay - 1] * first_y[:, ay + 1]
    first_y = np.concatenate((first_y, np.stack((low * after, high * before), axis=1)), axis=1)
    own = [(x, y) for x in range(ax) for y in range(ay)]
    corners = [(x, 2 * g + y) for g in range(2) for x in range(4) for y in range(2)]
    extra = []
    for start in range(2):
        extra += [(ax + k, y) for k in (start, start + 2) for y in range(ay)]
        extra += [(x, ay + k) for k in (start, start + 2) for x in range(ax)]
    extra += [(ax + x, ay + y) for x, y in corners]
    pair = 2 * ax + 2 * ay
    by_x = extra[: 2 * ay] + extra[pair : pair + 2 * ay]
    by_y = extra[2 * ay : pair] + extra[pair + 2 * ay :]
    extra += [(x, ay + 4 + k) for k in range(2) for x in range(ax)]
    extra += [(ax + x, ay + 4 + k) for x in range(4) for k in range(2)]
    taken = np.array(own + extra)
    given = own + [(ax + k, y) for k in range(2) for y in range(0, ay, 2)]
    given += [(x, ay + k) for k in range(2) for x in range(0, ax, 2)]
    given += [(ax + x, ay + y) for x in range(2) for y in range(2)]
    height = -(-len(given) // 16) * 16

    whole_x, whole_y = np.concatenate((np.eye(ax), sent_x)), np.concatenate((np.eye(ay), sent_y))
    ox, oy = np.array(own).T
    sends = []
    for kinds in (by_y, by_x):
        ex, ey = np.array(kinds).T
        sends.append(whole_x[np.ix_(ex, ox)] * whole_y[np.ix_(ey, oy)])
    sends.append(np.zeros((16, 2 * ax)))
    sends[2][:8] = np.kron(sent_x, np.eye(2)).reshape(8, ax, 2).transpose(0, 2, 1).reshape(8, -1)
    gx, gy = np.array(given).T
    tx, ty = taken.T
    rows = np.zeros((height, len(taken) + 8))
    rows[: len(given), : len(taken)] = first_x[np.ix_(gx, tx)] * first_y[np.ix_(gy, ty)]

    def spot(at, n):
        return np.where(at >= n, n // 2 + at - n, at // 2)

    half = np.array([(x, y) for x in range(ax // 2) for y in range(ay // 2)])
    use = ((gx % 2 == 0) | (gx >= ax)) & ((gy % 2 == 0) | (gy >= ay))
    last = np.zeros((len(half), height))
    pick_x = second_x[np.ix_(half[:, 0], spot(gx, ax))]
    pick_y = second_y[np.ix_(half[:, 1], spot(gy, ay))]
    last[:, : len(given)] = pick_x * pick_y * use

    lanes = np.arange(az) * step
    out = np.concatenate((lanes, [1, step + 1]))
    send_lanes = np.zeros((8, LANES))
    send_lanes[np.ix_(np.arange(4), lanes)] = sent_z
    along = np.zeros((LANES, LANES))
    along[np.ix_(lanes, out)] = first_z[:, :az].T
    rim = np.zeros((16, LANES))
    for part in range(3):
        rim[np.ix_(4 * part + np.arange(4), out)] = first_z[:, az:].T
    along_last = np.zeros((LANES, LANES))
    source = np.concatenate((lanes[0::2], [1, step + 1]))
    along_last[np.ix_(source, lanes[0::2])] = second_z.T
    last = np.concatenate(cut_table(last @ rows))
    along = np.concatenate((along, along @ along_last), axis=1)
    rim = np.concatenate((rim, rim @ along_last), axis=1)
    result = (*sends, rows[: len(own)], last, send_lanes, along, np.roll(along, 1, 0), rim)
    return tuple(table.astype(jnp.bfloat16) for table in result)


def iota(shape, axis):
    return lax.broadcasted_iota(jnp.int32, shape, axis)


def roll(values, shift, axis):
    return pltpu.roll(values, shift % values.shape[axis], axis)


def lift_rows(v, low, high):
    n = v.shape[0]
    row = iota(v.shape, 0)
    odd = row % 2 == 1
    up = jnp.where(row == n - 1, high, roll(v, -1, 0))
    w = jnp.where(odd, v - 0.5 * (roll(v, 1, 0) + up), v)
    down = jnp.where(row == 0, low - 0.5 * v, roll(w, 1, 0))
    return jnp.where(odd, w, w + 0.25 * (down + roll(w, -1, 0)))


def lift_groups(v, rim, s):
    lane = iota(v.shape, 1)
    odd = (lane // s) % 2 == 1
    up = jnp.where(lane >= LANES - s, rim, roll(v, -s, 1))
    w = jnp.where(odd, v - 0.5 * (roll(v, s, 1) + up), v)
    down = jnp.where(lane < s, rim - 0.5 * v, roll(w, s, 1))
    return jnp.where(odd, w, w + 0.25 * (down + roll(w, -s, 1)))


def shrink(v, thresh):
    return v - jnp.clip(v, -thresh, thresh)


def three(v):
    parts = []
    for _ in range(3):
        parts.append(v.astype(jnp.bfloat16))
        v = v - parts[-1].astype(jnp.float32)
    return parts


def mix(a, b, dims):
    return lax.dot_general(a, b, (dims, ((), ())), preferred_element_type=jnp.float32)


def mix_rows(table, v):
    wide = mix(table, jnp.concatenate(three(v), axis=1), ((1,), (0,)))
    return wide[:, :LANES] + wide[:, LANES : 2 * LANES] + wide[:, 2 * LANES :]


def doubled(v, n):
    return v[0:n] + v[n:]


def mix_lanes(v, table):
    return mix(jnp.concatenate(three(v), axis=1), jnp.concatenate([table] * 3, axis=0), ((1,), (0,)))


def total(v):
    return jnp.sum(jnp.sum(v, axis=0, keepdims=True), axis=1, keepdims=True)


def kernel(sizes, cells, layout, exps_in, field_in, rows_in, lanes_in, *rest):
    packs = 1 + max(pack for pack, _, _ in layout)
    tables_in, (out, stats), scratch = rest[:packs], rest[packs : packs + 2], rest[packs + 2 :]
    nx, ny, nz = sizes
    ndev = nx * ny * nz
    scratch = list(scratch)
    held = scratch[-packs:]
    scratch = scratch[:-packs]
    tables = [held[pack].at[pl.ds(start, size)] for pack, start, size in layout]
    field, exps, k_s, l_s, in_sem = scratch[-5:]
    scratch = scratch[:-5]
    pairs = [(field_in, field), (exps_in, exps), *zip(tables_in, held), (rows_in, k_s), (lanes_in, l_s)]
    loads = [pltpu.make_async_copy(a, b, in_sem.at[i]) for i, (a, b) in enumerate(pairs)]
    me = (lax.axis_index("gx"), lax.axis_index("gy"), lax.axis_index("gz"))

    def device(dx, dy, dz):
        return (
            lax.rem(me[0] + (dx + nx), nx),
            lax.rem(me[1] + (dy + ny), ny),
            lax.rem(me[2] + (dz + nz), nz),
        )

    def distance(spot):
        return sum(min(d, size - d) for d, size in zip(spot, sizes))

    def thresh(level):
        return jnp.exp2(jnp.full((1, LANES), exps[level].astype(jnp.float32)))

    def split(j):
        return j // (ny * nz), (j // nz) % ny, j % nz

    def launch(copies, send_sem, recv_sem):
        flights = [
            pltpu.make_async_remote_copy(
                src_ref=f, dst_ref=t, send_sem=send_sem, recv_sem=recv_sem,
                device_id=device(*d), device_id_type=MESH,
            )
            for f, t, d in copies
        ]
        for flight in flights:
            flight.start()
        return sum(t.size for _, t, _ in copies) // LANES

    def settle(span, send_sem, recv_sem):
        for sem in (recv_sem, send_sem):
            pltpu.make_async_copy(span, span, sem).wait()

    barrier = pltpu.get_barrier_semaphore()

    near = max(sizes) // 2 <= ROUNDS
    greeted = {
        tuple((d + size - 1) % size if near else d for d, size in zip(spot, sizes))
        for spot in np.ndindex(*(3, 3, 3) if near else sizes)
    } - {(0, 0, 0)}
    for spot in sorted(greeted, key=lambda spot: (-distance(spot), spot)):
        pl.semaphore_signal(barrier, inc=1, device_id=device(*spot), device_id_type=MESH)
    for load in loads:
        load.start()
    gath, msg, parts_s, final_s, tally_s, tallies, g_send, g_recv, t_send, t_recv = scratch[-10:]
    loads[0].wait()
    loads[1].wait()
    step_to = (1, -1)
    alone = nx == 2
    ways = (0,) if alone else (0, 1)
    (xs, xh, xe, xr, ys, yr, es, er, yl, zs, zr, ds, dr, ts, txr, tcr, rim, work, send_sem, recv_sem) = scratch[:BUFFERS]
    middle = scratch[BUFFERS : BUFFERS + 15]
    grown, lifted, sent, edge1, side, hz, xzr, t2r, t3r, o1s, o2s, m_send, m_recv, y_send, y_recv = middle
    fine_lanes, fine_edges, fine_place, reach_rows, reach_lanes, *tables = tables
    src = field.at[0]
    px, n = src.shape[0], src.shape[1]
    half, q = n // 2, LANES // px
    lane = iota((n, LANES), 1)
    row8 = iota((8, LANES), 0)

    def ends(v):
        return v[n - 1 : n] - 0.5 * v[n - 2 : n - 1], v[0:1]

    def under(pair):
        return jnp.where(row8 == 0, pair[0], jnp.where(row8 == 1, pair[1], 0.0))

    lane_half = iota((half, LANES), 1)
    share = jnp.where(lane_half == LANES - 2, -0.125, jnp.where(lane_half == 0, 0.25, 0.0))
    share = jnp.where(lane_half == LANES - 1, -0.5, share)
    level_thresh = thresh(0)
    row = iota((half, LANES), 0)
    ax, ay = px // 2, half
    own = ax * ay
    px_rows, py_rows = 2 * ay, 2 * ax
    pair = px_rows + py_rows
    send_y, send_x, send_q, rows1, rows2, send_lanes, lanes12, odd_lanes12, rim12 = tables
    none = jnp.zeros((1, LANES), jnp.float32)

    def halves(ref, x):
        return [ref[x, pl.ds(start, half, stride=2), :] for start in (0, 1)]

    def stored(x):
        return [work[x, 0:half], work[x, half:]]

    def lift_halves(v, below, above):
        even, odd = v
        after = jnp.where(row == half - 1, above, roll(even, -1, 0))
        detail = odd - 0.5 * (even + after)
        before = jnp.where(row == 0, below - 0.5 * even, roll(detail, 1, 0))
        return [even + 0.25 * (before + detail), detail]

    def lift_last(stack, border):
        whole = mix_lanes(jnp.concatenate([v for v, _, _ in stack], axis=0), fine_lanes[...])
        for i, (_, x, kind) in enumerate(stack):
            yield x, kind, whole[half * i : half * i + half] + roll(border[kind], LANES - 2 - q * x, 1) * share

    def sideways(parts, target):
        edges = sum(mix(send_lanes[...], part, ((1,), (1,))) for part in three(jnp.concatenate(parts, axis=0)))
        for g in (0, 1):
            target[g, :, pl.ds(target.shape[2] - LANES, LANES)] = jnp.zeros((2, LANES), jnp.float32)
            target[g, :, pl.ds(0, edges.shape[1])] = edges[2 * g : 2 * g + 2]

    def both_kinds(a, b):
        return jnp.where(iota(a.shape, 1) % 2 == 0, a, roll(b, 1, 1))

    planes = (src[px - 1] - 0.5 * src[px - 2], src[0])
    ys[0] = src[:, n - 1, :] - 0.5 * src[:, n - 2, :]
    ys[1] = src[:, 0, :]
    for gx in (0, 1):
        xs[gx] = planes[gx]
        xh[gx, 0:half], xh[gx, half:] = lift_halves(halves(xs, gx), none, none)
        es[2 * gx], es[2 * gx + 1] = ends(planes[gx])
    packed = jnp.zeros((n, LANES), jnp.float32)
    for x in range(px):
        packed = jnp.where(lane // q == x, roll(src[x], q * x + 2, 1), packed)
    odd_end = roll(packed - 0.5 * roll(packed, 1, 1), 1, 1)
    even_end = jnp.where(lane % q == 1, roll(packed, -1, 1), roll(packed, -2, 1))
    packed = jnp.where(lane % q == 2, odd_end, even_end)
    zs[...] = packed
    ds[0], ds[1] = ends(packed)
    for load in loads[2 : 2 + packs]:
        load.wait()
    edges = sum(
        mix(fine_edges[...], part, ((1,), (1,)))
        for part in three(jnp.concatenate((packed, under(ends(packed))), axis=0))
    )
    ts[...] = jnp.zeros(ts.shape, jnp.float32)
    for g in (0, 1):
        ts[g, :, pl.ds(0, n + 8)] = edges[2 * g : 2 * g + 2]

    pl.semaphore_wait(barrier, len(greeted))
    along_y, others = [], []
    for g in (0, 1):
        dz = step_to[g]
        for gx in ways:
            for gy in (0, 1):
                along_y.append((ts.at[g], tcr.at[g, gy, gx], (step_to[gx], step_to[gy], dz)))
            others.append((ts.at[g], txr.at[g, gx], (step_to[gx], 0, dz)))
        for gy in (0, 1):
            along_y.append((ds.at[gy], dr.at[2 * g + gy], (0, step_to[gy], dz)))
    for gx in (0, 1):
        for gy in (0, 1):
            along_y.append((es.at[2 * gx + gy], er.at[2 * gx + gy], (step_to[gx], step_to[gy], 0)))
    for g in (0, 1):
        along_y.append((ys.at[g], yr.at[g], (0, step_to[g], 0)))
    for g in (0, 1):
        ends_of = pl.ds(2 * g, 2)
        others.append((es.at[ends_of], xe.at[ends_of], (step_to[g], 0, 0)))
    for g in (0, 1):
        others.append((xh.at[g, pl.ds(0, half)], xr.at[g, pl.ds(0, half)], (step_to[g], 0, 0)))
        along_y.append((xh.at[g, pl.ds(half, half)], xr.at[g, pl.ds(half, half)], (step_to[g], 0, 0)))
    for g in (0, 1):
        others.append((zs, zr.at[g], (0, 0, step_to[g])))
    y_rows = launch(along_y[:-2], y_send, y_recv)
    sent_rows = launch(others, send_sem, recv_sem)
    y_rows += launch(along_y[-2:], y_send, y_recv)

    even = halves(src, 0)
    before = [-0.5 * e for e in even]
    stack = []
    for k in range(px // 2):
        after = halves(src, 2 * k + 2) if 2 * k + 2 < px else [0.0, 0.0]
        detail = [o - 0.5 * (e + a) for o, e, a in zip(halves(src, 2 * k + 1), even, after)]
        smooth = [e + 0.25 * (b + d) for e, b, d in zip(even, before, detail)]
        for x, v in ((2 * k, smooth), (2 * k + 1, detail)):
            work[x, 0:half], work[x, half:] = lift_halves(v, none, none)
        even, before = after, detail
    for start in range(0, px, 2 * BATCH):
        block = jnp.concatenate([work[x, 0:half] for x in range(start, start + 2 * BATCH, 2)], axis=0)
        grown[pl.ds(start // 2 * half, BATCH * half), :] = mix_lanes(block, fine_lanes[...])
    settle(grown.at[pl.ds(0, sent_rows)], send_sem, recv_sem)

    lane2, row2 = iota((2, LANES), 1), iota((2, LANES), 0)

    def both(ref):
        return ref[0] if alone else jnp.where(row2 == 0, ref[0], ref[1])

    def columns(top, table):
        pieces = [part.astype(jnp.float32) for part in three(top)]
        pieces.append(jnp.zeros_like(top))
        return mix(jnp.concatenate(pieces, axis=0).astype(jnp.bfloat16), table, ((0,), (0,)))

    def kinds(a, b):
        return jnp.where(iota(a.shape, 1) % q == 2, a, b)

    tops = [jnp.where(lane2 < n, both(txr.at[g]), 0.0) for g in (0, 1)]
    beside = columns(jnp.concatenate(tops, axis=0), fine_place[...])[0:n]
    v = lift_groups(kinds(zr[0], zr[1]), beside, q)
    outer_rims = ends(v)
    lifted[...] = v
    rim[...] = lift_rows(v, none, none)
    border = [rim[pl.ds(0, half, stride=2), :]]
    near_x = mix_lanes(jnp.concatenate((xr[0, 0:half], xr[1, 0:half]), axis=0), fine_lanes[...])
    terms = {0: 0.25 * near_x[0:half], px - 2: -0.125 * near_x[half:]}
    for x in range(0, px, 2):
        spot = (pl.ds(x // 2 * half, half), slice(None))
        v = roll(border[0], LANES - 2 - q * x, 1) * share
        grown[spot] = grown[spot] + (v + terms[x] if x in terms else v)
    halo = mix_rows(send_y[...], grown[0:own])
    halo = (halo[0:py_rows], halo[py_rows : 2 * py_rows], halo[2 * py_rows :])
    sent[px_rows:pair] = both_kinds(halo[0], halo[1])
    sent[pair : pair + 16] = halo[2]
    blank = jnp.zeros((px_rows, LANES), jnp.float32)
    sideways((blank, halo[0], blank, halo[1], halo[2]), edge1)
    copies = []

    def rows_copy(start, size, to):
        copies.append((sent.at[pl.ds(start, size)], grown.at[pl.ds(own + start, size)], to))

    parts = len(ways)
    for g in (0, 1):
        for gy in (0, 1):
            for gx in ways:
                copies.append((edge1.at[g, :, pl.ds(LANES, LANES)], t3r.at[g, gy, gx], (step_to[gx], step_to[gy], step_to[g])))
            copies.append((edge1.at[g, :, pl.ds(0, LANES)], t2r.at[g, gy], (0, step_to[gy], step_to[g])))
    for gy in (0, 1):
        for gx in ways:
            rows_copy(pair + 8 * gy + 4 * gx, 8 // parts, (step_to[gx], step_to[gy], 0))
    for gy in (0, 1):
        rows_copy(px_rows + ax * gy, ax, (0, step_to[gy], 0))
    sent_rows = launch(copies, m_send, m_recv)
    def along_x(rims):
        rows = jnp.concatenate([yl[g, pl.ds(0, ax, stride=2), :] for g in (0, 1)], axis=0)
        turned = []
        for v in rims:
            v = jnp.broadcast_to(v, (8, LANES))
            for start in range(0, ax, 8):
                tile = jnp.zeros((8, LANES), jnp.float32)
                for i in range(8):
                    tile = jnp.where(row8 == i, roll(v, LANES - 2 - 2 * q * (start + i), 1), tile)
                turned.append(tile)
        return mix_lanes(rows, fine_lanes[...]) + jnp.concatenate(turned, axis=0) * share[0:1]

    beyond = [(xe[2 * g], xe[2 * g + 1]) for g in (0, 1)]
    for g in (0, 1):
        yl[g] = lift_rows(ys[g], beyond[0][g], beyond[1][g])
    raw = along_x(outer_rims)
    grown[pl.ds(own + pair + 16, py_rows), :] = raw
    grown[pl.ds(own + pair + 24 + py_rows, 8), :] = jnp.zeros((8, LANES), jnp.float32)
    settle(grown.at[pl.ds(0, y_rows)], y_send, y_recv)

    tops = []
    for g in (0, 1):
        yl[g] = lift_rows(yr[g], er[g], er[2 + g])
        v = jnp.where(lane2 == n, both(tcr.at[g, 0]), both(tcr.at[g, 1]))
        tops.append(jnp.where(lane2 // 2 == n // 2, v, 0.0))
    beside = columns(jnp.concatenate(tops, axis=0), fine_place[...])[n : n + 8]
    lower = lift_groups(under((kinds(dr[0], dr[2]), kinds(dr[1], dr[3]))), beside, q)
    lower = (lower[0:1], lower[1:2])
    late = along_x(lower)
    for at, scale, v in ((0, 0.25, late[0:ax]), (ay - 1, -0.125, late[ax:])):
        spot = (pl.ds(at, ax, stride=ay), slice(None))
        grown[spot] = grown[spot] + scale * v

    def finish():
        energy = kept = jnp.zeros((half, LANES), jnp.float32)
        rim[...] = lift_rows(lifted[...], *lower)
        border = [rim[pl.ds(start, half, stride=2), :] for start in (0, 1)]

        def fixed(x):
            smooth, detail = stored(x)
            for plane, kind, scale in ((0, 0, 0.25), (px - 2, 1, -0.125), (px - 1, 1, -0.5)):
                if x == plane:
                    smooth = smooth + scale * xr[kind, 0:half]
                    detail = detail + scale * xr[kind, half:]
            below, above = yl[0, x : x + 1, :], yl[1, x : x + 1, :]
            smooth = smooth + jnp.where(row == 0, 0.25 * below, jnp.where(row == half - 1, -0.125 * above, 0.0))
            return smooth, detail + jnp.where(row == half - 1, -0.5 * above, 0.0)

        for start in range(0, px, 4):
            stack, ready = [], []
            for x in range(start, start + 4, 2):
                ready.append((x, 0, grown[pl.ds(x // 2 * half, half), :]))
                stack.append((fixed(x)[1], x, 1))
                whole = fixed(x + 1)
                stack += [(whole[0], x + 1, 0), (whole[1], x + 1, 1)]
            for x, kind, v in (*ready, *lift_last(stack, border)):
                small = shrink(v, level_thresh)
                out[0, x, pl.ds(kind, half, stride=2), :] = small
                square, size = v * v, jnp.abs(small)
                if x % 2 == 0 and kind == 0:
                    square, size = (jnp.where(lane_half % 2 == 0, 0.0, u) for u in (square, size))
                energy += square
                kept += size
        return [total(energy), total(kept)]

    here = grown[0:own]
    halo = mix_rows(send_x[...], here)
    corner = mix_rows(send_q[...], raw)[0:8]
    sent[0:px_rows] = both_kinds(halo[0:px_rows], halo[px_rows:])
    sent[pair + 16 :] = corner
    blank = jnp.zeros((py_rows, LANES), jnp.float32)
    filled = jnp.zeros((16, LANES), jnp.float32)
    sideways((here, halo[0:px_rows], blank, halo[px_rows:], blank, filled, raw, corner, filled[0:8]), side)
    copies = []
    for g in (0, 1):
        for gx in ways:
            copies.append((side.at[g, :, pl.ds(own, 2 * LANES)], xzr.at[g, gx], (step_to[gx], 0, step_to[g])))
        copies.append((side.at[g], hz.at[g], (0, 0, step_to[g])))
    for gx in ways:
        size = 8 // parts
        at = own + pair + 16 + py_rows + size * gx
        copies.append((sent.at[pl.ds(pair + 16 + size * gx, size)], grown.at[pl.ds(at, size)], (step_to[gx], 0, 0)))
        rows_copy(ay * gx, px_rows // parts, (step_to[gx], 0, 0))
    sent_rows += launch(copies, m_send, m_recv)
    extra = 2 * pair + 16 + py_rows + 16

    spots = nx * ny
    slot = (me[2] * nx + me[0]) * ny + me[1]
    cx, cy, cz = ax // 4, ay // 4, LANES // 2**FINE
    step = 2**FINE
    count = cx * cy
    long, deep, reach = cx + 3, cy + 3, cz + 3
    cut = LANES - reach * (deep - 1)
    rest = reach - cut

    def spread(source, target, send_sem, recv_sem, first=0, last=None):
        def post(j):
            return pltpu.make_async_remote_copy(
                src_ref=source, dst_ref=target, send_sem=send_sem, recv_sem=recv_sem,
                device_id=device(*split(j)), device_id_type=MESH,
            )

        def send(j, carry):
            post(j).start()
            return carry

        if ndev <= 32:
            order = sorted(range(1, ndev), key=lambda j: (-distance(split(j)), j))
            for j in order[first:last]:
                post(j).start()
        elif first == 0:
            lax.fori_loop(1, ndev, send, 0)

    pieces = mix_rows(reach_rows[...], here)
    pieces = doubled(pieces, 8 * deep)
    blocks = [part.astype(jnp.float32) for part in three(pieces)]

    def stack(first, last):
        rows = [jnp.concatenate([b[8 * y : 8 * y + 8] for y in range(first, last)], axis=1) for b in blocks]
        return jnp.concatenate(rows + [jnp.zeros_like(rows[0])], axis=0).astype(jnp.bfloat16)

    def fold(v):
        return v[0:8] + v[8:16] + v[16:24]

    sheet = fold(mix(stack(0, deep), reach_lanes[pl.ds(0, deep * LANES), :], ((1,), (0,))))
    loose = fold(mix(stack(deep - 1, deep), reach_lanes[pl.ds(deep * LANES, LANES), :], ((1,), (0,))))
    spare = loose[0:1]
    for x in range(1, long):
        spare += roll(loose[x : x + 1], rest * x, 1)
    msg[...] = jnp.where(row8 == long, spare, sheet)
    spread(msg, gath.at[slot], g_send, g_recv, 0, ndev // 2)
    gath[slot] = msg[...]
    sums = finish()
    quarter = own // 4

    def level_rows(v, columns):
        return (
            mix_rows(rows1[:, columns], v[:, 0:LANES]),
            doubled(mix_rows(rows2[:, columns], v[:, LANES:]), quarter),
        )

    o1s[...], early = level_rows(mix_lanes(here, lanes12[...]), pl.ds(0, own))
    o2s[...] = early.reshape(o2s.shape)
    spread(msg, gath.at[slot], g_send, g_recv, ndev // 2)
    settle(grown.at[pl.ds(0, sent_rows)], m_send, m_recv)

    for g in (0, 1):
        across = (xzr.at[g, 0], xzr.at[g, 0 if alone else 1])
        place_in = lane2 % pair
        v = jnp.where(place_in < ay, across[0][:, 0:LANES], across[1][:, 0:LANES])
        v = jnp.where(place_in < px_rows, v, jnp.where(place_in < px_rows + ax, t2r[g, 0], t2r[g, 1]))
        hz[g, :, pl.ds(own, LANES)] = v
        u = []
        for gy in (0, 1):
            u.append(jnp.where(lane2 % 8 < 4, t3r[g, gy, 0], t3r[g, gy, 0 if alone else 1]))
        v = jnp.where(lane2 < 8, u[0], u[1])
        w = jnp.where(lane2 < 20 + py_rows, across[0][:, LANES:], across[1][:, LANES:])
        w = jnp.where(lane2 < 16 + py_rows, hz[g, :, pl.ds(own + LANES, LANES)], w)
        v = jnp.where(lane2 < 16, v, jnp.where(lane2 < 24 + py_rows, w, 0.0))
        hz[g, :, pl.ds(own + LANES, LANES)] = v
    rim_rows = columns(jnp.concatenate((hz[0], hz[1]), axis=0), rim12[...])
    got = grown[pl.ds(own, extra - pair), :]
    outer = mix_lanes(got, lanes12[...])
    outer = (outer[0:pair], mix_lanes(got[0:pair], odd_lanes12[...]), outer[pair:])
    outer = jnp.concatenate(outer, axis=0) + rim_rows[own : own + extra]
    late = level_rows(jnp.concatenate((rim_rows[0:own], outer), axis=0), pl.ds(0, own + extra))
    first = o1s[...] + late[0]
    second = o2s[...].reshape(quarter, LANES) + late[1]
    o1s[...] = first
    o2s[...] = second.reshape(o2s.shape)

    def tally(v, level, ny):
        s = 2**level
        row, at = iota(v.shape, 0), iota(v.shape, 1)
        smooth = ((row // ny) % 2 == 0) & (row % 2 == 0) & (at % (2 * s) == 0)
        use = (at % s == 0) & ~smooth
        small = shrink(v, thresh(level))
        return [total(jnp.where(use, v * v, 0.0)), total(jnp.where(use, jnp.abs(small), 0.0))]

    sums += tally(first, 1, ay) + tally(second, 2, ay // 2)

    def place(source, level):
        s = 2**level
        small_y = ay >> (level - 1)
        keep = iota((small_y, LANES), 1) % s == 0
        for x in range(ax >> (level - 1)):
            spot = (0, s * x, pl.ds(0, small_y, stride=s), slice(None))
            out[spot] = jnp.where(keep, shrink(source(x), thresh(level)), out[spot])

    one = iota((1, LANES), 1)
    tail = jnp.zeros((1, LANES), jnp.float32)
    for i, whole in enumerate(sums):
        tail = jnp.where(one == i, whole, tail)
    tally_s[...] = tail
    spread(tally_s, tallies.at[slot], t_send, t_recv)
    tallies[slot] = tail
    place(lambda x: o1s[pl.ds(x * ay, ay), :], 1)
    place(lambda x: o2s[x], 2)
    settle(gath.at[pl.ds(0, ndev - 1)], g_send, g_recv)

    at = iota((spots, LANES), 1)
    spares = [gath[pl.ds(z * spots, spots), long, :] for z in range(nz)]

    def window(v, source, start, size):
        moved = roll(v, start - source, 1)
        return jnp.where((at >= start) & (at < start + size), moved, 0.0)

    for x in range(long):
        boxes = [gath[pl.ds(z * spots, spots), x, :] for z in range(nz)]
        for y in range(deep):
            fit = reach if y < deep - 1 else cut
            v = sum(window(boxes[z], reach * y, cz * z, fit) for z in range(nz))
            if fit < reach:
                v += sum(window(spares[z], rest * x, cz * z + cut, rest) for z in range(nz))
            parts_s[pl.ds((y * long + x) * spots, spots), :] = v

    filled = long * deep * spots
    spare_rows = parts_s.shape[0] - filled
    if spare_rows:
        parts_s[pl.ds(filled, spare_rows), :] = jnp.zeros((spare_rows, LANES), jnp.float32)
    grid = parts_s[...]
    loads[2 + packs].wait()
    loads[3 + packs].wait()
    cells_in = spots * count
    grid = mix_rows(k_s[...], grid)
    half3, half4 = grid[0:cells_in], doubled(grid[cells_in:], cells_in)
    grid, grid4 = mix_lanes(half3, l_s[0]), mix_lanes(half4, l_s[1])
    row = iota(grid.shape, 0)
    lane = iota(grid.shape, 1)
    inner_row = row % count
    gx, gy, gz = inner_row // cy, inner_row % cy, lane // step
    valid = lane % step < nz
    even3 = (gx % 2 == 0) & (gy % 2 == 0) & (gz % 2 == 0)
    even4 = (gx % 4 == 0) & (gy % 4 == 0) & (gz % 4 == 0)
    det3 = valid & ~even3
    det4 = valid & even3 & ~even4
    small3 = shrink(grid, thresh(FINE))
    small4 = shrink(grid4, thresh(FINE + 1))
    final_s[...] = jnp.where(even3, jnp.where(even4, grid4, small4), small3)

    def masked(mask, v):
        return total(jnp.where(mask, v, 0.0))

    coarse = ((masked(det3, grid * grid), masked(det3, jnp.abs(small3))),
              (masked(det4, grid4 * grid4), masked(det4, jnp.abs(small4))))
    first = pl.multiple_of((me[0] * ny + me[1]) * count, count)
    mine = pltpu.roll(final_s[pl.ds(first, count), :], lax.rem(LANES - me[2], LANES), 1)
    keep = iota((cy, LANES), 1) % step == 0
    for x in range(cx):
        spot = (0, step * x, pl.ds(0, cy, stride=step), slice(None))
        out[spot] = jnp.where(keep, mine[x * cy : x * cy + cy], out[spot])

    settle(tallies.at[pl.ds(0, ndev - 1)], t_send, t_recv)
    tail = jnp.sum(tallies[...], axis=0)
    for q in (0, 1):
        line = jnp.zeros((1, LANES), jnp.float32)
        for level in range(LEVELS):
            weight = 8.0 ** (level + 1) / (7.0 * cells)
            if level < FINE:
                value = jnp.sum(jnp.where(one == 2 * level + q, tail, 0.0), axis=1, keepdims=True)
            else:
                value = coarse[level - FINE][q]
            line = jnp.where(one == level, value * weight, line)
        stats[q] = line[:, 0:LEVELS]


def deliver(held, held_stats, out, stats, sem):
    rows = held.shape[1] // CHUNKS
    copies = [pltpu.make_async_copy(held_stats, stats, sem.at[CHUNKS])]
    for i in range(CHUNKS):
        part = pl.ds(i * rows, rows)
        copies.append(pltpu.make_async_copy(held.at[:, part], out.at[:, part], sem.at[i]))
    for copy in copies:
        copy.start()
    for copy in copies:
        copy.wait()


def pack_tables(tables):
    groups, layout = {}, []
    for table in tables:
        group = groups.setdefault(table.shape[1], [])
        start = sum(len(part) for part in group)
        layout.append((list(groups).index(table.shape[1]), start, len(table)))
        group.append(np.pad(table, ((0, -len(table) % 16), (0, 0))))
    return [np.concatenate(group) for group in groups.values()], layout


def shards(sizes, fields, exponents):
    nx, ny, nz = sizes
    ndev = nx * ny * nz
    _, lx, ly, lz = fields.shape
    cells = fields.size * ndev
    step = 2**FINE
    coarse = (lx // step, ly // step, lz // step)
    count = coarse[0] * coarse[1]
    tables = coarse_matrices(sizes, coarse)
    middle = middle_tables(lx // 2, ly // 2, lz // 2)
    own, extra = lx // 2 * (ly // 2), middle[0].shape[0]
    middle, layout = pack_tables(fine_tables(lx) + reach_tables(lx // 2, ly // 2, lz // 2) + middle)
    scratch = [
        *(pltpu.VMEM(shape, jnp.float32) for shape in (
            (2, ly, LANES), (2, ly, LANES), (4, 1, LANES), (2, ly, LANES), (2, lx, LANES), (2, lx, LANES),
            (4, 1, LANES), (4, 1, LANES),
            (2, lx, LANES), (ly, LANES), (2, ly, LANES), (2, 1, LANES), (4, 1, LANES), (2, 2, LANES),
            (2, 2, 2, LANES), (2, 2, 2, 2, LANES), (ly, LANES), (lx, ly, LANES),
        )),
        pltpu.SemaphoreType.DMA,
        pltpu.SemaphoreType.DMA,
        *(pltpu.VMEM(shape, jnp.float32) for shape in (
            (own + 2 * lx + ly + 32, LANES), (ly, LANES), (lx + ly + 24, LANES), (2, 2, 2 * LANES),
            (2, 2, own + 2 * LANES), (2, 2, own + 2 * LANES), (2, 2, 2, 2 * LANES), (2, 2, 2, LANES),
            (2, 2, 2, 2, LANES), (own, LANES), (lx // 4, ly // 4, LANES),
        )),
        pltpu.SemaphoreType.DMA,
        pltpu.SemaphoreType.DMA,
        pltpu.SemaphoreType.DMA,
        pltpu.SemaphoreType.DMA,
    ]
    scratch += [
        pltpu.VMEM((ndev, 8, LANES), jnp.float32),
        pltpu.VMEM((8, LANES), jnp.float32),
        pltpu.VMEM((tables[0].shape[1], LANES), jnp.float32),
        pltpu.VMEM((nx * ny * count, LANES), jnp.float32),
        pltpu.VMEM((1, LANES), jnp.float32),
        pltpu.VMEM((ndev, 1, LANES), jnp.float32),
        *[pltpu.SemaphoreType.DMA] * 4,
        pltpu.VMEM(fields.shape, jnp.float32),
        pltpu.SMEM(exponents.shape, jnp.int32),
        pltpu.VMEM(tables[0].shape, jnp.bfloat16),
        pltpu.VMEM(tables[1].shape, jnp.bfloat16),
        pltpu.SemaphoreType.DMA((4 + len(middle),)),
        *(pltpu.VMEM(table.shape, table.dtype) for table in middle),
    ]
    vmem = pl.BlockSpec(memory_space=pltpu.VMEM)
    held = pl.pallas_call(
        functools.partial(kernel, sizes, cells, layout),
        out_shape=(
            pltpu.VMEM(fields.shape, jnp.float32),
            pltpu.VMEM((2, 1, LEVELS), jnp.float32),
        ),
        in_specs=[pl.BlockSpec(memory_space=pltpu.HBM)] * (4 + len(middle)),
        out_specs=(vmem, vmem),
        scratch_shapes=scratch,
        compiler_params=pltpu.CompilerParams(
            collective_id=0, has_side_effects=True, vmem_limit_bytes=VMEM_LIMIT
        ),
    )(*(pltpu.with_memory_space_constraint(x, pltpu.HBM) for x in (exponents, fields, *map(jnp.asarray, (*tables, *middle)))))
    hbm = pl.BlockSpec(memory_space=pltpu.HBM)
    return pl.pallas_call(
        deliver,
        out_shape=(
            jax.ShapeDtypeStruct(fields.shape, jnp.float32),
            jax.ShapeDtypeStruct((2, 1, LEVELS), jnp.float32),
        ),
        in_specs=(vmem, vmem),
        out_specs=(hbm, hbm),
        scratch_shapes=[pltpu.SemaphoreType.DMA((CHUNKS + 1,))],
    )(*(pltpu.with_memory_space_constraint(x, pltpu.VMEM) for x in held))


def solution(mesh):
    sizes = tuple(mesh.shape[name] for name in ("gx", "gy", "gz"))
    placed = (P(None, "gx", "gy", "gz"), P())
    return jax.shard_map(
        functools.partial(shards, sizes),
        mesh=mesh,
        in_specs=placed,
        out_specs=placed,
        check_vma=False,
    )
```
